32 devices in a mesh: section: 2 (over x), dp: 8 (over z, y), tensor: 2 (over core).
Axes of the slice: x: 2, y: 2, z: 4, core: 2. Of those that a mesh axis runs over, the one named last changes fastest.
Arguments:
- images: bfloat16 [128, 196, 512], P('dp', 'tensor'), may hold values from -6 to 6
- cotangent: bfloat16 [128, 196, 512], P('dp', 'tensor'), may hold values from -6 to 6
- norm1_gain: bfloat16 [2, 512], P('section', 'dp'), may hold values from 0.5 to 1.5
- norm1_bias: bfloat16 [2, 512], P('section', 'dp'), may hold values from -1.75 to 1.75
- qkv_weight: bfloat16 [2, 512, 3, 512], P('section', 'dp', None, 'tensor'), may hold values from -0.25 to 0.25
- qkv_bias: bfloat16 [2, 3, 512], P('section', None, ('tensor', 'dp')), may hold values from -1.75 to 1.75
- position_table: float32 [2, 169, 16], P('section', None, 'tensor'), may hold values from -6 to 6
- proj_weight: bfloat16 [2, 512, 512], P('section', ('tensor', 'dp')), may hold values from -0.75 to 0.75
- proj_bias: bfloat16 [2, 512], P('section', 'dp'), may hold values from -1.75 to 1.75
- norm2_gain: bfloat16 [2, 512], P('section', 'dp'), may hold values from 0.5 to 1.5
- norm2_bias: bfloat16 [2, 512], P('section', 'dp'), may hold values from -1.75 to 1.75
- fc1_weight: bfloat16 [2, 512, 2048], P('section', 'dp', 'tensor'), may hold values from -0.25 to 0.25
- fc1_bias: bfloat16 [2, 2048], P('section', ('tensor', 'dp')), may hold values from -1.75 to 1.75
- fc2_weight: bfloat16 [2, 2048, 512], P('section', ('tensor', 'dp')), may hold values from -0.125 to 0.125
- fc2_bias: bfloat16 [2, 512], P('section', 'dp'), may hold values from -1.75 to 1.75
Outputs:
- activations: bfloat16 [2, 128, 196, 512], P('section', 'dp', 'tensor')
- input_grad: bfloat16 [2, 128, 196, 512], P('section', 'dp', 'tensor')
- norm1_gain_grad: float32 [2, 512], P('section', 'dp')
- norm1_bias_grad: float32 [2, 512], P('section', 'dp')
- qkv_weight_grad: float32 [2, 512, 3, 512], P('section', 'dp', None, 'tensor')
- qkv_bias_grad: float32 [2, 3, 512], P('section', None, ('tensor', 'dp'))
- position_table_grad: float32 [2, 169, 16], P('section', None, 'tensor')
- proj_weight_grad: float32 [2, 512, 512], P('section', ('tensor', 'dp'))
- proj_bias_grad: float32 [2, 512], P('section', 'dp')
- norm2_gain_grad: float32 [2, 512], P('section', 'dp')
- norm2_bias_grad: float32 [2, 512], P('section', 'dp')
- fc1_weight_grad: float32 [2, 512, 2048], P('section', 'dp', 'tensor')
- fc1_bias_grad: float32 [2, 2048], P('section', ('tensor', 'dp'))
- fc2_weight_grad: float32 [2, 2048, 512], P('section', ('tensor', 'dp'))
- fc2_bias_grad: float32 [2, 512], P('section', 'dp')
The draws below stay inside these ranges and needn't reach their ends.
All inputs are finite; a program needn't handle non-finite values.
Results may differ from the reference program's by a relative error of at most 0.023.
Values may be sent and summed in bfloat16 or wider, within the bound.
A program may use at most 256 MiB of HBM per device.

```python
import jax
import jax.numpy as jnp
from jax import lax

D = 512
HEADS = 16
FF = 2048
WIN = 7
SIDE = 14
SHIFT = 3
PATCHES = 196
IMAGES = 128
N_DP = 8


def block_scale(rng, extent, pieces, least, high):
    level = 1.0
    for axis_at, blocks in pieces:
        draws = jax.random.uniform(jax.random.fold_in(jax.random.fold_in(rng, 6), axis_at), (blocks,), jnp.float32, least / len(pieces), high / len(pieces))
        level = level * jnp.repeat(jnp.exp(draws), extent[axis_at] // blocks).reshape((-1,) + (1,) * (len(extent) - 1 - axis_at))
    return level


def normal_values(rng, shape, scale, reach, cuts=(), dtype=jnp.bfloat16):
    values = scale * jax.random.normal(rng, shape, jnp.float32)
    if cuts:
        values = values * block_scale(rng, shape, cuts, -0.22, 0.18)
    return jnp.clip(values, -reach, reach).astype(dtype)


def setup_inputs(seed: int = 0) -> dict:
    key_of = jax.random.split(jax.random.key(seed), 16)
    images = normal_values(key_of[0], (IMAGES, PATCHES, D), 1.0, 6.0, ((0, 8), (1, 2)))
    cotangent = normal_values(key_of[1], (IMAGES, PATCHES, D), 1.0, 6.0, ((0, 8), (1, 2)))
    norm1_gain = jnp.clip(1.0 + 0.1 * jax.random.normal(key_of[2], (2, D), jnp.float32), 0.5, 1.5).astype(jnp.bfloat16)
    norm1_bias = normal_values(key_of[3], (2, D), 0.3, 1.75, ((0, 2), (1, 8)))
    qkv_weight = normal_values(key_of[4], (2, D, 3, D), D ** -0.5, 0.25, ((0, 2), (1, 8), (3, 2)))
    qkv_bias = normal_values(key_of[5], (2, 3, D), 0.3, 1.75, ((0, 2), (2, 16)))
    position_table = normal_values(key_of[6], (2, (2 * WIN - 1) ** 2, HEADS), 1.0, 6.0, ((0, 2), (2, 2)), jnp.float32)
    proj_weight = normal_values(key_of[7], (2, D, D), (D // 8) ** -0.5, 0.75, ((0, 2), (1, 16)))
    proj_bias = normal_values(key_of[8], (2, D), 0.3, 1.75, ((0, 2), (1, 8)))
    norm2_gain = jnp.clip(1.0 + 0.1 * jax.random.normal(key_of[9], (2, D), jnp.float32), 0.5, 1.5).astype(jnp.bfloat16)
    norm2_bias = normal_values(key_of[10], (2, D), 0.3, 1.75, ((0, 2), (1, 8)))
    fc1_weight = normal_values(key_of[11], (2, D, FF), D ** -0.5, 0.25, ((0, 2), (1, 8), (2, 2)))
    fc1_bias = normal_values(key_of[12], (2, FF), 0.3, 1.75, ((0, 2), (1, 16)))
    fc2_weight = normal_values(key_of[13], (2, FF, D), FF ** -0.5, 0.125, ((0, 2), (1, 16)))
    fc2_bias = normal_values(key_of[14], (2, D), 0.3, 1.75, ((0, 2), (1, 8)))
    return {"images": images, "cotangent": cotangent, "norm1_gain": norm1_gain, "norm1_bias": norm1_bias, "qkv_weight": qkv_weight, "qkv_bias": qkv_bias, "position_table": position_table, "proj_weight": proj_weight, "proj_bias": proj_bias, "norm2_gain": norm2_gain, "norm2_bias": norm2_bias, "fc1_weight": fc1_weight, "fc1_bias": fc1_bias, "fc2_weight": fc2_weight, "fc2_bias": fc2_bias}


EPS = 1e-05
MASK_FILL = -100.0
ROOT_HALF = 0.7071067811865476
INV_ROOT_TWO_PI = 0.3989422804014327

def to_windows(grid, shift_amount):
    image_count = grid.shape[0]
    channels = grid.shape[-1]
    across = SIDE // WIN
    spatial = grid.reshape(image_count, SIDE, SIDE, channels)
    spatial = jnp.roll(spatial, -shift_amount, 1)
    spatial = jnp.roll(spatial, -shift_amount, 2)
    spatial = spatial.reshape(image_count, across, WIN, across, WIN, channels).transpose(0, 1, 3, 2, 4, 5)
    return spatial.reshape(image_count, across * across, WIN * WIN, channels)

def from_windows(windowed, shift_amount):
    image_count = windowed.shape[0]
    channels = windowed.shape[-1]
    across = SIDE // WIN
    spatial = windowed.reshape(image_count, across, across, WIN, WIN, channels).transpose(0, 1, 3, 2, 4, 5)
    spatial = spatial.reshape(image_count, SIDE, SIDE, channels)
    spatial = jnp.roll(spatial, shift_amount, 1)
    spatial = jnp.roll(spatial, shift_amount, 2)
    return spatial.reshape(image_count, SIDE * SIDE, channels)

def relative_onehot():
    positions = jnp.arange(WIN * WIN)
    row_of = positions // WIN
    col_of = positions % WIN
    table_side = 2 * WIN - 1
    offsets = (row_of[:, None] - row_of[None, :] + WIN - 1) * table_side + (col_of[:, None] - col_of[None, :] + WIN - 1)
    return (offsets.reshape(-1)[:, None] == jnp.arange(table_side * table_side)[None, :]).astype(jnp.float32)

def region_mask(shift_amount, active):
    lines = jnp.arange(SIDE)
    region = jnp.where(lines < SIDE - WIN, 0, jnp.where(lines < SIDE - shift_amount, 1, 2))
    labels = (region[:, None] * 3 + region[None, :]).astype(jnp.float32)
    window_labels = to_windows(labels.reshape(1, SIDE * SIDE, 1), 0)[0, :, :, 0]
    differs = window_labels[:, :, None] != window_labels[:, None, :]
    return jnp.where(differs, MASK_FILL, 0.0).astype(jnp.float32) * active

def norm_stats(values):
    center = values - lax.optimization_barrier(jnp.mean(values, -1, keepdims=True))
    inverse = lax.rsqrt(lax.optimization_barrier(jnp.mean(center * center, -1, keepdims=True)) + EPS)
    return (center * inverse, inverse)

def norm_backward(upstream, normed, inverse, gain):
    scaled = upstream * gain
    return inverse * (scaled - lax.optimization_barrier(jnp.mean(scaled, -1, keepdims=True)) - normed * lax.optimization_barrier(jnp.mean(scaled * normed, -1, keepdims=True)))

def gelu_value(values):
    return 0.5 * values * (1.0 + jax.scipy.special.erf(values * ROOT_HALF))

def gelu_slope(values):
    return 0.5 * (1.0 + jax.scipy.special.erf(values * ROOT_HALF)) + values * jnp.exp(-0.5 * values * values) * INV_ROOT_TWO_PI

def widen(array):
    return array.astype(jnp.float32)

def attention_scores(query_heads, key_heads, params):
    raw = jnp.einsum('bwihd,bwjhd->bwhij', widen(query_heads), widen(key_heads))
    return raw * params['scaling'] + params['bias_heads'][None, None] + params['mask'][None, :, None]

def block_forward(block_in, params):
    shift_amount = params['shift']
    heads = params['heads']
    residual = widen(block_in)
    normed_one, inverse_one = norm_stats(residual)
    first_norm = (normed_one * params['gain_one'] + params['beta_one']).astype(jnp.bfloat16)
    windows_a = to_windows(first_norm, shift_amount)
    projected = jnp.einsum('bwtc,cke->bwtke', widen(windows_a), widen(params['qkv_weight'])) + params['qkv_bias']
    split_heads = projected.astype(jnp.bfloat16).reshape(projected.shape[:3] + (3, heads, D // heads))
    query_heads = split_heads[:, :, :, 0]
    key_heads = split_heads[:, :, :, 1]
    value_heads = split_heads[:, :, :, 2]
    scores = attention_scores(query_heads, key_heads, params)
    row_max = lax.optimization_barrier(jnp.max(scores, -1, keepdims=True))
    log_total = row_max + jnp.log(lax.optimization_barrier(jnp.sum(jnp.exp(scores - row_max), -1, keepdims=True)))
    weights_b = jnp.exp(scores - log_total).astype(jnp.bfloat16)
    context = jnp.einsum('bwhij,bwjhd->bwihd', widen(weights_b), widen(value_heads)).astype(jnp.bfloat16)
    context = context.reshape(context.shape[:3] + (D,))
    attended = jnp.einsum('bwte,ed->bwtd', widen(context), widen(params['proj_weight']))
    midway = residual + from_windows(attended, shift_amount) + params['proj_bias']
    normed_two, inverse_two = norm_stats(midway)
    second_norm = (normed_two * params['gain_two'] + params['beta_two']).astype(jnp.bfloat16)
    hidden_pre = jnp.einsum('btc,cf->btf', widen(second_norm), widen(params['fc1_weight'])) + params['fc1_bias']
    activated = gelu_value(hidden_pre).astype(jnp.bfloat16)
    mlp_out = jnp.einsum('btf,fd->btd', widen(activated), widen(params['fc2_weight']))
    block_out = (midway + mlp_out + params['fc2_bias']).astype(jnp.bfloat16)
    saved = (block_in, windows_a, query_heads, key_heads, value_heads, log_total, context, midway, second_norm, hidden_pre)
    return (block_out, saved)

def block_backward(saved, grad_out, params):
    block_in, windows_a, query_heads, key_heads, value_heads, log_total, context, midway, second_norm, hidden_pre = saved
    shift_amount = params['shift']
    gradient = widen(grad_out)
    fc2_bias_part = lax.optimization_barrier(jnp.sum(gradient, (0, 1)))
    activated = gelu_value(hidden_pre).astype(jnp.bfloat16)
    fc2_part = jnp.einsum('btf,btd->fd', widen(activated), gradient)
    hidden_grad = jnp.einsum('btd,fd->btf', gradient, widen(params['fc2_weight'])) * gelu_slope(hidden_pre)
    fc1_bias_part = lax.optimization_barrier(jnp.sum(hidden_grad, (0, 1)))
    hidden_grad_b = hidden_grad.astype(jnp.bfloat16)
    fc1_part = jnp.einsum('btc,btf->cf', widen(second_norm), widen(hidden_grad_b))
    norm_two_grad = jnp.einsum('btf,cf->btc', widen(hidden_grad_b), widen(params['fc1_weight']))
    normed_two, inverse_two = norm_stats(midway)
    midway_grad = gradient + norm_backward(norm_two_grad, normed_two, inverse_two, params['gain_two'])
    gain_two_part = lax.optimization_barrier(jnp.sum(norm_two_grad * normed_two, (0, 1)))
    beta_two_part = lax.optimization_barrier(jnp.sum(norm_two_grad, (0, 1)))
    proj_bias_part = lax.optimization_barrier(jnp.sum(midway_grad, (0, 1)))
    midway_rows = to_windows(midway_grad.astype(jnp.bfloat16), shift_amount)
    proj_part = jnp.einsum('bwte,bwtd->ed', widen(context), widen(midway_rows))
    context_grad = jnp.einsum('bwtd,ed->bwte', widen(midway_rows), widen(params['proj_weight'])).astype(jnp.bfloat16)
    context_grad = context_grad.reshape(query_heads.shape)
    scores = attention_scores(query_heads, key_heads, params)
    soft = jnp.exp(scores - log_total)
    soft_b = soft.astype(jnp.bfloat16)
    prob_grad = jnp.einsum('bwihd,bwjhd->bwhij', widen(context_grad), widen(value_heads))
    value_grad = jnp.einsum('bwhij,bwihd->bwjhd', widen(soft_b), widen(context_grad))
    scores_grad = soft * (prob_grad - lax.optimization_barrier(jnp.sum(soft * prob_grad, -1, keepdims=True)))
    bias_part = lax.optimization_barrier(jnp.sum(scores_grad, (0, 1)))
    scores_b = scores_grad.astype(jnp.bfloat16)
    query_grad = jnp.einsum('bwhij,bwjhd->bwihd', widen(scores_b), widen(key_heads)) * params['scaling']
    key_grad = jnp.einsum('bwhij,bwihd->bwjhd', widen(scores_b), widen(query_heads)) * params['scaling']
    qkv_grad = jnp.stack([query_grad, key_grad, value_grad], 3).reshape(windows_a.shape[:3] + (3, D))
    qkv_bias_part = lax.optimization_barrier(jnp.sum(qkv_grad, (0, 1, 2)))
    qkv_grad_b = qkv_grad.astype(jnp.bfloat16)
    qkv_part = jnp.einsum('bwtc,bwtke->cke', widen(windows_a), widen(qkv_grad_b))
    norm_one_grad = from_windows(jnp.einsum('bwtke,cke->bwtc', widen(qkv_grad_b), widen(params['qkv_weight'])), shift_amount)
    normed_one, inverse_one = norm_stats(widen(block_in))
    input_grad = (midway_grad + norm_backward(norm_one_grad, normed_one, inverse_one, params['gain_one'])).astype(jnp.bfloat16)
    gain_one_part = lax.optimization_barrier(jnp.sum(norm_one_grad * normed_one, (0, 1)))
    beta_one_part = lax.optimization_barrier(jnp.sum(norm_one_grad, (0, 1)))
    shared = jnp.stack([gain_one_part, beta_one_part, proj_bias_part, gain_two_part, beta_two_part, fc2_bias_part])
    return (input_grad, (qkv_part, proj_part, fc1_part, fc2_part, qkv_bias_part, fc1_bias_part, shared, bias_part))

def reference(images, cotangent, norm1_gain, norm1_bias, qkv_weight, qkv_bias, position_table, proj_weight, proj_bias, norm2_gain, norm2_bias, fc1_weight, fc1_bias, fc2_weight, fc2_bias):
    onehot = relative_onehot()
    heads = position_table.shape[-1]
    sections = []
    for section_index in range(2):
        shift_amount = SHIFT * section_index
        bias_flat = jnp.dot(onehot, position_table[section_index], precision=lax.Precision.HIGHEST)
        sections.append({'shift': shift_amount, 'heads': heads, 'scaling': (D // heads) ** (-0.5), 'mask': region_mask(shift_amount, float(section_index)), 'bias_heads': bias_flat.reshape(WIN * WIN, WIN * WIN, heads).transpose(2, 0, 1), 'gain_one': widen(norm1_gain[section_index]), 'beta_one': widen(norm1_bias[section_index]), 'qkv_weight': qkv_weight[section_index], 'qkv_bias': widen(qkv_bias[section_index]), 'proj_weight': proj_weight[section_index], 'proj_bias': widen(proj_bias[section_index]), 'gain_two': widen(norm2_gain[section_index]), 'beta_two': widen(norm2_bias[section_index]), 'fc1_weight': fc1_weight[section_index], 'fc1_bias': widen(fc1_bias[section_index]), 'fc2_weight': fc2_weight[section_index], 'fc2_bias': widen(fc2_bias[section_index])})

    def zero_terms():
        return (jnp.zeros((D, 3, D), jnp.float32), jnp.zeros((D, D), jnp.float32), jnp.zeros((D, FF), jnp.float32), jnp.zeros((FF, D), jnp.float32), jnp.zeros((3, D), jnp.float32), jnp.zeros((FF,), jnp.float32), jnp.zeros((6, D), jnp.float32), jnp.zeros((heads, WIN * WIN, WIN * WIN), jnp.float32))

    def one_group(totals, group):
        block_in, grad_out = group
        middle, saved_zero = block_forward(block_in, sections[0])
        final, saved_one = block_forward(middle, sections[1])
        middle_grad, terms_one = block_backward(saved_one, grad_out, sections[1])
        first_grad, terms_zero = block_backward(saved_zero, middle_grad, sections[0])
        totals = jax.tree.map(jnp.add, totals, (terms_zero, terms_one))
        return (totals, (middle, final, first_grad, middle_grad))
    groups = IMAGES // N_DP
    grouped_in = images.reshape(N_DP, groups, PATCHES, D)
    grouped_cot = cotangent.reshape(N_DP, groups, PATCHES, D)
    totals, results = lax.scan(one_group, (zero_terms(), zero_terms()), (grouped_in, grouped_cot))
    middle, final, first_grad, middle_grad = [item.reshape(IMAGES, PATCHES, D) for item in results]
    activations = jnp.stack([middle, final])
    input_grad = jnp.stack([first_grad, middle_grad])

    def both(position):
        return jnp.stack([totals[0][position], totals[1][position]])
    shared = both(6)
    tables = []
    for section_index in range(2):
        bias_total = totals[section_index][7]
        tables.append(jnp.dot(onehot.T, bias_total.transpose(1, 2, 0).reshape(-1, heads), precision=lax.Precision.HIGHEST))
    table_grad = jnp.stack(tables)
    return (activations, input_grad, shared[:, 0], shared[:, 1], both(0), both(4), table_grad, both(1), shared[:, 2], shared[:, 3], shared[:, 4], both(2), both(5), both(3), shared[:, 5])
```

```python
import functools
import math
import types

import jax
import jax.numpy as jnp
import numpy as np
from jax import lax
from jax.experimental import pallas as pl
from jax.experimental.pallas import tpu as pltpu
from jax.sharding import PartitionSpec as P

HEADS = 16
WIN = 7
SIDE = 14
SHIFT = 3

EPS = 1e-05
MASK_FILL = -100.0
ROOT_HALF = 0.7071067811865476
INV_ROOT_TWO_PI = 0.3989422804014327

ACROSS = SIDE // WIN
NW = ACROSS * ACROSS
WT = WIN * WIN
WP = 64
TABLE_SIDE = 2 * WIN - 1
CENTER = (WIN - 1) * TABLE_SIDE + WIN - 1
TABLE_PAD = 256
CH = 512
GATHER_ROWS = 16

SECTION = "section"
DP = "dp"
TENSOR = "tensor"

f32 = jnp.float32
bf16 = jnp.bfloat16
MESH = pl.DeviceIdType.MESH
NN = ((1,), (0,))
NT = ((1,), (1,))
TN = ((0,), (0,))


def round_up(n, m):
    return -(-n // m) * m


def window_slots(shift):
    slot = np.zeros(SIDE * SIDE, np.int64)
    for p in range(SIDE):
        for q in range(SIDE):
            token = ((p + shift) % SIDE) * SIDE + (q + shift) % SIDE
            window = (p // WIN) * ACROSS + q // WIN
            slot[token] = window * WP + (p % WIN) * WIN + q % WIN
    return slot


def window_permutation(parts, half, padded):
    perm = np.zeros((2, NW * WP, parts * padded), np.float32)
    for block in range(2):
        for token, slot in enumerate(window_slots(SHIFT * block)):
            perm[block, slot, (token // half) * padded + token % half] = 1
    return perm


def dotf(a, b, dims):
    return lax.dot_general(a, b, (dims, ((), ())), preferred_element_type=f32)


def normalize(values):
    center = values - jnp.mean(values, -1, keepdims=True)
    inverse = lax.rsqrt(jnp.mean(center * center, -1, keepdims=True) + EPS)
    return center * inverse, inverse


def norm_pull(upstream, normed, inverse, gain):
    scaled = upstream * gain
    return inverse * (
        scaled
        - jnp.mean(scaled, -1, keepdims=True)
        - normed * jnp.mean(scaled * normed, -1, keepdims=True)
    )


def block(i, n):
    if isinstance(i, int):
        return pl.ds(i * n, n)
    return pl.ds(pl.multiple_of(i * n, n), n)


def column_sum(v):
    return jnp.sum(v, 0, keepdims=True)


class Sizes:
    def __init__(self, mesh, images, fc1_weight):
        self.sections = mesh.shape[SECTION]
        self.dp = mesh.shape[DP]
        self.parts = mesh.shape[TENSOR]
        inner = int(math.isqrt(self.dp))
        while self.dp % inner:
            inner -= 1
        self.nb = inner
        self.na = self.dp // inner
        self.local_images, self.half, self.d = images.shape
        self.ff = fc1_weight.shape[-1] * self.parts
        self.ni = self.local_images // (self.sections * self.parts)
        self.hp = round_up(self.half, 8)
        self.rows = self.parts * self.hp
        self.m = self.ni * self.rows
        self.mw = self.ni * NW * WP
        self.hd = self.d // HEADS
        self.quad = 128 // self.hd
        self.ng = HEADS // self.quad
        self.nch = self.ff // CH
        self.scaling = self.hd**-0.5
        self.heads_part = HEADS // self.parts


QKV, PROJ, FC1, FC2, SMALL = range(5)
KINDS = (SMALL, QKV, PROJ, FC1, FC2)


def kernel(z, *refs):
    names = z.names
    r = types.SimpleNamespace(**dict(zip(names, refs)))
    s = lax.axis_index(SECTION)
    d = lax.axis_index(DP)
    t = lax.axis_index(TENSOR)
    na, nb, nt, ns, ni = z.na, z.nb, z.parts, z.sections, z.ni
    a = d // nb
    b = lax.rem(d, nb)
    rows, m = z.rows, z.m

    def dev(s_=None, a_=None, b_=None, t_=None):
        s_ = s if s_ is None else s_
        a_ = a if a_ is None else a_
        b_ = b if b_ is None else b_
        t_ = t if t_ is None else t_
        return (s_, a_ * nb + b_, t_)

    def off(base, k, n):
        return lax.rem(base + k, n)

    x_peers = [off(s, k, ns) for k in range(1, ns)]
    a_peers = [off(a, k, na) for k in range(1, na)]
    a_from = [off(a, na - k, na) for k in range(1, na)]
    b_peers = [off(b, k, nb) for k in range(1, nb)]
    b_from = [off(b, nb - k, nb) for k in range(1, nb)]
    c_peers = [off(t, k, nt) for k in range(1, nt)]
    c_from = [off(t, nt - k, nt) for k in range(1, nt)]
    x_from = [off(s, ns - k, ns) for k in range(1, ns)]

    def part(p, n):
        return pl.ds(pl.multiple_of(p * n, 128), n)

    def win(w, ref, lead, a_, b_, t_):
        if w == QKV:
            return ref.at[lead + (slice(None), a_, b_, slice(None), part(t_, z.d // nt))]
        if w == FC1:
            return ref.at[lead + (a_, b_, slice(None), part(t_, z.ff // nt))]
        return ref.at[lead + (t_, a_, b_)]

    ALL = slice(None)
    wref = {QKV: r.wq, PROJ: r.wp, FC1: r.w1, FC2: r.w2, SMALL: r.sm}
    own = {QKV: r.q_in, PROJ: r.p_in, FC1: r.f1_in, FC2: r.f2_in, SMALL: r.sm_in}
    lx, xs = r.lx, r.xs
    zs, zr, ys, yr, cs, cr = r.zs, r.zr, r.ys, r.yr, r.cs, r.cr

    def remote(src, dst, ss, rs, device):
        return pltpu.make_async_remote_copy(
            src_ref=src, dst_ref=dst, send_sem=ss, recv_sem=rs, device_id=device, device_id_type=MESH
        )

    sends = []

    def send(src, dst, ss, rs, device):
        c = remote(src, dst, ss, rs, device)
        c.start()
        sends.append(c)

    def arrived(dst, sem):
        pltpu.make_async_copy(dst, dst, sem).wait()

    def start_x(w):
        target = win(w, wref[w], (s,), a, b, t)
        pltpu.make_async_copy(own[w], target, lx.at[w, s]).start()
        for k, peer in enumerate(x_peers):
            send(own[w], target, xs.at[w, k], lx.at[w, s], dev(s_=peer))

    def go_z(w, p):
        here = win(w, wref[w], (p,), a, b, t)
        arrived(here, lx.at[w, p])
        for k, peer in enumerate(a_peers):
            send(here, here, zs.at[w, p, k], zr.at[w, p, k], dev(a_=peer))

    def go_y(w, p):
        for k, source in enumerate(a_from):
            arrived(win(w, wref[w], (p,), source, b, t), zr.at[w, p, k])
        here = win(w, wref[w], (p,), ALL, b, t)
        for k, peer in enumerate(b_peers):
            send(here, here, ys.at[w, p, k], yr.at[w, p, k], dev(b_=peer))

    def go_c(w, p):
        for k, source in enumerate(b_from):
            arrived(win(w, wref[w], (p,), ALL, source, t), yr.at[w, p, k])
        here = win(w, wref[w], (p,), ALL, ALL, t)
        for k, peer in enumerate(c_peers):
            send(here, here, cs.at[w, p, k], cr.at[w, p, k], dev(t_=peer))

    def ready(w, p):
        for k, source in enumerate(c_from):
            arrived(win(w, wref[w], (p,), ALL, ALL, source), cr.at[w, p, k])

    group = s * nt + t

    def group_images(g):
        return pl.ds(g * ni, ni)

    barrier = pltpu.get_barrier_semaphore()
    peers = (
        [dev(a_=p) for p in a_peers]
        + [dev(b_=p) for p in b_peers]
        + [dev(t_=p) for p in c_peers]
        + [dev(s_=p) for p in x_peers]
        + [dev(s_=p, t_=q) for p in x_peers for q in c_peers]
    )
    for p in peers:
        pl.semaphore_signal(barrier, inc=1, device_id=p, device_id_type=MESH)
    pl.semaphore_wait(barrier, len(peers))

    for w in KINDS:
        start_x(w)
    tbl = r.tbl
    pltpu.make_async_copy(r.tbl_in, tbl.at[s, t], r.tx.at[s]).start()
    for k, peer in enumerate(x_peers):
        send(r.tbl_in, tbl.at[s, t], r.txs.at[k], r.tx.at[s], dev(s_=peer))
    xin = r.outb
    for j, src in enumerate((r.images, r.cotangent)):
        pltpu.make_async_copy(src.at[group_images(group)], xin.at[j, t], r.xl.at[j]).start()
        for k, peer in enumerate(c_peers):
            send(
                src.at[group_images(s * nt + peer)],
                xin.at[j, t],
                r.xcs.at[j, k],
                r.xcr.at[j, k],
                dev(t_=peer),
            )

    def image_ready(j):
        arrived(xin.at[j, t], r.xl.at[j])
        for k, source in enumerate(c_from):
            arrived(xin.at[j, source], r.xcr.at[j, k])

    pad_rows = jnp.zeros((z.hp - z.half, z.d), f32)

    def load_rows(j, ref):
        def one(i, _):
            pieces = []
            for h in range(nt):
                pieces.append(xin[j, h, i].astype(f32))
                if z.hp > z.half:
                    pieces.append(pad_rows)
            ref[block(i, rows), :] = jnp.concatenate(pieces, 0).astype(bf16)
            return 0

        lax.fori_loop(0, ni, one, 0)

    outb = r.outb

    def ship(kind, p, slot):
        out = r.act if kind == 0 else r.ig
        for h in range(nt):
            target = out.at[group_images(group)]
            mine = jnp.logical_and(s == p, t == h)

            @pl.when(mine)
            def _():
                pltpu.make_async_copy(outb.at[slot, h], target, r.os.at[kind, p, h]).start()

            @pl.when(jnp.logical_not(mine))
            def _():
                remote(
                    outb.at[slot, h], target, r.os.at[kind, p, h], r.orr.at[kind, group], (p, d, h)
                ).start()

    def shipped(kind, p, slot):
        for h in range(nt):
            arrived(outb.at[slot, h], r.os.at[kind, p, h])

    def received(kind):
        out = r.act if kind == 0 else r.ig
        for g in range(ns * nt):

            @pl.when(g != group)
            def _():
                arrived(out.at[group_images(g)], r.orr.at[kind, g])

    def stage_out(value, i, slot):
        for h in range(nt):
            outb[slot, h, i] = value[h * z.hp : h * z.hp + z.half].astype(bf16)

    def w_qkv(p, c):
        return r.wq[p, c].reshape(z.d, z.d)

    def w_proj(p):
        return r.wp[p].reshape(z.d, z.d)

    def w_fc1(p, c):
        return r.w1[p, :, :, :, block(c, CH)].reshape(z.d, CH)

    w2_per = CH // r.w2.shape[-2]
    w2_all = r.w2.reshape(2, z.nch, w2_per, r.w2.shape[-2], z.d)

    def w_fc2(p, c):
        return w2_all[p, c].reshape(CH, z.d)

    SMF = r.smf

    def unpack_small(p):
        acc = jnp.zeros((GATHER_ROWS, z.d), f32)
        for t_ in range(nt):
            for a_ in range(na):
                for b_ in range(nb):
                    acc = acc + r.sm[p, t_, a_, b_].astype(f32)
        SMF[p] = acc

    def row(p, k):
        return SMF[p, pl.ds(k, 1), :]

    def masks(dtype):
        lane = lax.broadcasted_iota(jnp.int32, (WP, 128), 1) // z.hd
        return [(lane == h).astype(dtype) for h in range(z.quad)]

    def spread(v, mk):
        return jnp.concatenate([v * q for q in mk], 0)

    def collect(v, mk):
        acc = v[0:WP] * mk[0]
        for h in range(1, z.quad):
            acc = acc + v[h * WP : (h + 1) * WP] * mk[h]
        return acc

    BM = r.bm
    lanes = 128
    per_lane = lanes // WP

    def build_bias(p):
        j = lax.broadcasted_iota(jnp.int32, (WP, lanes), 0)
        lane = lax.broadcasted_iota(jnp.int32, (WP, lanes), 1)
        i = lax.rem(lane, WP)
        iy, ix, jy, jx = i // WIN, lax.rem(i, WIN), j // WIN, lax.rem(j, WIN)
        valid = jnp.logical_and(i < WT, j < WT)
        index = (iy - jy + WIN - 1) * TABLE_SIDE + ix - jx + WIN - 1
        index = jnp.where(valid, index, 0)
        low = jnp.where(index < lanes, index, 0)
        high = jnp.where(index < lanes, 0, index - lanes)
        head_of_lane = lane // WP

        def look(head):
            tt, hh = head // z.heads_part, head % z.heads_part
            entry = tbl[p, tt, pl.ds(hh, 1), :]
            one = jnp.take_along_axis(jnp.broadcast_to(entry[:, :lanes], (WP, lanes)), low, axis=1)
            two = jnp.take_along_axis(jnp.broadcast_to(entry[:, lanes:], (WP, lanes)), high, axis=1)
            return jnp.where(index < lanes, one, two)

        def region(q, wy):
            first = jnp.zeros_like(q)
            if wy < ACROSS - 1:
                return first
            return jnp.where(q < WIN - SHIFT, first + 1, first + 2)

        for g in range(z.ng):
            for c in range(z.quad // per_lane):
                value = look(g * z.quad + c * per_lane)
                for e in range(1, per_lane):
                    value = jnp.where(head_of_lane == e, look(g * z.quad + c * per_lane + e), value)
                value = jnp.where(j < WT, value, -1e30)
                for w in range(NW if p else 1):
                    out = value
                    if p == 1:
                        wy, wx = w // ACROSS, w % ACROSS
                        label_i = region(iy, wy) * 3 + region(ix, wx)
                        label_j = region(jy, wy) * 3 + region(jx, wx)
                        out = out + jnp.where(
                            jnp.logical_and(valid, label_i != label_j), MASK_FILL, 0.0
                        )
                    BM[p + w, g, :, c * lanes : (c + 1) * lanes] = out

    X, G = r.x, r.g
    PM, PMT = r.pm, r.pmt
    FN, N1, K = r.fn, r.n1, r.k
    QK, PR, CTX, CTXT = r.qk, r.pr, r.ctx, r.ctxt
    MID, MG, SN, N2, ACT, SL = r.mid, r.mg, r.sn, r.n2, r.actv, r.sl
    SG, DB = r.sg, r.db

    def forward(p, hook):
        def ln1(i, _):
            n, inv = normalize(X[block(i, rows), :].astype(f32))
            N1[p, block(i, rows), :] = n.astype(bf16)
            K[block(i, rows), 2 * p : 2 * p + 1] = inv
            f = (n * row(p, 0) + row(p, 1)).astype(bf16)
            FN[p, block(i, rows), :] = f
            CTX[block(i, NW * WP), :] = dotf(PM[p], f, NN).astype(bf16)
            return 0

        hook("ln1")
        lax.fori_loop(0, ni, ln1, 0)
        hook("qkv")

        def qkv(c, _):
            QK[p, c] = (dotf(CTX[...], w_qkv(p, c), NN) + row(p, 6 + c)).astype(bf16)
            return 0

        lax.fori_loop(0, 3, qkv, 0)

        def attention(u, _):
            mb, mf = masks(bf16), masks(f32)
            w = 1 + lax.rem(u, NW) if p else 0
            for g in range(z.ng):
                L = slice(g * 128, (g + 1) * 128)
                q = QK[p, 0, block(u, WP), L]
                k = QK[p, 1, block(u, WP), L]
                v = QK[p, 2, block(u, WP), L]
                sc = dotf(k, spread(q, mb), NT) * z.scaling + BM[w, g]
                e = jnp.exp(sc - jnp.max(sc, 0, keepdims=True))
                pr = (e * (1.0 / jnp.sum(e, 0, keepdims=True))).astype(bf16)
                PR[p, u, g] = pr
                CTX[block(u, WP), L] = collect(dotf(pr, v, TN), mf).astype(bf16)
            return 0

        steps = ni * NW
        hook("attn0")
        lax.fori_loop(0, steps // 2, attention, 0)
        hook("attn1")
        lax.fori_loop(steps // 2, steps, attention, 0)

        def unperm(i, _):
            CTXT[p, block(i, rows), :] = dotf(PMT[p], CTX[block(i, NW * WP), :], NN).astype(bf16)
            return 0

        lax.fori_loop(0, ni, unperm, 0)
        hook("proj")
        MID[...] = dotf(CTXT[p], w_proj(p), NN)

        def ln2(i, _):
            mid = X[block(i, rows), :].astype(f32) + MID[block(i, rows), :] + row(p, 2)
            MID[block(i, rows), :] = mid
            n, inv = normalize(mid)
            N2[p, block(i, rows), :] = n.astype(bf16)
            K[block(i, rows), 2 * p + 1 : 2 * p + 2] = inv
            SN[p, block(i, rows), :] = (n * row(p, 3) + row(p, 4)).astype(bf16)
            return 0

        lax.fori_loop(0, ni, ln2, 0)
        hook("fc1")

        def rise(c, _):
            u = dotf(SN[p], w_fc1(p, c), NN) + row(p, 9 + c)
            e = 0.5 * (1.0 + lax.erf(u * ROOT_HALF))
            ACT[c] = (u * e).astype(bf16)
            SL[c] = (e + u * jnp.exp(-0.5 * u * u) * INV_ROOT_TWO_PI).astype(bf16)
            return 0

        lax.fori_loop(0, z.nch, rise, 0)
        hook("fc2")

        def fall(c, _):
            MID[...] += dotf(ACT[c], w_fc2(p, c), NN)
            return 0

        lax.fori_loop(0, z.nch, fall, 0)
        hook("out")

        def finish(i, _):
            value = MID[block(i, rows), :] + row(p, 5)
            X[block(i, rows), :] = value.astype(bf16)
            stage_out(value, i, p % 2)
            return 0

        lax.fori_loop(0, ni, finish, 0)
        ship(0, p, p % 2)

    gq, gp, g1, g2 = r.gq, r.gp, r.g1, r.g2
    g2_all = g2.reshape(z.nch, w2_per, g2.shape[-2], z.d)

    def backward(p, hook):
        def addrow(k, v):
            SG[p, pl.ds(k, 1), 0 : z.d] = SG[p, pl.ds(k, 1), 0 : z.d] + v

        SG[p] = jnp.zeros(SG.shape[1:], f32)
        DB[...] = jnp.zeros(DB.shape, f32)

        hook("fc2")

        def fc2(c, _):
            g2_all[c] = dotf(ACT[c], G[...], TN).astype(bf16).reshape(g2_all.shape[1:])
            hg = dotf(G[...], w_fc2(p, c), NT) * SL[c].astype(f32)
            SG[p, pl.ds(9 + c, 1), 0 : z.d] = column_sum(hg)
            SL[c] = hg.astype(bf16)
            return 0

        lax.fori_loop(0, z.nch, fc2, 0)
        hook("fc1")

        def fc1(c, _):
            g1[:, :, :, block(c, CH)] = (
                dotf(SN[p], SL[c], TN).astype(bf16).reshape(g1.shape[:-1] + (CH,))
            )
            return 0

        lax.fori_loop(0, z.nch, fc1, 0)
        hook("n2g")
        MID[...] = dotf(SL[0], w_fc1(p, 0), NT)

        def n2g(c, _):
            MID[...] += dotf(SL[c], w_fc1(p, c), NT)
            return 0

        lax.fori_loop(1, z.nch, n2g, 0)

        def ln2(i, _):
            sl = block(i, rows)
            ng = MID[sl, :]
            n = N2[p, sl, :].astype(f32)
            g = G[sl, :].astype(f32)
            mg = g + norm_pull(ng, n, K[sl, 2 * p + 1 : 2 * p + 2], row(p, 3))
            MG[sl, :] = mg
            addrow(5, column_sum(g))
            addrow(3, column_sum(ng * n))
            addrow(4, column_sum(ng))
            addrow(2, column_sum(mg))
            G[sl, :] = mg.astype(bf16)
            return 0

        lax.fori_loop(0, ni, ln2, 0)
        hook("proj")
        gp[...] = dotf(CTXT[p], G[...], TN).astype(bf16).reshape(gp.shape)
        CTXT[p] = dotf(G[...], w_proj(p), NT).astype(bf16)

        def cgrad(i, _):
            CTX[block(i, NW * WP), :] = dotf(PM[p], CTXT[p, block(i, rows), :], NN).astype(bf16)
            return 0

        lax.fori_loop(0, ni, cgrad, 0)

        def attention(u, _):
            mb, mf = masks(bf16), masks(f32)
            for g in range(z.ng):
                L = slice(g * 128, (g + 1) * 128)
                q = QK[p, 0, block(u, WP), L]
                k = QK[p, 1, block(u, WP), L]
                v = QK[p, 2, block(u, WP), L]
                pr = PR[p, u, g]
                cbd = spread(CTX[block(u, WP), L], mb)
                qbd = spread(q, mb)
                pf = pr.astype(f32)
                tt = pf * dotf(v, cbd, NT)
                sc = tt - pf * jnp.sum(tt, 0, keepdims=True)
                DB[g] = DB[g] + sc
                sb = sc.astype(bf16)
                QK[p, 1, block(u, WP), L] = (dotf(sb, qbd, NN) * z.scaling).astype(bf16)
                QK[p, 2, block(u, WP), L] = dotf(pr, cbd, NN).astype(bf16)
                QK[p, 0, block(u, WP), L] = (collect(dotf(sb, k, TN), mf) * z.scaling).astype(bf16)
            return 0

        steps = ni * NW
        hook("attn0")
        lax.fori_loop(0, steps // 2, attention, 0)
        hook("attn1")
        lax.fori_loop(steps // 2, steps, attention, 0)
        hook("qkv")
        for c in range(3):

            def un(i, _):
                dv = dotf(PMT[p], QK[p, c, block(i, NW * WP), :], NN)
                addrow(6 + c, column_sum(dv))
                QK[p, c, block(i, rows), :] = dv.astype(bf16)
                return 0

            lax.fori_loop(0, ni, un, 0)
            gq[c] = dotf(FN[p], QK[p, c, 0:m, :], TN).astype(bf16).reshape(gq.shape[1:])
        hook("qkv_done")
        for c in range(3):
            v = dotf(QK[p, c, 0:m, :], w_qkv(p, c), NT)
            MID[...] = v if c == 0 else MID[...] + v
        hook("ln1")

        def ln1(i, _):
            sl = block(i, rows)
            ng = MID[sl, :]
            n = N1[p, sl, :].astype(f32)
            xg = MG[sl, :] + norm_pull(ng, n, K[sl, 2 * p : 2 * p + 1], row(p, 0))
            addrow(0, column_sum(ng * n))
            addrow(1, column_sum(ng))
            G[sl, :] = xg.astype(bf16)
            stage_out(xg, i, 1 - p)
            return 0

        lax.fori_loop(0, ni, ln1, 0)
        ship(1, p, 1 - p)
        table_rows(p)

    def table_rows(p):
        src = lax.broadcasted_iota(jnp.int32, (z.quad * WP, TABLE_PAD), 0)
        dst = lax.broadcasted_iota(jnp.int32, (z.quad * WP, TABLE_PAD), 1)
        i = lax.rem(src, WP)
        place = jnp.logical_and(
            i < WT, dst == CENTER - ((i // WIN) * TABLE_SIDE + lax.rem(i, WIN))
        )
        head = src // WP
        j = lax.broadcasted_iota(jnp.int32, (WP, TABLE_PAD), 0)
        jy = j // WIN
        step = TABLE_SIDE - WIN
        for h in range(z.quad):
            pick = jnp.logical_and(place, head == h).astype(bf16)
            for g in range(z.ng):
                v = DB[g]
                hi = v.astype(bf16)
                lo = (v - hi.astype(f32)).astype(bf16)
                e = dotf(hi, pick, NN) + dotf(lo, pick, NN)
                e = pltpu.roll(e, 0, 1, stride=1, stride_axis=0)
                for bit in (1, 2, 4):
                    moved = pltpu.roll(e, step * bit, 1)
                    e = jnp.where(lax.rem(jy // bit, 2) == 1, moved, e)
                e = jnp.where(j < WT, e, 0.0)
                SG[p, pl.ds(g * z.quad + h, 1), z.d :] = column_sum(e)

    gref = {QKV: gq, PROJ: gp, FC1: g1, FC2: g2}
    rx1 = {QKV: r.q1, PROJ: r.p1, FC1: r.f11, FC2: r.f21}
    rx2 = {QKV: r.q2, PROJ: r.p2, FC1: r.f12, FC2: r.f22}
    rx3 = {QKV: r.q3, PROJ: r.p3, FC1: r.f13, FC2: r.f23}
    rx4 = {QKV: r.q4, PROJ: r.p4, FC1: r.f14, FC2: r.f24}
    gout = {QKV: r.gq_out, PROJ: r.gp_out, FC1: r.g1_out, FC2: r.g2_out}
    s1, v1, s2, v2, s3, v3, s4, v4 = (r.s1, r.v1, r.s2, r.v2, r.s3, r.v3, r.s4, r.v4)
    k1, k2, k3 = r.k1, r.k2, r.k3

    def credit(sem, w, k, p, device):
        if p == 1:
            pl.semaphore_signal(sem.at[w, k], inc=1, device_id=device, device_id_type=MESH)

    def spend(sem, w, k, p):
        if p == 0:
            pl.semaphore_wait(sem.at[w, k], 1)

    def r1(w, p):
        for k, peer in enumerate(c_peers):
            spend(k1, w, k, p)
            remote(
                win(w, gref[w], (), ALL, ALL, peer), rx1[w].at[k], s1.at[w, k], v1.at[w, k], dev(t_=peer)
            ).start()

    def r2(w, p):
        mine = win(w, gref[w], (), ALL, ALL, t)
        for k, source in enumerate(c_from):
            arrived(rx1[w].at[k], v1.at[w, k])
        add_into(w, mine, [rx1[w].at[k] for k in range(nt - 1)])
        for k, source in enumerate(c_from):
            credit(k1, w, k, p, dev(t_=source))
        for k, peer in enumerate(b_peers):
            spend(k2, w, k, p)
            remote(
                win(w, gref[w], (), ALL, peer, t), rx2[w].at[k], s2.at[w, k], v2.at[w, k], dev(b_=peer)
            ).start()

    def r3(w, p):
        mine = win(w, gref[w], (), ALL, b, t)
        for k, source in enumerate(b_from):
            arrived(rx2[w].at[k], v2.at[w, k])
        add_into(w, mine, [rx2[w].at[k] for k in range(nb - 1)])
        for k, source in enumerate(b_from):
            credit(k2, w, k, p, dev(b_=source))
        for k, peer in enumerate(a_peers):
            spend(k3, w, k, p)
            remote(
                win(w, gref[w], (), peer, b, t), rx3[w].at[k], s3.at[w, k], v3.at[w, k], dev(a_=peer)
            ).start()

    def r4(w, p):
        mine = win(w, gref[w], (), a, b, t)
        for k, source in enumerate(a_from):
            arrived(rx3[w].at[k], v3.at[w, k])
        total = mine[...].astype(f32)
        for k in range(na - 1):
            total = total + rx3[w][k].astype(f32)
        for k, source in enumerate(a_from):
            credit(k3, w, k, p, dev(a_=source))

        @pl.when(s == p)
        def _():
            gout[w][...] = total

        @pl.when(s != p)
        def _():
            mine[...] = total.astype(bf16)
            remote(mine, rx4[w], s4.at[w], v4.at[w], dev(s_=p)).start()

    def r5(w, p):
        @pl.when(s == p)
        def _():
            arrived(rx4[w], v4.at[w])
            gout[w][...] = gout[w][...] + rx4[w][...].astype(f32)

        @pl.when(s != p)
        def _():
            arrived(win(w, gref[w], (), a, b, t), s4.at[w])

        for k, peer in enumerate(c_peers):
            arrived(win(w, gref[w], (), ALL, ALL, peer), s1.at[w, k])
        for k, peer in enumerate(b_peers):
            arrived(win(w, gref[w], (), ALL, peer, t), s2.at[w, k])
        for k, peer in enumerate(a_peers):
            arrived(win(w, gref[w], (), peer, b, t), s3.at[w, k])

    def add_into(w, mine, others):
        lead = mine.shape[:-2]
        count = int(np.prod(lead))

        def one(i, _):
            index = []
            rest = i
            for extent in reversed(lead):
                index.append(lax.rem(rest, extent))
                rest = rest // extent
            index = tuple(reversed(index))
            total = mine[index].astype(f32)
            for o in others:
                total = total + o[index].astype(f32)
            mine[index] = total.astype(bf16)
            return 0

        lax.fori_loop(0, count, one, 0)

    for w in KINDS:
        go_z(w, 0)
    for q in range(ns):
        arrived(tbl.at[q, t], r.tx.at[q])
        for k, peer in enumerate(c_peers):
            send(tbl.at[q, t], tbl.at[q, t], r.tcs.at[q, k], r.tcr.at[q, k], dev(t_=peer))
    image_ready(0)
    load_rows(0, X)
    for q in range(ns):
        for k, source in enumerate(c_from):
            arrived(tbl.at[q, source], r.tcr.at[q, k])
    for p in range(2):
        build_bias(p)
    for w in (SMALL, QKV):
        go_y(w, 0)
    for w in (SMALL, QKV):
        go_c(w, 0)
    image_ready(1)
    load_rows(1, G)

    def forward_hook(p, name):
        if p == 0:
            if name == "ln1":
                ready(SMALL, 0)
                unpack_small(0)
                go_z(SMALL, 1)
            if name == "qkv":
                ready(QKV, 0)
            if name == "attn0":
                go_y(PROJ, 0)
                go_y(FC1, 0)
                go_c(PROJ, 0)
            if name == "attn1":
                go_c(FC1, 0)
                go_y(FC2, 0)
                for w in (QKV, PROJ, FC1, FC2):
                    go_z(w, 1)
            if name == "proj":
                ready(PROJ, 0)
                go_c(FC2, 0)
                go_y(SMALL, 1)
                go_c(SMALL, 1)
            if name == "fc1":
                ready(FC1, 0)
            if name == "fc2":
                go_y(QKV, 1)
                ready(FC2, 0)
            if name == "out":
                go_c(QKV, 1)
                for j, ref in enumerate((ACT, SL)):
                    pltpu.make_async_copy(ref, r.spill.at[j], r.sp.at[j]).start()
        else:
            if name == "ln1":
                ready(SMALL, 1)
                unpack_small(1)
            if name == "qkv":
                ready(QKV, 1)
                go_y(PROJ, 1)
            if name == "attn0":
                go_c(PROJ, 1)
                go_y(FC1, 1)
            if name == "attn1":
                go_c(FC1, 1)
                go_y(FC2, 1)
            if name == "proj":
                ready(PROJ, 1)
                go_c(FC2, 1)
            if name == "fc1":
                for j, ref in enumerate((ACT, SL)):
                    arrived(ref, r.sp.at[j])
                ready(FC1, 1)
            if name == "fc2":
                ready(FC2, 1)

    for p in range(2):
        forward(p, functools.partial(forward_hook, p))

    def backward_hook(p, name):
        if p == 1:
            if name == "fc2":
                shipped(0, 0, 0)
            if name == "fc1":
                r1(FC2, 1)
            if name == "n2g":
                r1(FC1, 1)
                r2(FC2, 1)
            if name == "proj":
                for j, ref in enumerate((ACT, SL)):
                    pltpu.make_async_copy(r.spill.at[j], ref, r.sp.at[j]).start()
            if name == "attn0":
                r1(PROJ, 1)
                r2(FC1, 1)
            if name == "attn1":
                r3(FC2, 1)
                r2(PROJ, 1)
            if name == "qkv":
                r3(FC1, 1)
                r3(PROJ, 1)
                r4(FC2, 1)
            if name == "qkv_done":
                r1(QKV, 1)
                r4(FC1, 1)
                r4(PROJ, 1)
            if name == "ln1":
                r2(QKV, 1)
                r5(FC2, 1)
                r5(FC1, 1)
        else:
            if name == "fc2":
                shipped(0, 1, 1)
                for j, ref in enumerate((ACT, SL)):
                    arrived(ref, r.sp.at[j])
            if name == "fc1":
                r1(FC2, 0)
                r3(QKV, 1)
                r5(PROJ, 1)
            if name == "n2g":
                r1(FC1, 0)
                r2(FC2, 0)
                r4(QKV, 1)
            if name == "attn0":
                r1(PROJ, 0)
                r2(FC1, 0)
                r5(QKV, 1)
            if name == "attn1":
                r3(FC2, 0)
                r2(PROJ, 0)
            if name == "qkv":
                r3(FC1, 0)
                r3(PROJ, 0)
                r4(FC2, 0)
            if name == "qkv_done":
                r1(QKV, 0)
                r4(FC1, 0)
                r4(PROJ, 0)
            if name == "ln1":
                r2(QKV, 0)
                r5(FC2, 0)
                r5(FC1, 0)
                r5(PROJ, 0)

    for p in (1, 0):
        backward(p, functools.partial(backward_hook, p))

    ra, rb, rc, rd = r.ra, r.rb, r.rc, r.rd
    ss, sv = r.ss, r.sv
    slots = iter(range(16))

    def exchange(src, dst, targets, sources):
        ids = [next(slots) for _ in targets]
        for k, target in enumerate(targets):
            send(src(k), dst.at[k], ss.at[ids[k]], sv.at[ids[k]], target)
        for k in range(len(sources)):
            arrived(dst.at[k], sv.at[ids[k]])

    exchange(lambda k: SG, ra, [dev(t_=p) for p in c_peers], c_from)
    r.sum1[...] = SG[...] + sum(ra[k] for k in range(nt - 1))
    r3(QKV, 0)
    exchange(lambda k: r.sum1.at[x_peers[k]], rb, [dev(s_=p) for p in x_peers], x_from)
    r.sum2[...] = r.sum1[s] + sum(rb[k] for k in range(ns - 1))
    exchange(lambda k: r.sum2, rc, [dev(b_=p) for p in b_peers], b_from)
    r.sum3[...] = r.sum2[...] + sum(rc[k] for k in range(nb - 1))
    exchange(lambda k: r.sum3, rd, [dev(a_=p) for p in a_peers], a_from)
    r4(QKV, 0)
    r.small_out[...] = r.sum3[...] + sum(rd[k] for k in range(na - 1))
    r5(QKV, 0)

    received(0)
    received(1)
    shipped(1, 1, 0)
    shipped(1, 0, 1)
    for c in sends:
        c.wait_send()


def per_device(z, images, cotangent, norm1_gain, norm1_bias, qkv_weight, qkv_bias, position_table,
               proj_weight, proj_bias, norm2_gain, norm2_bias, fc1_weight, fc1_bias, fc2_weight,
               fc2_bias):
    s = lax.axis_index(SECTION)
    d = lax.axis_index(DP)
    t = lax.axis_index(TENSOR)
    D, nt, na, nb, ns, ni = z.d, z.parts, z.na, z.nb, z.sections, z.ni
    part = t * z.dp + d

    def spread_to(values, width, at):
        blank = jnp.zeros((values.shape[0], width), bf16)
        return lax.dynamic_update_slice(blank, values, (0, at))

    vectors = jnp.concatenate(
        [norm1_gain, norm1_bias, proj_bias, norm2_gain, norm2_bias, fc2_bias], 0
    )
    vectors = jnp.where(t == 0, vectors, jnp.zeros_like(vectors))
    small = jnp.concatenate(
        [
            spread_to(vectors, D, d * vectors.shape[1]),
            spread_to(qkv_bias[0], D, part * qkv_bias.shape[-1]),
            spread_to(fc1_bias, z.ff, part * fc1_bias.shape[-1]).reshape(-1, D),
        ],
        0,
    )
    small = jnp.pad(small, ((0, GATHER_ROWS - small.shape[0]), (0, 0)))
    table = jnp.pad(position_table[0].T, ((0, 0), (0, TABLE_PAD - position_table.shape[1])))
    perm = window_permutation(nt, z.half, z.hp)

    qrow, prow, f2row = qkv_weight.shape[1], proj_weight.shape[1], fc2_weight.shape[1]
    m, mw, nch = z.m, z.mw, z.nch
    S = jax.ShapeDtypeStruct
    V = pl.BlockSpec(memory_space=pltpu.VMEM)
    A = pl.BlockSpec(memory_space=pl.ANY)
    dma = pltpu.SemaphoreType.DMA
    reg = pltpu.SemaphoreType.REGULAR
    inputs = dict(
        images=(images, A),
        cotangent=(cotangent, A),
        q_in=(qkv_weight[0].transpose(1, 0, 2), A),
        p_in=(proj_weight[0], A),
        f1_in=(fc1_weight[0], A),
        f2_in=(fc2_weight[0], A),
        sm_in=(small, V),
        tbl_in=(table, V),
        pm=(jnp.asarray(perm, bf16), V),
        pmt=(jnp.asarray(perm.transpose(0, 2, 1), bf16), V),
    )
    wide = D + TABLE_PAD
    outputs = dict(
        act=(S(images.shape, bf16), A),
        ig=(S(images.shape, bf16), A),
        gq_out=(S((3, qrow, D // nt), f32), V),
        gp_out=(S((prow, D), f32), V),
        g1_out=(S((qrow, z.ff // nt), f32), V),
        g2_out=(S((f2row, D), f32), V),
        small_out=(S((GATHER_ROWS, wide), f32), V),
        spill=(S((2, nch, m, CH), bf16), A),
    )
    vm = pltpu.VMEM
    W = 5
    scratch = dict(
        wq=vm((2, 3, na, nb, qrow, D), bf16),
        wp=vm((2, nt, na, nb, prow, D), bf16),
        w1=vm((2, na, nb, qrow, z.ff), bf16),
        w2=vm((2, nt, na, nb, f2row, D), bf16),
        sm=vm((2, nt, na, nb, GATHER_ROWS, D), bf16),
        smf=vm((2, GATHER_ROWS, D), f32),
        tbl=vm((2, nt, z.heads_part, TABLE_PAD), f32),
        outb=vm((2, nt, ni, z.half, D), bf16),
        bm=vm((1 + NW, z.ng, WP, z.quad * WP), f32),
        x=vm((m, D), bf16),
        g=vm((m, D), bf16),
        fn=vm((2, m, D), bf16),
        n1=vm((2, m, D), bf16),
        k=vm((m, 4), f32),
        qk=vm((2, 3, mw, D), bf16),
        pr=vm((2, ni * NW, z.ng, WP, z.quad * WP), bf16),
        ctx=vm((mw, D), bf16),
        ctxt=vm((2, m, D), bf16),
        mid=vm((m, D), f32),
        mg=vm((m, D), f32),
        sn=vm((2, m, D), bf16),
        n2=vm((2, m, D), bf16),
        actv=vm((nch, m, CH), bf16),
        sl=vm((nch, m, CH), bf16),
        sg=vm((2, GATHER_ROWS, wide), f32),
        db=vm((z.ng, WP, z.quad * WP), f32),
        gq=vm((3, na, nb, qrow, D), bf16),
        gp=vm((nt, na, nb, prow, D), bf16),
        g1=vm((na, nb, qrow, z.ff), bf16),
        g2=vm((nt, na, nb, f2row, D), bf16),
        q1=vm((nt - 1, 3, na, nb, qrow, D // nt), bf16),
        p1=vm((nt - 1, na, nb, prow, D), bf16),
        f11=vm((nt - 1, na, nb, qrow, z.ff // nt), bf16),
        f21=vm((nt - 1, na, nb, f2row, D), bf16),
        q2=vm((nb - 1, 3, na, qrow, D // nt), bf16),
        p2=vm((nb - 1, na, prow, D), bf16),
        f12=vm((nb - 1, na, qrow, z.ff // nt), bf16),
        f22=vm((nb - 1, na, f2row, D), bf16),
        q3=vm((na - 1, 3, qrow, D // nt), bf16),
        p3=vm((na - 1, prow, D), bf16),
        f13=vm((na - 1, qrow, z.ff // nt), bf16),
        f23=vm((na - 1, f2row, D), bf16),
        q4=vm((3, qrow, D // nt), bf16),
        p4=vm((prow, D), bf16),
        f14=vm((qrow, z.ff // nt), bf16),
        f24=vm((f2row, D), bf16),
        ra=vm((nt - 1, 2, GATHER_ROWS, wide), f32),
        rb=vm((ns - 1, GATHER_ROWS, wide), f32),
        rc=vm((nb - 1, GATHER_ROWS, wide), f32),
        rd=vm((na - 1, GATHER_ROWS, wide), f32),
        sum1=vm((2, GATHER_ROWS, wide), f32),
        sum2=vm((GATHER_ROWS, wide), f32),
        sum3=vm((GATHER_ROWS, wide), f32),
        lx=dma((W, ns)),
        xs=dma((W, ns - 1)),
        zs=dma((W, 2, na - 1)),
        zr=dma((W, 2, na - 1)),
        ys=dma((W, 2, nb - 1)),
        yr=dma((W, 2, nb - 1)),
        cs=dma((W, 2, nt - 1)),
        cr=dma((W, 2, nt - 1)),
        tx=dma((ns,)),
        txs=dma((ns - 1,)),
        tcs=dma((ns, nt - 1)),
        tcr=dma((ns, nt - 1)),
        xl=dma((2,)),
        xcs=dma((2, nt - 1)),
        xcr=dma((2, nt - 1)),
        os=dma((2, 2, nt)),
        orr=dma((2, ns * nt)),
        sp=dma((2,)),
        s1=dma((4, nt - 1)),
        v1=dma((4, nt - 1)),
        s2=dma((4, nb - 1)),
        v2=dma((4, nb - 1)),
        s3=dma((4, na - 1)),
        v3=dma((4, na - 1)),
        s4=dma((4,)),
        v4=dma((4,)),
        k1=reg((4, nt - 1)),
        k2=reg((4, nb - 1)),
        k3=reg((4, na - 1)),
        ss=dma((16,)),
        sv=dma((16,)),
    )
    z.names = list(inputs) + list(outputs) + list(scratch)
    results = pl.pallas_call(
        functools.partial(kernel, z),
        out_shape=tuple(o for o, _ in outputs.values()),
        in_specs=[spec for _, spec in inputs.values()],
        out_specs=tuple(spec for _, spec in outputs.values()),
        scratch_shapes=list(scratch.values()),
        compiler_params=pltpu.CompilerParams(
            collective_id=0, has_side_effects=True, vmem_limit_bytes=67043328
        ),
        name="two_blocks",
    )(*[x for x, _ in inputs.values()])
    act, ig, gq, gp, g1, g2, sums, _ = results

    def own_vector(k):
        width = norm1_gain.shape[1]
        return lax.dynamic_slice(sums, (k, d * width), (1, width))

    width = qkv_bias.shape[-1]
    qkv_bias_grad = lax.dynamic_slice(sums, (6, part * width), (3, width))[None]
    width = fc1_bias.shape[1]
    fc1_flat = sums[9 : 9 + nch, :D].reshape(1, -1)
    fc1_bias_grad = lax.dynamic_slice(fc1_flat, (0, part * width), (1, width))
    tables = lax.dynamic_slice(sums, (t * z.heads_part, D), (z.heads_part, TABLE_PAD))
    tables = tables[:, : position_table.shape[1]][:, ::-1].T[None]
    return (
        act[None],
        ig[None],
        own_vector(0),
        own_vector(1),
        gq.transpose(1, 0, 2)[None],
        qkv_bias_grad,
        tables,
        gp[None],
        own_vector(2),
        own_vector(3),
        own_vector(4),
        g1[None],
        fc1_bias_grad,
        g2[None],
        own_vector(5),
    )


def solution(mesh):
    def run(*args):
        z = Sizes(mesh, args[0], args[11])
        return per_device(z, *args)

    in_specs = (
        P(DP, TENSOR, None),
        P(DP, TENSOR, None),
        P(SECTION, DP),
        P(SECTION, DP),
        P(SECTION, DP, None, TENSOR),
        P(SECTION, None, (TENSOR, DP)),
        P(SECTION, None, TENSOR),
        P(SECTION, (TENSOR, DP), None),
        P(SECTION, DP),
        P(SECTION, DP),
        P(SECTION, DP),
        P(SECTION, DP, TENSOR),
        P(SECTION, (TENSOR, DP)),
        P(SECTION, (TENSOR, DP), None),
        P(SECTION, DP),
    )
    out_specs = (
        P(SECTION, DP, TENSOR, None),
        P(SECTION, DP, TENSOR, None),
        P(SECTION, DP),
        P(SECTION, DP),
        P(SECTION, DP, None, TENSOR),
        P(SECTION, None, (TENSOR, DP)),
        P(SECTION, None, TENSOR),
        P(SECTION, (TENSOR, DP), None),
        P(SECTION, DP),
        P(SECTION, DP),
        P(SECTION, DP),
        P(SECTION, DP, TENSOR),
        P(SECTION, (TENSOR, DP)),
        P(SECTION, (TENSOR, DP), None),
        P(SECTION, DP),
    )
    return jax.shard_map(
        run, mesh=mesh, in_specs=in_specs, out_specs=out_specs, check_vma=False
    )
```

```python
import functools
import heapq
import math
import types

import jax
import jax.numpy as jnp
import numpy as np
from jax import lax
from jax.experimental import pallas as pl
from jax.experimental.pallas import tpu as pltpu
from jax.sharding import PartitionSpec as P

HEADS = 16
WIN = 7
SIDE = 14
SHIFT = 3

EPS = 1e-05
MASK_FILL = -100.0
ROOT_HALF = 0.7071067811865476
INV_ROOT_TWO_PI = 0.3989422804014327

ACROSS = SIDE // WIN
NW = ACROSS * ACROSS
WT = WIN * WIN
WP = 64
TABLE_SIDE = 2 * WIN - 1
CENTER = (WIN - 1) * TABLE_SIDE + WIN - 1
TABLE_PAD = 256
CH = 512
GATHER_ROWS = 16
BATCH = 2

SECTION = "section"
DP = "dp"
TENSOR = "tensor"

f32 = jnp.float32
bf16 = jnp.bfloat16
MESH = pl.DeviceIdType.MESH
NN = ((1,), (0,))
NT = ((1,), (1,))
TN = ((0,), (0,))


def round_up(n, m):
    return -(-n // m) * m


def window_slots(shift):
    slot = np.zeros(SIDE * SIDE, np.int64)
    for p in range(SIDE):
        for q in range(SIDE):
            token = ((p + shift) % SIDE) * SIDE + (q + shift) % SIDE
            window = (p // WIN) * ACROSS + q // WIN
            slot[token] = window * WP + (p % WIN) * WIN + q % WIN
    return slot


def window_permutation(parts, half, padded):
    perm = np.zeros((2, NW * WP, parts * padded), np.float32)
    for block in range(2):
        for token, slot in enumerate(window_slots(SHIFT * block)):
            perm[block, slot, (token // half) * padded + token % half] = 1
    return perm


def dotf(a, b, dims):
    return lax.dot_general(a, b, (dims, ((), ())), preferred_element_type=f32)


def normalize(values):
    center = values - jnp.mean(values, -1, keepdims=True)
    inverse = lax.rsqrt(jnp.mean(center * center, -1, keepdims=True) + EPS)
    return center * inverse, inverse


def norm_pull(upstream, normed, inverse, gain):
    scaled = upstream * gain
    return inverse * (
        scaled
        - jnp.mean(scaled, -1, keepdims=True)
        - normed * jnp.mean(scaled * normed, -1, keepdims=True)
    )


def block(i, n):
    if isinstance(i, int):
        return pl.ds(i * n, n)
    return pl.ds(pl.multiple_of(i * n, n), n)


def column_sum(v):
    return jnp.sum(v, 0, keepdims=True)


class Sizes:
    def __init__(self, mesh, images, fc1_weight):
        self.sections = mesh.shape[SECTION]
        self.dp = mesh.shape[DP]
        self.parts = mesh.shape[TENSOR]
        inner = int(math.isqrt(self.dp))
        while self.dp % inner:
            inner -= 1
        self.nb = inner
        self.na = self.dp // inner
        self.local_images, self.half, self.d = images.shape
        self.ff = fc1_weight.shape[-1] * self.parts
        self.ni = self.local_images // (self.sections * self.parts)
        self.hp = round_up(self.half, 8)
        self.rows = self.parts * self.hp
        self.m = self.ni * self.rows
        self.mw = self.ni * NW * WP
        self.hd = self.d // HEADS
        self.quad = 128 // self.hd
        self.ng = HEADS // self.quad
        self.nch = self.ff // CH
        self.scaling = self.hd**-0.5
        self.heads_part = HEADS // self.parts


LINK = 90.0e3
CORE_LINK = 430.0e3
HOP = 2.0
CORE_HOP = 0.8
MARGIN = 0.3


class Plan:
    def __init__(self):
        self.clock = 0.0
        self.free = {}
        self.queue = []
        self.count = 0

    def link(self, name, size, rate, hop):
        begin = max(self.free.get(name, 0.0), self.clock)
        self.free[name] = begin + size / rate
        return begin + size / rate + hop + MARGIN

    def add(self, when, step):
        heapq.heappush(self.queue, (when, self.count, step))
        self.count += 1

    def pop(self):
        when, _, step = heapq.heappop(self.queue)
        self.clock = max(self.clock, when)
        step()

    def until(self, when):
        while self.queue and self.queue[0][0] <= when:
            self.pop()
        self.clock = max(self.clock, when)

    def due(self, when):
        return bool(self.queue) and self.queue[0][0] <= when


class Piece:
    def __init__(self, z, kind, index, rows, cols):
        self.kind, self.index, self.rows, self.cols = kind, index, rows, cols
        self.unit = rows * cols * 2 * z.parts

    def home(self, p):
        if self.kind == PROJ or (self.kind == QKV and self.index == 2):
            return None
        if self.kind == QKV:
            return p if self.index == 0 else 1 - p
        if p == 1 and self.index == 1:
            return None
        return p if self.kind == FC1 else 1 - p

QKV, PROJ, FC1, FC2 = range(4)


def make_pieces(z, qrow, prow, f2row):
    pieces = [Piece(z, QKV, k, qrow, z.d // z.parts) for k in range(3)]
    pieces.append(Piece(z, PROJ, 0, prow, z.d))
    pieces += [Piece(z, FC1, k, qrow, z.ff // z.parts // 2) for k in range(2)]
    pieces += [Piece(z, FC2, k, f2row // 2, z.d) for k in range(2)]
    for i, piece in enumerate(pieces):
        piece.id = i
    return pieces


def kernel(z, *refs):
    r = types.SimpleNamespace(**dict(zip(z.names, refs)))
    s = lax.axis_index(SECTION)
    d = lax.axis_index(DP)
    t = lax.axis_index(TENSOR)
    na, nb, nt, ns, ni = z.na, z.nb, z.parts, z.sections, z.ni
    a = d // nb
    b = lax.rem(d, nb)
    rows, m = z.rows, z.m
    pieces = z.pieces
    plan = Plan()

    def dev(s_=None, a_=None, b_=None, t_=None):
        s_ = s if s_ is None else s_
        a_ = a if a_ is None else a_
        b_ = b if b_ is None else b_
        t_ = t if t_ is None else t_
        return (s_, a_ * nb + b_, t_)

    def ahead(base, n):
        return [lax.rem(base + k, n) for k in range(1, n)]

    def behind(base, n):
        return [lax.rem(base + n - k, n) for k in range(1, n)]

    x_peers, x_from = ahead(s, ns), behind(s, ns)
    a_peers, a_from = ahead(a, na), behind(a, na)
    b_peers, b_from = ahead(b, nb), behind(b, nb)
    c_peers, c_from = ahead(t, nt), behind(t, nt)
    ALL = slice(None)

    def win(q, ref, lead, a_, b_, t_):
        if q.kind == QKV:
            return ref.at[lead + (q.index, t_, a_, b_)]
        if q.kind == FC1:
            return ref.at[lead + (t_, q.index, a_, b_)]
        if q.kind == FC2:
            return ref.at[lead + (t_, a_, b_, pl.ds(q.index * q.rows, q.rows))]
        return ref.at[lead + (t_, a_, b_)]

    wref = {QKV: r.wq, PROJ: r.wp, FC1: r.w1, FC2: r.w2}

    def shard(q, q_ref, p_ref, f1_ref, f2_ref):
        if q.kind == QKV:
            return q_ref.at[q.index]
        if q.kind == FC1:
            return f1_ref.at[:, pl.ds(q.index * q.cols, q.cols)]
        if q.kind == FC2:
            return f2_ref.at[pl.ds(q.index * q.rows, q.rows)]
        return p_ref

    lx, xs = r.lx, r.xs
    zs, zr, ys, yr, cs, cr = r.zs, r.zr, r.ys, r.yr, r.cs, r.cr

    def remote(src, dst, ss, rs, device):
        return pltpu.make_async_remote_copy(
            src_ref=src, dst_ref=dst, send_sem=ss, recv_sem=rs, device_id=device, device_id_type=MESH
        )

    def send(src, dst, ss, rs, device):
        remote(src, dst, ss, rs, device).start()

    def arrived(dst, sem):
        pltpu.make_async_copy(dst, dst, sem).wait()

    ready_at, x_at = {}, {}
    steps_left = {}

    def planes(home):
        return range(ns) if home is None else (home,)

    def on(home, body):
        if home is None:
            body()
        else:
            pl.when(s == home)(body)

    def other(home):
        return 1 - home

    def own_shard(q):
        return shard(q, r.q_in, r.p_in, r.f1_in, r.f2_in)

    def start_x(q):
        for p in range(ns):
            home = q.home(p)
            target = win(q, wref[q.kind], (p,), a, b, t)

            @pl.when(s == p)
            def _():
                if home in (None, p):
                    pltpu.make_async_copy(own_shard(q), target, lx.at[q.id, p]).start()
                if home != p:
                    send(own_shard(q), target, xs.at[q.id], lx.at[q.id, p], dev(s_=other(p)))

            x_at[q.id, p] = plan.clock + 1.0
            if home != p:
                x_at[q.id, p] = plan.link(f"x{p}", q.unit, LINK, HOP)
            steps_left[q.id, p] = na if home is None else 2 * na

    def link_of(name, home, size):
        return max(plan.link(f"{name}{h}", size, LINK, HOP) for h in planes(home))

    def go_z(q, p):
        here = win(q, wref[q.kind], (p,), a, b, t)
        home = q.home(p)
        plan.clock = max(plan.clock, x_at[q.id, p])

        def body():
            arrived(here, lx.at[q.id, p])
            for k, peer in enumerate(a_peers):
                send(here, here, zs.at[q.id, p, k], zr.at[q.id, p, k], dev(a_=peer))

        on(home, body)
        plan.add(plan.clock, functools.partial(go_y, q, p, 0))
        for k in range(na - 1):
            when = link_of("z", home, q.unit * na / (na - 1))
            plan.add(when, functools.partial(go_y, q, p, k + 1))

    def source_row(k):
        return a if k == 0 else a_from[k - 1]

    def go_y(q, p, k):
        here = win(q, wref[q.kind], (p,), source_row(k), b, t)
        home = q.home(p)

        def body():
            if k:
                arrived(here, zr.at[q.id, p, k - 1])
            for j, peer in enumerate(b_peers):
                send(here, here, ys.at[q.id, p, k, j], yr.at[q.id, p, k, j], dev(b_=peer))

        on(home, body)
        for j in range(nb - 1):
            when = link_of("y", home, q.unit)
        plan.add(when, functools.partial(go_c, q, p, k))

    def to_core(q, p, k):
        here = win(q, wref[q.kind], (p,), source_row(k), ALL, t)
        for j, peer in enumerate(c_peers):
            send(here, here, cs.at[q.id, p, k, j], cr.at[q.id, p, k, j], dev(t_=peer))

    def core_time(q, p):
        when = plan.link("c", q.unit * nb / nt, CORE_LINK, CORE_HOP)
        ready_at[q.id, p] = max(when, ready_at.get((q.id, p), 0.0))
        steps_left[q.id, p] -= 1

    def go_c(q, p, k):
        home = q.home(p)

        def body():
            for j, source in enumerate(b_from):
                arrived(win(q, wref[q.kind], (p,), source_row(k), source, t), yr.at[q.id, p, k, j])
            if home is not None:
                here = win(q, wref[q.kind], (p,), source_row(k), ALL, t)
                send(here, here, r.ws.at[q.id, p, k], r.wr.at[q.id, p, k], dev(s_=other(home)))
            to_core(q, p, k)

        on(home, body)
        core_time(q, p)
        if home is not None:
            when = plan.link(f"x{home}", q.unit * nb, LINK, HOP)
            plan.add(when, functools.partial(go_w, q, p, k))

    def go_w(q, p, k):
        def body():
            arrived(win(q, wref[q.kind], (p,), source_row(k), ALL, t), r.wr.at[q.id, p, k])
            to_core(q, p, k)

        on(other(q.home(p)), body)
        core_time(q, p)

    def need(kind, p, index=None):
        for q in pieces:
            if q.kind == kind and index in (None, q.index):
                while steps_left[q.id, p]:
                    plan.pop()
                plan.until(ready_at[q.id, p])
                for k in range(na):
                    for j, source in enumerate(c_from):
                        arrived(
                            win(q, wref[q.kind], (p,), source_row(k), ALL, source), cr.at[q.id, p, k, j]
                        )

    def gather_sent():
        for q in pieces:
            for p in range(ns):
                home = q.home(p)
                here = win(q, wref[q.kind], (p,), a, b, t)

                if home != p:

                    @pl.when(s == p)
                    def _():
                        arrived(own_shard(q), xs.at[q.id])

                def plane():
                    for k in range(na - 1):
                        arrived(here, zs.at[q.id, p, k])
                    for k in range(na):
                        for j in range(nb - 1):
                            arrived(here, ys.at[q.id, p, k, j])
                        if home is not None:
                            arrived(win(q, wref[q.kind], (p,), a, ALL, t), r.ws.at[q.id, p, k])

                on(home, plane)
                for k in range(na):
                    for j in range(nt - 1):
                        arrived(win(q, wref[q.kind], (p,), a, ALL, t), cs.at[q.id, p, k, j])

    def run(lo, hi, cost, body):
        base = plan.clock

        def one(i, carry):
            for k in range(lo, hi):
                when = base + (k - lo) * cost
                if plan.due(when):

                    @pl.when(i == k)
                    def _():
                        plan.until(when)

            body(i)
            return carry

        lax.fori_loop(lo, hi, one, 0)
        plan.until(base + (hi - lo) * cost)

    def spent(cost):
        plan.until(plan.clock + cost)

    SMF = r.smf
    P0, P1, P2 = r.p0, r.p1, r.p2
    small_ready = []

    def small_start():
        P0[s] = r.sm_in[...]
        for k, peer in enumerate(x_peers):
            send(r.sm_in, P0.at[s], r.ps.at[0, k], r.psr.at[0, k], dev(s_=peer))
        plan.add(plan.link("x0", P0.size * nt, LINK, HOP), small_a)

    def small_part(src, dst, level, targets):
        for k, target in enumerate(targets):
            send(src, dst.at[k], r.ps.at[level, k], r.psr.at[level, k], target)

    def small_sum(base, takes, level):
        total = base[...].astype(f32)
        for k in range(takes.shape[0]):
            arrived(takes.at[k], r.psr.at[level, k])
            total = total + takes[k].astype(f32)
        return total

    def small_a():
        for k, source in enumerate(x_from):
            arrived(P0.at[source], r.psr.at[0, k])
        small_part(P0, r.pa, 1, [dev(a_=p) for p in a_peers])
        plan.add(plan.link("z0", P0.size * 2 * nt * na, LINK, HOP), small_b)

    def small_b():
        P1[...] = small_sum(P0, r.pa, 1).astype(bf16)
        small_part(P1, r.pb, 2, [dev(b_=p) for p in b_peers])
        plan.add(plan.link("y0", P0.size * 2 * nt, LINK, HOP), small_c)

    def small_c():
        P2[...] = small_sum(P1, r.pb, 2).astype(bf16)
        small_part(P2, r.pc, 3, [dev(t_=p) for p in c_peers])
        plan.add(plan.clock + CORE_HOP, small_d)

    def small_d():
        SMF[...] = small_sum(P2, r.pc, 3)
        small_ready.append(True)

    def need_small():
        while not small_ready:
            plan.pop()

    def small_sent():
        arrived(r.sm_in, r.ps.at[0, 0])
        for level, takes in ((1, r.pa), (2, r.pb), (3, r.pc)):
            for k in range(takes.shape[0]):
                arrived(takes.at[k], r.ps.at[level, k])

    group = s * nt + t

    def group_images(g):
        return pl.ds(g * ni, ni)

    barrier = pltpu.get_barrier_semaphore()
    peers = (
        [dev(a_=p) for p in a_peers]
        + [dev(b_=p) for p in b_peers]
        + [dev(t_=p) for p in c_peers]
        + [dev(s_=p) for p in x_peers]
        + [dev(s_=p, t_=q) for p in x_peers for q in c_peers]
    )
    for p in peers:
        pl.semaphore_signal(barrier, inc=1, device_id=p, device_id_type=MESH)
    pl.semaphore_wait(barrier, len(peers))

    tbl = r.tbl
    pltpu.make_async_copy(r.tbl_in, tbl.at[s, t], r.tx.at[s]).start()
    for k, peer in enumerate(x_peers):
        send(r.tbl_in, tbl.at[s, t], r.txs.at[k], r.tx.at[s], dev(s_=peer))
    small_start()
    for q in pieces:
        start_x(q)
    xin = r.outb
    for j, src in enumerate((r.images, r.cotangent)):
        pltpu.make_async_copy(src.at[group_images(group)], xin.at[j, t], r.xl.at[j]).start()
        for k, peer in enumerate(c_peers):
            send(
                src.at[group_images(s * nt + peer)],
                xin.at[j, t],
                r.xcs.at[j, k],
                r.xcr.at[j, k],
                dev(t_=peer),
            )

    def image_ready(j):
        arrived(xin.at[j, t], r.xl.at[j])
        for k, source in enumerate(c_from):
            arrived(xin.at[j, source], r.xcr.at[j, k])

    pad_rows = jnp.zeros((z.hp - z.half, z.d), f32)

    def load_rows(j, ref):
        def one(i, _):
            pieces = []
            for h in range(nt):
                pieces.append(xin[j, h, i].astype(f32))
                if z.hp > z.half:
                    pieces.append(pad_rows)
            ref[block(i, rows), :] = jnp.concatenate(pieces, 0).astype(ref.dtype)
            return 0

        lax.fori_loop(0, ni, one, 0)

    outb = r.outb

    ships = {}

    def ship(kind, p, slot, i):
        out = r.act if kind == 0 else r.ig
        for h in range(nt):
            target = out.at[group * ni + i]
            mine = jnp.logical_and(s == p, t == h)

            @pl.when(mine)
            def _():
                pltpu.make_async_copy(outb.at[slot, h, i], target, r.os.at[kind, p, h]).start()

            @pl.when(jnp.logical_not(mine))
            def _():
                remote(
                    outb.at[slot, h, i], target, r.os.at[kind, p, h], r.orr.at[kind, group], (p, d, h)
                ).start()

        plan.link(f"x{other(p)}", rows * z.d * 2 * nt, LINK, HOP)
        ships[kind, p] = ships.get((kind, p), 0) + 1

    def ship_later(kind, p, slot, times):
        for i in range(ni):
            plan.add(plan.clock + times[i % len(times)], functools.partial(ship, kind, p, slot, i))

    def shipped(kind, p, slot):
        while ships.get((kind, p), 0) < ni:
            plan.pop()
        for h in range(nt):
            arrived(outb.at[slot, h], r.os.at[kind, p, h])

    def received(kind):
        out = r.act if kind == 0 else r.ig
        for g in range(ns * nt):

            @pl.when(g != group)
            def _():
                arrived(out.at[group_images(g)], r.orr.at[kind, g])

    def stage_out(value, i, slot):
        for h in range(nt):
            outb[slot, h, i] = value[h * z.hp : h * z.hp + z.half].astype(bf16)

    width = z.d // nt

    def w_qkv(p, c, part):
        return r.wq[p, c, part].reshape(z.d, width)

    def q_part(part):
        return slice(part * width, (part + 1) * width)

    def w_proj(p):
        return r.wp[p].reshape(z.d, z.d)

    w1_all = r.w1.reshape(2, z.nch, na, nb, r.w1.shape[-2], CH)

    def w_fc1(p, c):
        return w1_all[p, c].reshape(z.d, CH)

    w2_per = CH // r.w2.shape[-2]
    w2_all = r.w2.reshape(2, z.nch, w2_per, r.w2.shape[-2], z.d)

    def w_fc2(p, c):
        return w2_all[p, c].reshape(CH, z.d)

    def row(p, k):
        return SMF[p, pl.ds(k, 1), :]

    def masks(dtype):
        lane = lax.broadcasted_iota(jnp.int32, (WP, 128), 1) // z.hd
        return [(lane == h).astype(dtype) for h in range(z.quad)]

    def spread(v, mk):
        return jnp.concatenate([v * q for q in mk], 0)

    def collect(v, mk):
        acc = v[0:WP] * mk[0]
        for h in range(1, z.quad):
            acc = acc + v[h * WP : (h + 1) * WP] * mk[h]
        return acc

    BM = r.bm
    lanes = 128
    per_lane = lanes // WP

    def build_bias(p):
        j = lax.broadcasted_iota(jnp.int32, (WP, lanes), 0)
        lane = lax.broadcasted_iota(jnp.int32, (WP, lanes), 1)
        i = lax.rem(lane, WP)
        iy, ix, jy, jx = i // WIN, lax.rem(i, WIN), j // WIN, lax.rem(j, WIN)
        valid = jnp.logical_and(i < WT, j < WT)
        index = (iy - jy + WIN - 1) * TABLE_SIDE + ix - jx + WIN - 1
        index = jnp.where(valid, index, 0)
        low = jnp.where(index < lanes, index, 0)
        high = jnp.where(index < lanes, 0, index - lanes)
        head_of_lane = lane // WP

        def look(head):
            tt, hh = head // z.heads_part, head % z.heads_part
            entry = tbl[p, tt, pl.ds(hh, 1), :]
            one = jnp.take_along_axis(jnp.broadcast_to(entry[:, :lanes], (WP, lanes)), low, axis=1)
            two = jnp.take_along_axis(jnp.broadcast_to(entry[:, lanes:], (WP, lanes)), high, axis=1)
            return jnp.where(index < lanes, one, two)

        def region(q, wy):
            first = jnp.zeros_like(q)
            if wy < ACROSS - 1:
                return first
            return jnp.where(q < WIN - SHIFT, first + 1, first + 2)

        for g in range(z.ng):
            for c in range(z.quad // per_lane):
                value = look(g * z.quad + c * per_lane)
                for e in range(1, per_lane):
                    value = jnp.where(head_of_lane == e, look(g * z.quad + c * per_lane + e), value)
                value = jnp.where(j < WT, value, -1e30)
                for w in range(NW if p else 1):
                    out = value
                    if p == 1:
                        wy, wx = w // ACROSS, w % ACROSS
                        label_i = region(iy, wy) * 3 + region(ix, wx)
                        label_j = region(jy, wy) * 3 + region(jx, wx)
                        out = out + jnp.where(
                            jnp.logical_and(valid, label_i != label_j), MASK_FILL, 0.0
                        )
                    BM[p + w, g, :, c * lanes : (c + 1) * lanes] = out

    X, G = r.mg, r.g
    PM, PMT = r.pm, r.pmt
    FN, N1, K = r.fn, r.n1, r.k
    QK, PR, CTX, CTXT = r.qk, r.pr, r.ctx, r.ctxt
    MID, MG, SN, N2, ACT, SL = r.mid, r.mg, r.sn, r.n2, r.actv, r.sl
    SG, DB = r.sg, r.db

    def forward(p):
        need_small()

        def ln1(i):
            n, inv = normalize(X[block(i, rows), :])
            N1[p, block(i, rows), :] = n.astype(bf16)
            K[block(i, rows), 2 * p : 2 * p + 1] = inv
            f = (n * row(p, 0) + row(p, 1)).astype(bf16)
            FN[p, block(i, rows), :] = f
            CTX[block(i, NW * WP), :] = dotf(PM[p], f, NN).astype(bf16)

        run(0, ni, 0.45, ln1)
        for c in range(3):
            need(QKV, p, c)
            for e in range(nt):
                bias = row(p, 6 + c)[:, q_part(e)]
                QK[p, c, :, q_part(e)] = (dotf(CTX[...], w_qkv(p, c, e), NN) + bias).astype(bf16)
            spent(0.7)

        def attention(i):
            mb, mf = masks(bf16), masks(f32)
            units = [(i * BATCH + e, g) for e in range(BATCH) for g in range(z.ng)]
            at = [(block(u, WP), slice(g * 128, (g + 1) * 128)) for u, g in units]
            raw = [dotf(QK[p, 1, S, L], spread(QK[p, 0, S, L], mb), NT) for S, L in at]
            prs = []
            for (u, g), sc in zip(units, raw):
                w = 1 + lax.rem(u, NW) if p else 0
                sc = sc * z.scaling + BM[w, g]
                e = jnp.exp(sc - jnp.max(sc, 0, keepdims=True))
                pr = (e * (1.0 / jnp.sum(e, 0, keepdims=True))).astype(bf16)
                PR[p, u, g] = pr
                prs.append(pr)
            mixed = [dotf(pr, QK[p, 2, S, L], TN) for pr, (S, L) in zip(prs, at)]
            for v, (S, L) in zip(mixed, at):
                CTX[S, L] = collect(v, mf).astype(bf16)

        run(0, ni * NW // BATCH, 0.72, attention)

        def unperm(i):
            CTXT[p, block(i, rows), :] = dotf(PMT[p], CTX[block(i, NW * WP), :], NN).astype(bf16)

        run(0, ni, 0.21, unperm)
        need(PROJ, p)
        MID[...] = dotf(CTXT[p], w_proj(p), NN)
        spent(0.6)

        def ln2(i):
            mid = X[block(i, rows), :] + MID[block(i, rows), :] + row(p, 2)
            MID[block(i, rows), :] = mid
            n, inv = normalize(mid)
            N2[p, block(i, rows), :] = n.astype(bf16)
            K[block(i, rows), 2 * p + 1 : 2 * p + 2] = inv
            SN[p, block(i, rows), :] = (n * row(p, 3) + row(p, 4)).astype(bf16)

        run(0, ni, 0.26, ln2)
        if p == 1:
            for j, ref in enumerate((ACT, SL)):
                arrived(ref, r.sp.at[j])
        per = z.nch // 2

        for j in range(2):
            need(FC1, p, j)

            def rise(i):
                c = j + 2 * i
                u = dotf(SN[p], w_fc1(p, c), NN) + row(p, 9 + c)
                e = 0.5 * (1.0 + lax.erf(u * ROOT_HALF))
                ACT[c] = (u * e).astype(bf16)
                SL[c] = (e + u * jnp.exp(-0.5 * u * u) * INV_ROOT_TWO_PI).astype(bf16)

            run(0, per, 1.16, rise)
        need(FC2, p)

        def fall(c):
            MID[...] += dotf(ACT[c], w_fc2(p, c), NN)

        run(0, z.nch, 0.6, fall)
        if p == 0:
            for j, ref in enumerate((ACT, SL)):
                pltpu.make_async_copy(ref, r.spill.at[j], r.sp.at[j]).start()

        def finish(i):
            value = MID[block(i, rows), :] + row(p, 5)
            X[block(i, rows), :] = value.astype(bf16).astype(f32)
            stage_out(value, i, p)

        run(0, ni, 0.05, finish)
        ship_later(0, p, p, (18.0, 24.0, 30.0, 36.0) if p == 0 else (0.0, 5.0, 10.0, 15.0))

    g1_own = r.g1.reshape(z.nch, *w1_all.shape[2:])
    g2_own = r.g2.reshape(z.nch, *w2_all.shape[2:])

    def backward(p):
        gq, gp, g1, g2 = (
            (r.gq, r.gp, g1_own, g2_own) if p else (r.wq.at[1], r.wp.at[1], w1_all.at[1], w2_all.at[1])
        )
        def addrow(k, v):
            SG[p, pl.ds(k, 1), 0 : z.d] = SG[p, pl.ds(k, 1), 0 : z.d] + v

        SG[p] = jnp.zeros(SG.shape[1:], f32)
        DB[...] = jnp.zeros(DB.shape, f32)
        if p == 0:
            for j, ref in enumerate((ACT, SL)):
                arrived(ref, r.sp.at[j])
            gather_sent()

        def fc2(c):
            g2[c] = dotf(ACT[c], G[...], TN).astype(bf16).reshape(g2.shape[1:])
            hg = dotf(G[...], w_fc2(p, c), NT) * SL[c].astype(f32)
            SG[p, pl.ds(9 + c, 1), 0 : z.d] = column_sum(hg)
            SL[c] = hg.astype(bf16)

        run(0, z.nch, 1.2, fc2)

        def fc1(c):
            g1[c] = dotf(SN[p], SL[c], TN).astype(bf16).reshape(g1.shape[1:])

        run(0, 1, 0.78, fc1)
        emit(FC2, p)
        run(1, z.nch, 0.78, fc1)
        MID[...] = dotf(SL[0], w_fc1(p, 0), NT)
        emit(FC1, p)
        spent(0.5)

        def n2g(c):
            MID[...] += dotf(SL[c], w_fc1(p, c), NT)

        run(1, z.nch, 0.65, n2g)
        if p == 1:
            for j, ref in enumerate((ACT, SL)):
                pltpu.make_async_copy(r.spill.at[j], ref, r.sp.at[j]).start()

        def ln2(i):
            sl = block(i, rows)
            ng = MID[sl, :]
            n = N2[p, sl, :].astype(f32)
            g = G[sl, :].astype(f32)
            mg = g + norm_pull(ng, n, K[sl, 2 * p + 1 : 2 * p + 2], row(p, 3))
            MG[sl, :] = mg
            addrow(5, column_sum(g))
            addrow(3, column_sum(ng * n))
            addrow(4, column_sum(ng))
            addrow(2, column_sum(mg))
            G[sl, :] = mg.astype(bf16)

        run(0, ni, 0.31, ln2)
        gp[...] = dotf(CTXT[p], G[...], TN).astype(bf16).reshape(gp.shape)
        CTXT[p] = dotf(G[...], w_proj(p), NT).astype(bf16)
        spent(1.2)

        def cgrad(i):
            CTX[block(i, NW * WP), :] = dotf(PM[p], CTXT[p, block(i, rows), :], NN).astype(bf16)

        run(0, ni, 0.23, cgrad)
        emit(PROJ, p)

        def attention(i):
            mb, mf = masks(bf16), masks(f32)
            units = [(i * BATCH + e, g) for e in range(BATCH) for g in range(z.ng)]
            at = [(block(u, WP), slice(g * 128, (g + 1) * 128)) for u, g in units]
            cbd = [spread(CTX[S, L], mb) for S, L in at]
            dps = [dotf(QK[p, 2, S, L], c, NT) for (S, L), c in zip(at, cbd)]
            dvs = [dotf(PR[p, u, g], c, NN) for (u, g), c in zip(units, cbd)]
            sbs = []
            for (u, g), dp in zip(units, dps):
                pf = PR[p, u, g].astype(f32)
                tt = pf * dp
                sc = tt - pf * jnp.sum(tt, 0, keepdims=True)
                DB[g] = DB[g] + sc
                sbs.append(sc.astype(bf16))
            for v, (S, L) in zip(dvs, at):
                QK[p, 2, S, L] = v.astype(bf16)
            dks = [dotf(sb, spread(QK[p, 0, S, L], mb), NN) for sb, (S, L) in zip(sbs, at)]
            dqs = [dotf(sb, QK[p, 1, S, L], TN) for sb, (S, L) in zip(sbs, at)]
            for dk, dq, (S, L) in zip(dks, dqs, at):
                QK[p, 1, S, L] = (dk * z.scaling).astype(bf16)
                QK[p, 0, S, L] = (collect(dq, mf) * z.scaling).astype(bf16)

        def un(c, i):
            dv = dotf(PMT[p], QK[p, c, block(i, NW * WP), :], NN)
            addrow(6 + c, column_sum(dv))
            QK[p, c, block(i, rows), :] = dv.astype(bf16)

        def qkv_grad(c):
            value = dotf(FN[p], QK[p, c, 0:m, :], TN).astype(bf16)
            for e in range(nt):
                gq[c, e] = value[:, q_part(e)].reshape(gq.shape[2:])
            spent(0.75)

        def pull(sl, c):
            return sum(dotf(QK[p, c, sl, q_part(e)], w_qkv(p, c, e), NT) for e in range(nt))

        def ln1(i):
            sl = block(i, rows)
            ng = MID[sl, :] if p else pull(sl, 0) + pull(sl, 1) + pull(sl, 2)
            n = N1[p, sl, :].astype(f32)
            xg = MG[sl, :] + norm_pull(ng, n, K[sl, 2 * p : 2 * p + 1], row(p, 0))
            addrow(0, column_sum(ng * n))
            addrow(1, column_sum(ng))
            if p:
                G[sl, :] = xg.astype(bf16)
            stage_out(xg, i, 1 - p)

        if p == 1:
            run(0, ni * NW // BATCH, 0.82, attention)
            for c in range(3):
                run(0, ni, 0.23, functools.partial(un, c))
                qkv_grad(c)
                if c:
                    emit(QKV, p, c - 1)
            for c in range(3):
                v = pull(slice(0, m), c)
                MID[...] = v if c == 0 else MID[...] + v
                if c == 0:
                    emit(QKV, p, 2)
                spent(0.8)
            shipped(0, 0, 0)
            run(0, ni, 0.28, ln1)
            ship_later(1, p, 1 - p, (1.0, 6.0, 11.0, 16.0))
            table_rows(p)
            spent(1.6)
        else:
            shipped(0, 1, 1)
            per = NW // BATCH
            cost = 1.8

            def image_step(k):
                attention(k)

                @pl.when(lax.rem(k, per) == per - 1)
                def _():
                    for c in range(3):
                        un(c, k // per)
                    ln1(k // per)

            ship_later(1, p, 1 - p, [per * cost * (i + 1) for i in range(ni)])
            run(0, ni * per, cost, image_step)
            for c in range(3):
                qkv_grad(c)
                if c:
                    emit(QKV, p, c - 1)
            table_rows(p)
            emit(QKV, p, 2)
            spent(1.6)

    def table_rows(p):
        src = lax.broadcasted_iota(jnp.int32, (z.quad * WP, TABLE_PAD), 0)
        dst = lax.broadcasted_iota(jnp.int32, (z.quad * WP, TABLE_PAD), 1)
        i = lax.rem(src, WP)
        place = jnp.logical_and(
            i < WT, dst == CENTER - ((i // WIN) * TABLE_SIDE + lax.rem(i, WIN))
        )
        head = src // WP
        pick = jnp.concatenate(
            [jnp.logical_and(place, head == h).astype(bf16) for h in range(z.quad)], 1
        )
        group_row = lax.broadcasted_iota(jnp.int32, (8, WP), 0)
        group_of = lax.broadcasted_iota(jnp.int32, (8, WP), 1)
        rows_of = jnp.logical_and(group_of < WT, group_of // WIN == group_row).astype(bf16)

        def split_dot(x, y, left):
            big = x if left else y
            hi = big.astype(bf16)
            lo = (big - hi.astype(f32)).astype(bf16)
            if left:
                return dotf(hi, y, NN) + dotf(lo, y, NN)
            return dotf(x, hi, NN) + dotf(x, lo, NN)

        for g in range(z.ng):
            e = split_dot(DB[g], pick, True)
            for h in range(z.quad):
                v = e[:, h * TABLE_PAD : (h + 1) * TABLE_PAD]
                v = pltpu.roll(v, 0, 1, stride=1, stride_axis=0)
                v = split_dot(rows_of, v, False)
                v = pltpu.roll(v, 0, 1, stride=TABLE_SIDE - WIN, stride_axis=0)
                SG[p, pl.ds(g * z.quad + h, 1), z.d :] = column_sum(v)

    gref = {QKV: r.gq, PROJ: r.gp, FC1: r.g1, FC2: r.g2}
    s1, v1, s2, v2, s3, v3, s4, v4 = (r.s1, r.v1, r.s2, r.v2, r.s3, r.v3, r.s4, r.v4)
    k1, k2, k3 = r.k1, r.k2, r.k3
    done = {}

    def buffer(level, q):
        return getattr(r, f"r{level}_{q.id}")

    def gwin(q, p, a_, b_, t_):
        if p == 0:
            return win(q, wref[q.kind], (1,), a_, b_, t_)
        return win(q, gref[q.kind], (), a_, b_, t_)

    def gout(q):
        return shard(q, r.gq_out, r.gp_out, r.g1_out, r.g2_out)

    def reached(q, p, level):
        while done.get((q.id, p), 0) < level:
            plan.pop()

    def credit(sem, q, k, p, device):
        if p == 1:
            pl.semaphore_signal(sem.at[q.id, k], inc=1, device_id=device, device_id_type=MESH)

    def spend(sem, q, k, p):
        if p == 0:
            pl.semaphore_wait(sem.at[q.id, k], 1)

    def emit(kind, p, index=None):
        for q in pieces:
            if q.kind == kind and index in (None, q.index):
                r1(q, p)

    def r1(q, p):
        if p == 0:
            reached(q, 1, 4)
            settle(q, 1)
        for k, peer in enumerate(c_peers):
            spend(k1, q, k, p)
            send(gwin(q, p, ALL, ALL, peer), buffer(1, q).at[k], s1.at[q.id, k], v1.at[q.id, k], dev(t_=peer))
            when = plan.link("c", q.unit * na * nb / nt, CORE_LINK, CORE_HOP)
        done[q.id, p] = 1
        plan.add(when, functools.partial(r2, q, p))

    def r2(q, p):
        if p == 0:
            reached(q, 1, 3)
        for k in range(nt - 1):
            arrived(buffer(1, q).at[k], v1.at[q.id, k])
        mine = gwin(q, p, ALL, ALL, t)
        add_into(mine, [buffer(1, q).at[k] for k in range(nt - 1)])
        for k, source in enumerate(c_from):
            credit(k1, q, k, p, dev(t_=source))
        plan.clock += q.unit * na * nb / 10e6
        done[q.id, p] = 2
        to_y(q, p)

    def to_y(q, p):
        for k, peer in enumerate(b_peers):
            spend(k2, q, k, p)
            send(
                gwin(q, p, ALL, peer, t), buffer(2, q).at[k], s2.at[q.id, k], v2.at[q.id, k], dev(b_=peer)
            )
            when = link_of("y", None, q.unit * na)
        plan.add(when, functools.partial(r3, q, p))

    def r3(q, p):
        if p == 0:
            reached(q, 1, 4)
        for k in range(nb - 1):
            arrived(buffer(2, q).at[k], v2.at[q.id, k])
        add_into(gwin(q, p, ALL, b, t), [buffer(2, q).at[k] for k in range(nb - 1)])
        for k, source in enumerate(b_from):
            credit(k2, q, k, p, dev(b_=source))
        for k, peer in enumerate(a_peers):
            spend(k3, q, k, p)
            send(
                gwin(q, p, peer, b, t), buffer(3, q).at[k], s3.at[q.id, k], v3.at[q.id, k], dev(a_=peer)
            )
            when = link_of("z", None, q.unit * na / (na - 1))
        done[q.id, p] = 3
        plan.add(when, functools.partial(r4, q, p))

    def r4(q, p):
        if p == 0:
            reached(q, 1, 5)
        mine = gwin(q, p, a, b, t)
        for k in range(na - 1):
            arrived(buffer(3, q).at[k], v3.at[q.id, k])
        total = mine[...].astype(f32)
        for k in range(na - 1):
            total = total + buffer(3, q)[k].astype(f32)
        for k, source in enumerate(a_from):
            credit(k3, q, k, p, dev(a_=source))

        @pl.when(s == p)
        def _():
            gout(q)[...] = total

        @pl.when(s != p)
        def _():
            buffer(5, q)[...] = total.astype(bf16)
            remote(buffer(5, q), buffer(4, q), s4.at[q.id], v4.at[q.id], dev(s_=p)).start()

        done[q.id, p] = 4
        plan.add(plan.link(f"x{other(p)}", q.unit, LINK, HOP), functools.partial(r5, q, p))

    def r5(q, p):
        @pl.when(s == p)
        def _():
            arrived(buffer(4, q), v4.at[q.id])
            out = gout(q)
            out[...] = out[...] + buffer(4, q)[...].astype(f32)

        @pl.when(s != p)
        def _():
            arrived(buffer(5, q), s4.at[q.id])

        done[q.id, p] = 5

    def settle(q, p):
        for k, peer in enumerate(c_peers):
            arrived(gwin(q, p, ALL, ALL, peer), s1.at[q.id, k])
        for k, peer in enumerate(b_peers):
            arrived(gwin(q, p, ALL, peer, t), s2.at[q.id, k])
        for k, peer in enumerate(a_peers):
            arrived(gwin(q, p, peer, b, t), s3.at[q.id, k])

    def add_into(mine, others):
        lead = mine.shape[:-2]
        count = int(np.prod(lead))

        def one(i, _):
            index = []
            rest = i
            for extent in reversed(lead):
                index.append(lax.rem(rest, extent))
                rest = rest // extent
            index = tuple(reversed(index))
            total = mine[index].astype(f32)
            for o in others:
                total = total + o[index].astype(f32)
            mine[index] = total.astype(bf16)
            return 0

        lax.fori_loop(0, count, one, 0)

    first = [q for q in pieces if q.kind == QKV]
    plan.pop()
    for q in first:
        go_z(q, 0)
    plan.until(plan.clock)
    proj = [q for q in pieces if q.kind == PROJ]
    mixed = [q for k in range(2) for q in pieces if q.kind in (FC1, FC2) and q.index == k]
    order = [(q, 0) for q in proj + mixed] + [(q, 1) for q in first + proj + mixed]

    def z_free(q, p):
        return max(plan.free.get(f"z{h}", 0.0) for h in planes(q.home(p)))

    def next_z(k):
        q, p = order[k]
        go_z(q, p)
        if k + 1 < len(order):
            after = order[k + 1]
            plan.add(
                max(x_at[after[0].id, after[1]], z_free(*after) - 8.0), functools.partial(next_z, k + 1)
            )

    plan.add(x_at[order[0][0].id, 0], functools.partial(next_z, 0))
    for q in range(ns):
        arrived(tbl.at[q, t], r.tx.at[q])
        for k, peer in enumerate(c_peers):
            send(tbl.at[q, t], tbl.at[q, t], r.tcs.at[q, k], r.tcr.at[q, k], dev(t_=peer))
    spent(0.5)
    image_ready(0)
    load_rows(0, X)
    spent(0.3)
    for q in range(ns):
        for k, source in enumerate(c_from):
            arrived(tbl.at[q, source], r.tcr.at[q, k])
    for p in range(2):
        build_bias(p)
        spent(0.7)
    image_ready(1)
    load_rows(1, G)
    spent(0.2)

    for p in range(2):
        forward(p)
    for p in (1, 0):
        backward(p)

    ss, sv = r.ss, r.sv
    sums = [SG, r.sum1, r.sum2, r.sum3]
    takes = [r.ra, r.rc, r.rd, r.rb]
    lists = [
        [dev(t_=p) for p in c_peers],
        [dev(b_=p) for p in b_peers],
        [dev(a_=p) for p in a_peers],
        [dev(s_=p) for p in x_peers],
    ]

    def small_send(k):
        for j, target in enumerate(lists[k]):
            src = sums[k] if k < 3 else sums[k].at[x_peers[j]]
            send(src, takes[k].at[j], ss.at[k, j], sv.at[k, j], target)
        when = plan.link(("c", "y0", "z0", "x1")[k], SG.size * 4 * nt * len(lists[k]), LINK, HOP)
        plan.add(when, functools.partial(small_take, k))

    def small_take(k):
        for j in range(len(lists[k])):
            arrived(takes[k].at[j], sv.at[k, j])
        base = sums[k][...] if k < 3 else sums[k][s]
        total = base + sum(takes[k][j] for j in range(len(lists[k])))
        if k < 3:
            sums[k + 1][...] = total
            small_send(k + 1)
        else:
            r.small_out[...] = total

    small_send(0)
    while plan.queue:
        plan.pop()

    for q in pieces:
        settle(q, 0)
    small_sent()
    received(0)
    received(1)
    shipped(1, 1, 0)
    shipped(1, 0, 1)
    for k in range(ns - 1):
        arrived(r.tbl_in, r.txs.at[k])
    for q in range(ns):
        for k in range(nt - 1):
            arrived(tbl.at[q, t], r.tcs.at[q, k])
    for j, src in enumerate((r.images, r.cotangent)):
        for k in range(nt - 1):
            arrived(outb.at[j, t], r.xcs.at[j, k])
    for k in range(4):
        for j in range(len(lists[k])):
            arrived(takes[k].at[j], ss.at[k, j])


def per_device(z, images, cotangent, norm1_gain, norm1_bias, qkv_weight, qkv_bias, position_table,
               proj_weight, proj_bias, norm2_gain, norm2_bias, fc1_weight, fc1_bias, fc2_weight,
               fc2_bias):
    s = lax.axis_index(SECTION)
    d = lax.axis_index(DP)
    t = lax.axis_index(TENSOR)
    D, nt, na, nb, ns, ni = z.d, z.parts, z.na, z.nb, z.sections, z.ni
    part = t * z.dp + d

    def spread_to(values, width, at):
        blank = jnp.zeros((values.shape[0], width), bf16)
        return lax.dynamic_update_slice(blank, values, (0, at))

    vectors = jnp.concatenate(
        [norm1_gain, norm1_bias, proj_bias, norm2_gain, norm2_bias, fc2_bias], 0
    )
    vectors = jnp.where(t == 0, vectors, jnp.zeros_like(vectors))
    small = jnp.concatenate(
        [
            spread_to(vectors, D, d * vectors.shape[1]),
            spread_to(qkv_bias[0], D, part * qkv_bias.shape[-1]),
            spread_to(fc1_bias, z.ff, part * fc1_bias.shape[-1]).reshape(-1, D),
        ],
        0,
    )
    small = jnp.pad(small, ((0, GATHER_ROWS - small.shape[0]), (0, 0)))
    table = jnp.pad(position_table[0].T, ((0, 0), (0, TABLE_PAD - position_table.shape[1])))
    perm = window_permutation(nt, z.half, z.hp)

    qrow, prow, f2row = qkv_weight.shape[1], proj_weight.shape[1], fc2_weight.shape[1]
    m, mw, nch = z.m, z.mw, z.nch
    S = jax.ShapeDtypeStruct
    V = pl.BlockSpec(memory_space=pltpu.VMEM)
    A = pl.BlockSpec(memory_space=pl.ANY)
    dma = pltpu.SemaphoreType.DMA
    reg = pltpu.SemaphoreType.REGULAR
    inputs = dict(
        images=(images, A),
        cotangent=(cotangent, A),
        q_in=(qkv_weight[0].transpose(1, 0, 2), A),
        p_in=(proj_weight[0], A),
        f1_in=(fc1_weight[0], A),
        f2_in=(fc2_weight[0], A),
        sm_in=(small, V),
        tbl_in=(table, V),
        pm=(jnp.asarray(perm, bf16), V),
        pmt=(jnp.asarray(perm.transpose(0, 2, 1), bf16), V),
    )
    wide = D + TABLE_PAD
    outputs = dict(
        act=(S(images.shape, bf16), A),
        ig=(S(images.shape, bf16), A),
        gq_out=(S((3, qrow, D // nt), f32), V),
        gp_out=(S((prow, D), f32), V),
        g1_out=(S((qrow, z.ff // nt), f32), V),
        g2_out=(S((f2row, D), f32), V),
        small_out=(S((GATHER_ROWS, wide), f32), V),
        spill=(S((2, nch, m, CH), bf16), A),
    )
    vm = pltpu.VMEM
    z.pieces = make_pieces(z, qrow, prow, f2row)
    W = len(z.pieces)
    scratch = dict(
        wq=vm((2, 3, nt, na, nb, qrow, D // nt), bf16),
        wp=vm((2, nt, na, nb, prow, D), bf16),
        w1=vm((2, nt, 2, na, nb, qrow, z.ff // nt // 2), bf16),
        w2=vm((2, nt, na, nb, f2row, D), bf16),
        p0=vm((2, GATHER_ROWS, D), bf16),
        p1=vm((2, GATHER_ROWS, D), bf16),
        p2=vm((2, GATHER_ROWS, D), bf16),
        pa=vm((na - 1, 2, GATHER_ROWS, D), bf16),
        pb=vm((nb - 1, 2, GATHER_ROWS, D), bf16),
        pc=vm((nt - 1, 2, GATHER_ROWS, D), bf16),
        ps=dma((4, max(na, nb, nt, ns))),
        psr=dma((4, max(na, nb, nt, ns))),
        ws=dma((W, 2, na)),
        wr=dma((W, 2, na)),
        smf=vm((2, GATHER_ROWS, D), f32),
        tbl=vm((2, nt, z.heads_part, TABLE_PAD), f32),
        outb=vm((2, nt, ni, z.half, D), bf16),
        bm=vm((1 + NW, z.ng, WP, z.quad * WP), f32),
        g=vm((m, D), bf16),
        fn=vm((2, m, D), bf16),
        n1=vm((2, m, D), bf16),
        k=vm((m, 4), f32),
        qk=vm((2, 3, mw, D), bf16),
        pr=vm((2, ni * NW, z.ng, WP, z.quad * WP), bf16),
        ctx=vm((mw, D), bf16),
        ctxt=vm((2, m, D), bf16),
        mid=vm((m, D), f32),
        mg=vm((m, D), f32),
        sn=vm((2, m, D), bf16),
        n2=vm((2, m, D), bf16),
        actv=vm((nch, m, CH), bf16),
        sl=vm((nch, m, CH), bf16),
        sg=vm((2, GATHER_ROWS, wide), f32),
        db=vm((z.ng, WP, z.quad * WP), f32),
        gq=vm((3, nt, na, nb, qrow, D // nt), bf16),
        gp=vm((nt, na, nb, prow, D), bf16),
        g1=vm((nt, 2, na, nb, qrow, z.ff // nt // 2), bf16),
        g2=vm((nt, na, nb, f2row, D), bf16),
        ra=vm((nt - 1, 2, GATHER_ROWS, wide), f32),
        rb=vm((ns - 1, GATHER_ROWS, wide), f32),
        rc=vm((nb - 1, 2, GATHER_ROWS, wide), f32),
        rd=vm((na - 1, 2, GATHER_ROWS, wide), f32),
        sum1=vm((2, GATHER_ROWS, wide), f32),
        sum2=vm((2, GATHER_ROWS, wide), f32),
        sum3=vm((2, GATHER_ROWS, wide), f32),
        lx=dma((W, ns)),
        xs=dma((W,)),
        zs=dma((W, 2, na - 1)),
        zr=dma((W, 2, na - 1)),
        ys=dma((W, 2, na, nb - 1)),
        yr=dma((W, 2, na, nb - 1)),
        cs=dma((W, 2, na, nt - 1)),
        cr=dma((W, 2, na, nt - 1)),
        tx=dma((ns,)),
        txs=dma((ns - 1,)),
        tcs=dma((ns, nt - 1)),
        tcr=dma((ns, nt - 1)),
        xl=dma((2,)),
        xcs=dma((2, nt - 1)),
        xcr=dma((2, nt - 1)),
        os=dma((2, 2, nt)),
        orr=dma((2, ns * nt)),
        sp=dma((2,)),
        s1=dma((W, nt - 1)),
        v1=dma((W, nt - 1)),
        s2=dma((W, nb - 1)),
        v2=dma((W, nb - 1)),
        s3=dma((W, na - 1)),
        v3=dma((W, na - 1)),
        s4=dma((W,)),
        v4=dma((W,)),
        k1=reg((W, nt - 1)),
        k2=reg((W, nb - 1)),
        k3=reg((W, na - 1)),
        ss=dma((4, max(na, nb, nt, ns))),
        sv=dma((4, max(na, nb, nt, ns))),
    )
    for q in z.pieces:
        scratch[f"r1_{q.id}"] = vm((nt - 1, na, nb, q.rows, q.cols), bf16)
        scratch[f"r2_{q.id}"] = vm((nb - 1, na, q.rows, q.cols), bf16)
        scratch[f"r3_{q.id}"] = vm((na - 1, q.rows, q.cols), bf16)
        scratch[f"r4_{q.id}"] = vm((q.rows, q.cols), bf16)
        scratch[f"r5_{q.id}"] = vm((q.rows, q.cols), bf16)
    z.names = list(inputs) + list(outputs) + list(scratch)
    results = pl.pallas_call(
        functools.partial(kernel, z),
        out_shape=tuple(o for o, _ in outputs.values()),
        in_specs=[spec for _, spec in inputs.values()],
        out_specs=tuple(spec for _, spec in outputs.values()),
        scratch_shapes=list(scratch.values()),
        compiler_params=pltpu.CompilerParams(
            collective_id=0, has_side_effects=True, vmem_limit_bytes=67043328
        ),
        name="two_blocks",
    )(*[x for x, _ in inputs.values()])
    act, ig, gq, gp, g1, g2, sums, _ = results

    def own_vector(k):
        width = norm1_gain.shape[1]
        return lax.dynamic_slice(sums, (k, d * width), (1, width))

    width = qkv_bias.shape[-1]
    qkv_bias_grad = lax.dynamic_slice(sums, (6, part * width), (3, width))[None]
    width = fc1_bias.shape[1]
    fc1_flat = sums[9 : 9 + nch, :D].reshape(1, -1)
    fc1_bias_grad = lax.dynamic_slice(fc1_flat, (0, part * width), (1, width))
    tables = lax.dynamic_slice(sums, (t * z.heads_part, D), (z.heads_part, TABLE_PAD))
    tables = tables[:, : position_table.shape[1]][:, ::-1].T[None]
    return (
        act[None],
        ig[None],
        own_vector(0),
        own_vector(1),
        gq.transpose(1, 0, 2)[None],
        qkv_bias_grad,
        tables,
        gp[None],
        own_vector(2),
        own_vector(3),
        own_vector(4),
        g1[None],
        fc1_bias_grad,
        g2[None],
        own_vector(5),
    )


def solution(mesh):
    def run(*args):
        z = Sizes(mesh, args[0], args[11])
        return per_device(z, *args)

    in_specs = (
        P(DP, TENSOR, None),
        P(DP, TENSOR, None),
        P(SECTION, DP),
        P(SECTION, DP),
        P(SECTION, DP, None, TENSOR),
        P(SECTION, None, (TENSOR, DP)),
        P(SECTION, None, TENSOR),
        P(SECTION, (TENSOR, DP), None),
        P(SECTION, DP),
        P(SECTION, DP),
        P(SECTION, DP),
        P(SECTION, DP, TENSOR),
        P(SECTION, (TENSOR, DP)),
        P(SECTION, (TENSOR, DP), None),
        P(SECTION, DP),
    )
    out_specs = (
        P(SECTION, DP, TENSOR, None),
        P(SECTION, DP, TENSOR, None),
        P(SECTION, DP),
        P(SECTION, DP),
        P(SECTION, DP, None, TENSOR),
        P(SECTION, None, (TENSOR, DP)),
        P(SECTION, None, TENSOR),
        P(SECTION, (TENSOR, DP), None),
        P(SECTION, DP),
        P(SECTION, DP),
        P(SECTION, DP),
        P(SECTION, DP, TENSOR),
        P(SECTION, (TENSOR, DP)),
        P(SECTION, (TENSOR, DP), None),
        P(SECTION, DP),
    )
    return jax.shard_map(
        run, mesh=mesh, in_specs=in_specs, out_specs=out_specs, check_vma=False
    )
```

```python
import functools
import heapq
import math
import types

import jax
import jax.numpy as jnp
import numpy as np
from jax import lax
from jax.experimental import pallas as pl
from jax.experimental.pallas import tpu as pltpu
from jax.sharding import PartitionSpec as P

HEADS = 16
WIN = 7
SIDE = 14
SHIFT = 3

EPS = 1e-05
MASK_FILL = -100.0
ROOT_HALF = 0.7071067811865476
INV_ROOT_TWO_PI = 0.3989422804014327

ACROSS = SIDE // WIN
NW = ACROSS * ACROSS
WT = WIN * WIN
WP = 64
TABLE_SIDE = 2 * WIN - 1
CENTER = (WIN - 1) * TABLE_SIDE + WIN - 1
TABLE_PAD = 256
CH = 512
GATHER_ROWS = 16
BATCH = 2

SECTION = "section"
DP = "dp"
TENSOR = "tensor"

f32 = jnp.float32
bf16 = jnp.bfloat16
MESH = pl.DeviceIdType.MESH
NN = ((1,), (0,))
NT = ((1,), (1,))
TN = ((0,), (0,))


def round_up(n, m):
    return -(-n // m) * m


def window_slots(shift):
    slot = np.zeros(SIDE * SIDE, np.int64)
    for p in range(SIDE):
        for q in range(SIDE):
            token = ((p + shift) % SIDE) * SIDE + (q + shift) % SIDE
            window = (p // WIN) * ACROSS + q // WIN
            slot[token] = window * WP + (p % WIN) * WIN + q % WIN
    return slot


def window_permutation(parts, half, padded):
    perm = np.zeros((2, NW * WP, parts * padded), np.float32)
    for block in range(2):
        for token, slot in enumerate(window_slots(SHIFT * block)):
            perm[block, slot, (token // half) * padded + token % half] = 1
    return perm


def dotf(a, b, dims):
    return lax.dot_general(a, b, (dims, ((), ())), preferred_element_type=f32)


def normalize(values):
    center = values - jnp.mean(values, -1, keepdims=True)
    inverse = lax.rsqrt(jnp.mean(center * center, -1, keepdims=True) + EPS)
    return center * inverse, inverse


def norm_pull(upstream, normed, inverse, gain):
    scaled = upstream * gain
    return inverse * (
        scaled
        - jnp.mean(scaled, -1, keepdims=True)
        - normed * jnp.mean(scaled * normed, -1, keepdims=True)
    )


def block(i, n):
    if isinstance(i, int):
        return pl.ds(i * n, n)
    return pl.ds(pl.multiple_of(i * n, n), n)


def column_sum(v):
    return jnp.sum(v, 0, keepdims=True)


class Sizes:
    def __init__(self, mesh, images, fc1_weight):
        self.sections = mesh.shape[SECTION]
        self.dp = mesh.shape[DP]
        self.parts = mesh.shape[TENSOR]
        inner = int(math.isqrt(self.dp))
        while self.dp % inner:
            inner -= 1
        self.nb = inner
        self.na = self.dp // inner
        self.local_images, self.half, self.d = images.shape
        self.ff = fc1_weight.shape[-1] * self.parts
        self.ni = self.local_images // (self.sections * self.parts)
        self.hp = round_up(self.half, 8)
        self.rows = self.parts * self.hp
        self.m = self.ni * self.rows
        self.mw = self.ni * NW * WP
        self.hd = self.d // HEADS
        self.quad = 128 // self.hd
        self.ng = HEADS // self.quad
        self.nch = self.ff // CH
        self.scaling = self.hd**-0.5
        self.heads_part = HEADS // self.parts


LINK = 90.0e3
CORE_LINK = 430.0e3
HOP = 2.0
CORE_HOP = 0.8
MARGIN = 0.3
SKEW = 0.0
ZLAG = 0.0


class Plan:
    def __init__(self):
        self.clock = 0.0
        self.free = {}
        self.queue = []
        self.count = 0

    def link(self, name, size, rate, hop):
        begin = max(self.free.get(name, 0.0), self.clock)
        self.free[name] = begin + size / rate
        return begin + size / rate + hop + MARGIN

    def add(self, when, step):
        heapq.heappush(self.queue, (when, self.count, step))
        self.count += 1

    def pop(self):
        when, _, step = heapq.heappop(self.queue)
        self.clock = max(self.clock, when)
        step()

    def pop_of(self, wanted):
        found = [e for e in self.queue if isinstance(e[2], functools.partial) and wanted(e[2])]
        if found:
            entry = min(found)
            self.queue.remove(entry)
            heapq.heapify(self.queue)
            self.clock = max(self.clock, entry[0])
            entry[2]()
        return bool(found)

    def until(self, when):
        while self.queue and self.queue[0][0] <= when:
            self.pop()
        self.clock = max(self.clock, when)

    def due(self, when):
        return bool(self.queue) and self.queue[0][0] <= when


class Piece:
    def __init__(self, z, kind, index, rows, cols):
        self.kind, self.index, self.rows, self.cols = kind, index, rows, cols
        self.unit = rows * cols * 2 * z.parts

    def home(self, p):
        if self.kind == PROJ or (self.kind == QKV and self.index == 2):
            return None
        if self.kind == QKV:
            return p if self.index == 0 else 1 - p
        if p == 1 and self.index == 1:
            return None
        return p if self.kind == FC1 else 1 - p

    def sum_home(self, p):
        if self.index == 1 and self.kind in (FC1, FC2):
            return 0 if self.kind == FC1 else 1
        return None


QKV, PROJ, FC1, FC2 = range(4)


def make_pieces(z, qrow, prow, f2row):
    pieces = [Piece(z, QKV, k, qrow, z.d // z.parts) for k in range(3)]
    pieces.append(Piece(z, PROJ, 0, prow, z.d))
    pieces += [Piece(z, FC1, k, qrow, z.ff // z.parts // 2) for k in range(2)]
    pieces += [Piece(z, FC2, k, f2row // 2, z.d) for k in range(2)]
    for i, piece in enumerate(pieces):
        piece.id = i
    return pieces


def kernel(z, *refs):
    r = types.SimpleNamespace(**dict(zip(z.names, refs)))
    s = lax.axis_index(SECTION)
    d = lax.axis_index(DP)
    t = lax.axis_index(TENSOR)
    na, nb, nt, ns, ni = z.na, z.nb, z.parts, z.sections, z.ni
    a = d // nb
    b = lax.rem(d, nb)
    rows, m = z.rows, z.m
    pieces = z.pieces
    plan = Plan()

    def dev(s_=None, a_=None, b_=None, t_=None):
        s_ = s if s_ is None else s_
        a_ = a if a_ is None else a_
        b_ = b if b_ is None else b_
        t_ = t if t_ is None else t_
        return (s_, a_ * nb + b_, t_)

    def ahead(base, n):
        return [lax.rem(base + k, n) for k in range(1, n)]

    def behind(base, n):
        return [lax.rem(base + n - k, n) for k in range(1, n)]

    x_peers, x_from = ahead(s, ns), behind(s, ns)
    a_peers, a_from = ahead(a, na), behind(a, na)
    b_peers, b_from = ahead(b, nb), behind(b, nb)
    c_peers, c_from = ahead(t, nt), behind(t, nt)
    ALL = slice(None)

    def win(q, ref, lead, a_, b_, t_):
        if q.kind == QKV:
            return ref.at[lead + (q.index, t_, a_, b_)]
        if q.kind == FC1:
            return ref.at[lead + (t_, q.index, a_, b_)]
        if q.kind == FC2:
            return ref.at[lead + (t_, a_, b_, pl.ds(q.index * q.rows, q.rows))]
        return ref.at[lead + (t_, a_, b_)]

    wref = {QKV: r.wq, PROJ: r.wp, FC1: r.w1, FC2: r.w2}

    def shard(q, q_ref, p_ref, f1_ref, f2_ref):
        if q.kind == QKV:
            return q_ref.at[q.index]
        if q.kind == FC1:
            return f1_ref.at[:, pl.ds(q.index * q.cols, q.cols)]
        if q.kind == FC2:
            return f2_ref.at[pl.ds(q.index * q.rows, q.rows)]
        return p_ref

    lx, xs = r.lx, r.xs
    zs, zr, ys, yr, cs, cr = r.zs, r.zr, r.ys, r.yr, r.cs, r.cr

    def remote(src, dst, ss, rs, device):
        return pltpu.make_async_remote_copy(
            src_ref=src, dst_ref=dst, send_sem=ss, recv_sem=rs, device_id=device, device_id_type=MESH
        )

    def send(src, dst, ss, rs, device):
        remote(src, dst, ss, rs, device).start()

    def arrived(dst, sem):
        pltpu.make_async_copy(dst, dst, sem).wait()

    ready_at, x_at = {}, {}
    steps_left = {}

    def planes(home):
        return range(ns) if home is None else (home,)

    def on(home, body):
        if home is None:
            body()
        else:
            pl.when(s == home)(body)

    def other(home):
        return 1 - home

    def own_shard(q):
        return shard(q, r.q_in, r.p_in, r.f1_in, r.f2_in)

    def start_x(q):
        for p in range(ns):
            home = q.home(p)
            target = win(q, wref[q.kind], (p,), a, b, t)

            @pl.when(s == p)
            def _():
                if home in (None, p):
                    pltpu.make_async_copy(own_shard(q), target, lx.at[q.id, p]).start()
                if home != p:
                    send(own_shard(q), target, xs.at[q.id], lx.at[q.id, p], dev(s_=other(p)))

            x_at[q.id, p] = plan.clock + 1.0
            if home != p:
                x_at[q.id, p] = plan.link(f"x{p}", q.unit, LINK, HOP)
            steps_left[q.id, p] = na if home is None else 2 * na

    def link_of(name, home, size):
        return max(plan.link(f"{name}{h}", size, LINK, HOP) for h in planes(home))

    def go_z(q, p):
        here = win(q, wref[q.kind], (p,), a, b, t)
        home = q.home(p)
        plan.clock = max(plan.clock, x_at[q.id, p])

        def body():
            arrived(here, lx.at[q.id, p])
            for k, peer in enumerate(a_peers):
                send(here, here, zs.at[q.id, p, k], zr.at[q.id, p, k], dev(a_=peer))

        on(home, body)
        plan.add(plan.clock, functools.partial(go_y, q, p, 0))
        for k in range(na - 1):
            when = link_of("z", home, q.unit * na / (na - 1))
            plan.add(when + ZLAG * p, functools.partial(go_y, q, p, k + 1))

    def source_row(k):
        return a if k == 0 else a_from[k - 1]

    def go_y(q, p, k):
        here = win(q, wref[q.kind], (p,), source_row(k), b, t)
        home = q.home(p)

        def body():
            if k:
                arrived(here, zr.at[q.id, p, k - 1])
            for j, peer in enumerate(b_peers):
                send(here, here, ys.at[q.id, p, k, j], yr.at[q.id, p, k, j], dev(b_=peer))

        on(home, body)
        for j in range(nb - 1):
            when = link_of("y", home, q.unit)
        plan.add(when, functools.partial(go_c, q, p, k))

    def to_core(q, p, k):
        here = win(q, wref[q.kind], (p,), source_row(k), ALL, t)
        for j, peer in enumerate(c_peers):
            send(here, here, cs.at[q.id, p, k, j], cr.at[q.id, p, k, j], dev(t_=peer))

    def core_time(q, p):
        when = plan.link("c", q.unit * nb / nt, CORE_LINK, CORE_HOP)
        ready_at[q.id, p] = max(when, ready_at.get((q.id, p), 0.0))
        steps_left[q.id, p] -= 1

    def go_c(q, p, k):
        home = q.home(p)

        def body():
            for j, source in enumerate(b_from):
                arrived(win(q, wref[q.kind], (p,), source_row(k), source, t), yr.at[q.id, p, k, j])
            if home is not None:
                here = win(q, wref[q.kind], (p,), source_row(k), ALL, t)
                send(here, here, r.ws.at[q.id, p, k], r.wr.at[q.id, p, k], dev(s_=other(home)))
            to_core(q, p, k)

        on(home, body)
        core_time(q, p)
        if home is not None:
            when = plan.link(f"x{home}", q.unit * nb, LINK, HOP)
            plan.add(when, functools.partial(go_w, q, p, k))

    def go_w(q, p, k):
        def body():
            arrived(win(q, wref[q.kind], (p,), source_row(k), ALL, t), r.wr.at[q.id, p, k])
            to_core(q, p, k)

        on(other(q.home(p)), body)
        core_time(q, p)

    def concerns(group, p, step):
        args = getattr(step, "args", ())
        if step.func is next_z:
            return any(q in group and e == p for q, e in order[args[0] :])
        return len(args) > 1 and args[1] == p and args[0] in group

    def need(kind, p, index=None):
        group = [q for q in pieces if q.kind == kind or (kind == FC1 and q.kind == FC2)]
        mine = [q for q in pieces if q.kind == kind and index in (None, q.index)]
        while any(steps_left[q.id, p] for q in mine):
            plan.pop()
        for q in mine:
            plan.clock = max(plan.clock, ready_at[q.id, p])
            for k in range(na):
                for j, source in enumerate(c_from):
                    arrived(win(q, wref[q.kind], (p,), source_row(k), ALL, source), cr.at[q.id, p, k, j])

    def gather_sent():
        for q in pieces:
            for p in range(ns):
                home = q.home(p)
                here = win(q, wref[q.kind], (p,), a, b, t)

                if home != p:

                    @pl.when(s == p)
                    def _():
                        arrived(own_shard(q), xs.at[q.id])

                def plane():
                    for k in range(na - 1):
                        arrived(here, zs.at[q.id, p, k])
                    for k in range(na):
                        for j in range(nb - 1):
                            arrived(here, ys.at[q.id, p, k, j])
                        if home is not None:
                            arrived(win(q, wref[q.kind], (p,), a, ALL, t), r.ws.at[q.id, p, k])

                on(home, plane)
                for k in range(na):
                    for j in range(nt - 1):
                        arrived(win(q, wref[q.kind], (p,), a, ALL, t), cs.at[q.id, p, k, j])

    def run(lo, hi, cost, body, before=None):
        def one(i, carry):
            for k in range(lo, hi):
                if before is not None or plan.due(plan.clock):

                    @pl.when(i == k)
                    def _():
                        plan.until(plan.clock)
                        if before is not None:
                            before(k)

                plan.clock += cost

            body(i)
            return carry

        lax.fori_loop(lo, hi, one, 0)
        plan.until(plan.clock)

    def spent(cost):
        plan.until(plan.clock + cost)

    SMF = r.smf
    P0, P1, P2 = r.p0, r.p1, r.p2
    small_ready = []

    def small_start():
        P0[s] = r.sm_in[...]
        for k, peer in enumerate(x_peers):
            send(r.sm_in, P0.at[s], r.ps.at[0, k], r.psr.at[0, k], dev(s_=peer))
        plan.add(plan.link("x0", P0.size * nt, LINK, HOP), small_a)

    def small_part(src, dst, level, targets):
        for k, target in enumerate(targets):
            send(src, dst.at[k], r.ps.at[level, k], r.psr.at[level, k], target)

    def small_sum(base, takes, level):
        total = base[...].astype(f32)
        for k in range(takes.shape[0]):
            arrived(takes.at[k], r.psr.at[level, k])
            total = total + takes[k].astype(f32)
        return total

    def small_a():
        for k, source in enumerate(x_from):
            arrived(P0.at[source], r.psr.at[0, k])
        small_part(P0, r.pa, 1, [dev(a_=p) for p in a_peers])
        for h in range(ns):
            when = plan.link(f"z{h}", P0.size * 2 * nt * na + SKEW * LINK, LINK, HOP)
        plan.add(when, small_b)

    def small_b():
        P1[...] = small_sum(P0, r.pa, 1).astype(bf16)
        small_part(P1, r.pb, 2, [dev(b_=p) for p in b_peers])
        plan.add(plan.link("y0", P0.size * 2 * nt, LINK, HOP), small_c)

    def small_c():
        P2[...] = small_sum(P1, r.pb, 2).astype(bf16)
        small_part(P2, r.pc, 3, [dev(t_=p) for p in c_peers])
        plan.add(plan.clock + CORE_HOP, small_d)

    def small_d():
        SMF[...] = small_sum(P2, r.pc, 3)
        small_ready.append(True)

    def need_small():
        while not small_ready:
            plan.pop()

    def small_sent():
        arrived(r.sm_in, r.ps.at[0, 0])
        for level, takes in ((1, r.pa), (2, r.pb), (3, r.pc)):
            for k in range(takes.shape[0]):
                arrived(takes.at[k], r.ps.at[level, k])

    group = s * nt + t

    def group_images(g):
        return pl.ds(g * ni, ni)

    barrier = pltpu.get_barrier_semaphore()
    peers = (
        [dev(a_=p) for p in a_peers]
        + [dev(b_=p) for p in b_peers]
        + [dev(t_=p) for p in c_peers]
        + [dev(s_=p) for p in x_peers]
        + [dev(s_=p, t_=q) for p in x_peers for q in c_peers]
    )
    for p in peers:
        pl.semaphore_signal(barrier, inc=1, device_id=p, device_id_type=MESH)
    pl.semaphore_wait(barrier, len(peers))

    tbl = r.tbl
    pltpu.make_async_copy(r.tbl_in, tbl.at[s, t], r.tx.at[s]).start()
    for k, peer in enumerate(x_peers):
        send(r.tbl_in, tbl.at[s, t], r.txs.at[k], r.tx.at[s], dev(s_=peer))
    small_start()
    for q in pieces:
        start_x(q)
    xin = r.outb
    for j, src in enumerate((r.images, r.cotangent)):
        pltpu.make_async_copy(src.at[group_images(group)], xin.at[j, t], r.xl.at[j]).start()
        for k, peer in enumerate(c_peers):
            send(
                src.at[group_images(s * nt + peer)],
                xin.at[j, t],
                r.xcs.at[j, k],
                r.xcr.at[j, k],
                dev(t_=peer),
            )

    def image_ready(j):
        arrived(xin.at[j, t], r.xl.at[j])
        for k, source in enumerate(c_from):
            arrived(xin.at[j, source], r.xcr.at[j, k])

    pad_rows = jnp.zeros((z.hp - z.half, z.d), f32)

    def load_rows(j, ref):
        def one(i, _):
            pieces = []
            for h in range(nt):
                pieces.append(xin[j, h, i].astype(f32))
                if z.hp > z.half:
                    pieces.append(pad_rows)
            ref[block(i, rows), :] = jnp.concatenate(pieces, 0).astype(ref.dtype)
            return 0

        lax.fori_loop(0, ni, one, 0)

    outb = r.outb

    ships = {}

    def ship(kind, p, slot, i):
        out = r.act if kind == 0 else r.ig
        for h in range(nt):
            target = out.at[group * ni + i]
            mine = jnp.logical_and(s == p, t == h)

            @pl.when(mine)
            def _():
                pltpu.make_async_copy(outb.at[slot, h, i], target, r.os.at[kind, p, h]).start()

            @pl.when(jnp.logical_not(mine))
            def _():
                remote(
                    outb.at[slot, h, i], target, r.os.at[kind, p, h], r.orr.at[kind, group], (p, d, h)
                ).start()

        plan.link(f"x{other(p)}", rows * z.d * 2 * nt, LINK, HOP)
        ships[kind, p] = ships.get((kind, p), 0) + 1

    def ship_later(kind, p, slot, times):
        for i in range(ni):
            plan.add(plan.clock + times[i % len(times)], functools.partial(ship, kind, p, slot, i))

    def shipped(kind, p, slot):
        while ships.get((kind, p), 0) < ni:
            plan.pop()
        for h in range(nt):
            arrived(outb.at[slot, h], r.os.at[kind, p, h])

    def received(kind):
        out = r.act if kind == 0 else r.ig
        for g in range(ns * nt):

            @pl.when(g != group)
            def _():
                arrived(out.at[group_images(g)], r.orr.at[kind, g])

    def stage_out(value, i, slot):
        for h in range(nt):
            outb[slot, h, i] = value[h * z.hp : h * z.hp + z.half].astype(bf16)

    width = z.d // nt

    def w_qkv(p, c, part):
        return r.wq[p, c, part].reshape(z.d, width)

    def q_part(part):
        return slice(part * width, (part + 1) * width)

    def w_proj(p):
        return r.wp[p].reshape(z.d, z.d)

    w1_all = r.w1.reshape(2, z.nch, na, nb, r.w1.shape[-2], CH)

    def w_fc1(p, c):
        return w1_all[p, c].reshape(z.d, CH)

    w2_per = CH // r.w2.shape[-2]
    w2_all = r.w2.reshape(2, z.nch, w2_per, r.w2.shape[-2], z.d)

    def w_fc2(p, c):
        return w2_all[p, c].reshape(CH, z.d)

    def row(p, k):
        return SMF[p, pl.ds(k, 1), :]

    def masks(dtype):
        lane = lax.broadcasted_iota(jnp.int32, (WP, 128), 1) // z.hd
        return [(lane == h).astype(dtype) for h in range(z.quad)]

    def spread(v, mk):
        return jnp.concatenate([v * q for q in mk], 0)

    def collect(v, mk):
        acc = v[0:WP] * mk[0]
        for h in range(1, z.quad):
            acc = acc + v[h * WP : (h + 1) * WP] * mk[h]
        return acc

    BM = r.bm
    lanes = 128
    per_lane = lanes // WP

    def build_bias(p):
        j = lax.broadcasted_iota(jnp.int32, (WP, lanes), 0)
        lane = lax.broadcasted_iota(jnp.int32, (WP, lanes), 1)
        i = lax.rem(lane, WP)
        iy, ix, jy, jx = i // WIN, lax.rem(i, WIN), j // WIN, lax.rem(j, WIN)
        valid = jnp.logical_and(i < WT, j < WT)
        index = (iy - jy + WIN - 1) * TABLE_SIDE + ix - jx + WIN - 1
        index = jnp.where(valid, index, 0)
        low = jnp.where(index < lanes, index, 0)
        high = jnp.where(index < lanes, 0, index - lanes)
        head_of_lane = lane // WP
        tables = tbl.reshape(2, HEADS, TABLE_PAD)

        def look(head):
            entry = tables[p, pl.ds(head, 1), :]
            one = jnp.take_along_axis(jnp.broadcast_to(entry[:, :lanes], (WP, lanes)), low, axis=1)
            two = jnp.take_along_axis(jnp.broadcast_to(entry[:, lanes:], (WP, lanes)), high, axis=1)
            return jnp.where(index < lanes, one, two)

        def region(q, wy):
            first = jnp.zeros_like(q)
            if wy < ACROSS - 1:
                return first
            return jnp.where(q < WIN - SHIFT, first + 1, first + 2)

        def group_of_heads(g, carry):
            for c in range(z.quad // per_lane):
                value = look(g * z.quad + c * per_lane)
                for e in range(1, per_lane):
                    value = jnp.where(head_of_lane == e, look(g * z.quad + c * per_lane + e), value)
                value = jnp.where(j < WT, value, -1e30)
                for w in range(NW if p else 1):
                    out = value
                    if p == 1:
                        wy, wx = w // ACROSS, w % ACROSS
                        label_i = region(iy, wy) * 3 + region(ix, wx)
                        label_j = region(jy, wy) * 3 + region(jx, wx)
                        out = out + jnp.where(
                            jnp.logical_and(valid, label_i != label_j), MASK_FILL, 0.0
                        )
                    BM[p + w, g, :, c * lanes : (c + 1) * lanes] = out
            return carry

        lax.fori_loop(0, z.ng, group_of_heads, 0)

    X, G = r.mg, r.g
    PM, PMT = r.pm, r.pmt
    FN, N1, K = r.fn, r.n1, r.k
    QK, PR, CTX, CTXT = r.qk, r.pr, r.ctx, r.ctxt
    MID, MG, SN, N2, ACT, SL = r.mid, r.mg, r.sn, r.n2, r.actv, r.sl
    SG, DB = r.sg, r.db

    def forward(p):
        need_small()

        def ln1(i):
            n, inv = normalize(X[block(i, rows), :])
            N1[p, block(i, rows), :] = n.astype(bf16)
            K[block(i, rows), 2 * p : 2 * p + 1] = inv
            f = (n * row(p, 0) + row(p, 1)).astype(bf16)
            FN[p, block(i, rows), :] = f
            CTX[block(i, NW * WP), :] = dotf(PM[p], f, NN).astype(bf16)

        run(0, ni, 0.45, ln1)

        def qkv(c):
            for e in range(nt):
                bias = row(p, 6 + c)[:, q_part(e)]
                QK[p, c, :, q_part(e)] = (dotf(CTX[...], w_qkv(p, c, e), NN) + bias).astype(bf16)

        need(QKV, p)
        run(0, 3, 0.7, qkv)

        def attention(i):
            mb, mf = masks(bf16), masks(f32)
            units = [(i * BATCH + e, g) for e in range(BATCH) for g in range(z.ng)]
            at = [(block(u, WP), slice(g * 128, (g + 1) * 128)) for u, g in units]
            raw = [dotf(QK[p, 1, S, L], spread(QK[p, 0, S, L], mb), NT) for S, L in at]
            prs = []
            for (u, g), sc in zip(units, raw):
                w = 1 + lax.rem(u, NW) if p else 0
                sc = sc * z.scaling + BM[w, g]
                e = jnp.exp(sc - jnp.max(sc, 0, keepdims=True))
                pr = (e * (1.0 / jnp.sum(e, 0, keepdims=True))).astype(bf16)
                PR[p, u, g] = pr
                prs.append(pr)
            mixed = [dotf(pr, QK[p, 2, S, L], TN) for pr, (S, L) in zip(prs, at)]
            for v, (S, L) in zip(mixed, at):
                CTX[S, L] = collect(v, mf).astype(bf16)

        run(0, ni * NW // BATCH, 0.72, attention)

        def unperm(i):
            CTXT[p, block(i, rows), :] = dotf(PMT[p], CTX[block(i, NW * WP), :], NN).astype(bf16)

        run(0, ni, 0.21, unperm)
        need(PROJ, p)
        MID[...] = dotf(CTXT[p], w_proj(p), NN)
        spent(0.6)

        def ln2(i):
            mid = X[block(i, rows), :] + MID[block(i, rows), :] + row(p, 2)
            MID[block(i, rows), :] = mid
            n, inv = normalize(mid)
            N2[p, block(i, rows), :] = n.astype(bf16)
            K[block(i, rows), 2 * p + 1 : 2 * p + 2] = inv
            SN[p, block(i, rows), :] = (n * row(p, 3) + row(p, 4)).astype(bf16)

        run(0, ni, 0.26, ln2)
        if p == 1:
            for j, ref in enumerate((ACT, SL)):
                arrived(ref, r.sp.at[j])
        per = z.nch // 2

        for j in range(2):
            need(FC1, p, j)

            def rise(i):
                c = j + 2 * i
                u = dotf(SN[p], w_fc1(p, c), NN) + row(p, 9 + c)
                e = 0.5 * (1.0 + lax.erf(u * ROOT_HALF))
                ACT[c] = (u * e).astype(bf16)
                SL[c] = (e + u * jnp.exp(-0.5 * u * u) * INV_ROOT_TWO_PI).astype(bf16)

            run(0, per, 1.16, rise)
        need(FC2, p)

        def fall(c):
            MID[...] += dotf(ACT[c], w_fc2(p, c), NN)

        run(0, z.nch, 0.6, fall)
        if p == 0:
            for j, ref in enumerate((ACT, SL)):
                pltpu.make_async_copy(ref, r.spill.at[j], r.sp.at[j]).start()

        def finish(i):
            value = MID[block(i, rows), :] + row(p, 5)
            X[block(i, rows), :] = value.astype(bf16).astype(f32)
            stage_out(value, i, p)

        run(0, ni, 0.05, finish)
        ship_later(0, p, p, (9.0, 14.0, 19.0, 24.0) if p == 0 else (0.0, 5.0, 10.0, 15.0))

    g1_own = r.g1.reshape(z.nch, *w1_all.shape[2:])
    g2_own = r.g2.reshape(z.nch, *w2_all.shape[2:])

    def backward(p):
        gq, gp, g1, g2 = (
            (r.gq, r.gp, g1_own, g2_own) if p else (r.wq.at[1], r.wp.at[1], w1_all.at[1], w2_all.at[1])
        )
        def addrow(k, v):
            SG[p, pl.ds(k, 1), 0 : z.d] = SG[p, pl.ds(k, 1), 0 : z.d] + v

        SG[p] = jnp.zeros(SG.shape[1:], f32)
        DB[...] = jnp.zeros(DB.shape, f32)
        if p == 0:
            for j, ref in enumerate((ACT, SL)):
                arrived(ref, r.sp.at[j])
            gather_sent()

        def fc2_grad(c):
            g2[c] = dotf(ACT[c], G[...], TN).astype(bf16).reshape(g2.shape[1:])

        run(0, z.nch, 0.62, fc2_grad)
        emit(FC2, p)

        def hidden(c):
            hg = dotf(G[...], w_fc2(p, c), NT) * SL[c].astype(f32)
            SG[p, pl.ds(9 + c, 1), 0 : z.d] = column_sum(hg)
            SL[c] = hg.astype(bf16)

        run(0, z.nch, 0.65, hidden)

        def fc1(c):
            g1[c] = dotf(SN[p], SL[c], TN).astype(bf16).reshape(g1.shape[1:])

        run(0, z.nch, 0.75, fc1)
        MID[...] = jnp.zeros(MID.shape, f32)
        emit(FC1, p)

        def n2g(c):
            MID[...] += dotf(SL[c], w_fc1(p, c), NT)

        run(0, z.nch, 0.65, n2g)
        if p == 1:
            for j, ref in enumerate((ACT, SL)):
                pltpu.make_async_copy(r.spill.at[j], ref, r.sp.at[j]).start()

        def ln2(i):
            sl = block(i, rows)
            ng = MID[sl, :]
            n = N2[p, sl, :].astype(f32)
            g = G[sl, :].astype(f32)
            mg = g + norm_pull(ng, n, K[sl, 2 * p + 1 : 2 * p + 2], row(p, 3))
            MG[sl, :] = mg
            addrow(5, column_sum(g))
            addrow(3, column_sum(ng * n))
            addrow(4, column_sum(ng))
            addrow(2, column_sum(mg))
            G[sl, :] = mg.astype(bf16)

        run(0, ni, 0.31, ln2)
        gp[...] = dotf(CTXT[p], G[...], TN).astype(bf16).reshape(gp.shape)
        CTXT[p] = dotf(G[...], w_proj(p), NT).astype(bf16)
        spent(1.2)

        def cgrad(i):
            CTX[block(i, NW * WP), :] = dotf(PM[p], CTXT[p, block(i, rows), :], NN).astype(bf16)

        run(0, ni, 0.23, cgrad)
        emit(PROJ, p)

        def attention(i):
            mb, mf = masks(bf16), masks(f32)
            units = [(i * BATCH + e, g) for e in range(BATCH) for g in range(z.ng)]
            at = [(block(u, WP), slice(g * 128, (g + 1) * 128)) for u, g in units]
            cbd = [spread(CTX[S, L], mb) for S, L in at]
            dps = [dotf(QK[p, 2, S, L], c, NT) for (S, L), c in zip(at, cbd)]
            dvs = [dotf(PR[p, u, g], c, NN) for (u, g), c in zip(units, cbd)]
            sbs = []
            for (u, g), dp in zip(units, dps):
                pf = PR[p, u, g].astype(f32)
                tt = pf * dp
                sc = tt - pf * jnp.sum(tt, 0, keepdims=True)
                DB[g] = DB[g] + sc
                sbs.append(sc.astype(bf16))
            for v, (S, L) in zip(dvs, at):
                QK[p, 2, S, L] = v.astype(bf16)
            dks = [dotf(sb, spread(QK[p, 0, S, L], mb), NN) for sb, (S, L) in zip(sbs, at)]
            dqs = [dotf(sb, QK[p, 1, S, L], TN) for sb, (S, L) in zip(sbs, at)]
            for dk, dq, (S, L) in zip(dks, dqs, at):
                QK[p, 1, S, L] = (dk * z.scaling).astype(bf16)
                QK[p, 0, S, L] = (collect(dq, mf) * z.scaling).astype(bf16)

        def un(c, i):
            dv = dotf(PMT[p], QK[p, c, block(i, NW * WP), :], NN)
            addrow(6 + c, column_sum(dv))
            QK[p, c, block(i, rows), :] = dv.astype(bf16)

        def qkv_grad(c):
            value = dotf(FN[p], QK[p, c, 0:m, :], TN).astype(bf16)
            for e in range(nt):
                gq[c, e] = value[:, q_part(e)].reshape(gq.shape[2:])

        def emit_last(k):
            if k:
                emit(QKV, p, k - 1)

        def pull(sl, c):
            return sum(dotf(QK[p, c, sl, q_part(e)], w_qkv(p, c, e), NT) for e in range(nt))

        def ln1(i):
            sl = block(i, rows)
            ng = pull(sl, 0) + pull(sl, 1) + pull(sl, 2)
            n = N1[p, sl, :].astype(f32)
            xg = MG[sl, :] + norm_pull(ng, n, K[sl, 2 * p : 2 * p + 1], row(p, 0))
            addrow(0, column_sum(ng * n))
            addrow(1, column_sum(ng))
            if p:
                G[sl, :] = xg.astype(bf16)
            stage_out(xg, i, 1 - p)

        shipped(0, 1 - p, 1 - p)
        per = NW // BATCH
        cost = 1.6

        def image_step(k):
            attention(k)

            @pl.when(lax.rem(k, per) == per - 1)
            def _():
                for c in range(3):
                    un(c, k // per)
                ln1(k // per)

        first = per * cost
        if p == 0:
            ship_later(1, p, 1 - p, [first * (i + 1) for i in range(ni)])
        else:
            ship_later(1, p, 1 - p, [first * ni + 4.0 + 5.0 * i for i in range(ni)])
        run(0, ni * per, cost, image_step)
        run(0, 3, 0.75, qkv_grad, emit_last)
        emit(QKV, p, 2)
        table_rows(p)
        sum_send(p, 0)

    def table_rows(p):
        src = lax.broadcasted_iota(jnp.int32, (z.quad * WP, TABLE_PAD), 0)
        dst = lax.broadcasted_iota(jnp.int32, (z.quad * WP, TABLE_PAD), 1)
        i = lax.rem(src, WP)
        place = jnp.logical_and(
            i < WT, dst == CENTER - ((i // WIN) * TABLE_SIDE + lax.rem(i, WIN))
        )
        head = src // WP
        pick = jnp.concatenate(
            [jnp.logical_and(place, head == h).astype(bf16) for h in range(z.quad)], 1
        )
        group_row = lax.broadcasted_iota(jnp.int32, (8, WP), 0)
        group_of = lax.broadcasted_iota(jnp.int32, (8, WP), 1)
        rows_of = jnp.logical_and(group_of < WT, group_of // WIN == group_row).astype(bf16)

        def split_dot(x, y, left):
            big = x if left else y
            hi = big.astype(bf16)
            lo = (big - hi.astype(f32)).astype(bf16)
            if left:
                return dotf(hi, y, NN) + dotf(lo, y, NN)
            return dotf(x, hi, NN) + dotf(x, lo, NN)

        def one_group(g):
            e = split_dot(DB[g], pick, True)
            for h in range(z.quad):
                v = e[:, h * TABLE_PAD : (h + 1) * TABLE_PAD]
                v = pltpu.roll(v, 0, 1, stride=1, stride_axis=0)
                v = split_dot(rows_of, v, False)
                v = pltpu.roll(v, 0, 1, stride=TABLE_SIDE - WIN, stride_axis=0)
                SG[p, pl.ds(g * z.quad + h, 1), z.d :] = column_sum(v)

        run(0, z.ng, 0.4, one_group)

    gref = {QKV: r.gq, PROJ: r.gp, FC1: r.g1, FC2: r.g2}
    s1, v1, s2, v2, s3, v3, s4, v4 = (r.s1, r.v1, r.s2, r.v2, r.s3, r.v3, r.s4, r.v4)
    k1, k2, k3 = r.k1, r.k2, r.k3
    done = {}

    def buffer(level, q):
        return getattr(r, f"r{level}_{q.id}")

    def gwin(q, p, a_, b_, t_):
        if p == 0:
            return win(q, wref[q.kind], (1,), a_, b_, t_)
        return win(q, gref[q.kind], (), a_, b_, t_)

    def gout(q):
        return shard(q, r.gq_out, r.gp_out, r.g1_out, r.g2_out)

    def reached(q, p, level):
        while done.get((q.id, p), 0) < level:
            plan.pop()

    def credit(sem, q, k, p, device):
        if p == 1:
            pl.semaphore_signal(sem.at[q.id, k], inc=1, device_id=device, device_id_type=MESH)

    def spend(sem, q, k, p):
        if p == 0:
            pl.semaphore_wait(sem.at[q.id, k], 1)

    def emit(kind, p, index=None):
        for q in pieces:
            if q.kind == kind and index in (None, q.index):
                r1(q, p)

    def r1(q, p):
        if p == 0:
            reached(q, 1, 2)
        for k, peer in enumerate(c_peers):
            spend(k1, q, k, p)
            send(gwin(q, p, ALL, ALL, peer), buffer(1, q).at[k], s1.at[p, q.id, k], v1.at[p, q.id, k], dev(t_=peer))
            when = plan.link("c", q.unit * na * nb / nt, CORE_LINK, CORE_HOP)
        done[q.id, p] = 1
        plan.add(when, functools.partial(r2, q, p))

    def r2(q, p):
        if p == 0:
            reached(q, 1, 3)
        for k in range(nt - 1):
            arrived(buffer(1, q).at[k], v1.at[p, q.id, k])
        mine = gwin(q, p, ALL, ALL, t)
        add_into(mine, [buffer(1, q).at[k] for k in range(nt - 1)])
        for k, source in enumerate(c_from):
            credit(k1, q, k, p, dev(t_=source))
        plan.clock += q.unit * na * nb / 10e6
        done[q.id, p] = 2
        home = q.sum_home(p)
        if home is None:
            to_y(q, p)
            return

        @pl.when(s != home)
        def _():
            spend(r.k6, q, 0, p)
            send(mine, buffer(6, q), r.s6.at[p, q.id], r.v6.at[p, q.id], dev(s_=home))

        when = plan.link(f"x{other(home)}", q.unit * na * nb, LINK, HOP)
        plan.add(when, functools.partial(r2x, q, p))

    def r2x(q, p):
        home = q.sum_home(p)

        def body():
            arrived(buffer(6, q), r.v6.at[p, q.id])
            add_into(gwin(q, p, ALL, ALL, t), [buffer(6, q)])
            credit(r.k6, q, 0, p, dev(s_=other(home)))

        on(home, body)
        plan.clock += q.unit * na * nb / 10e6
        to_y(q, p)

    def to_y(q, p):
        home = q.sum_home(p)

        def body():
            for k, peer in enumerate(b_peers):
                spend(k2, q, k, p)
                send(
                    gwin(q, p, ALL, peer, t),
                    buffer(2, q).at[k],
                    s2.at[p, q.id, k],
                    v2.at[p, q.id, k],
                    dev(b_=peer),
                )

        on(home, body)
        for k in range(nb - 1):
            when = link_of("y", home, q.unit * na)
        plan.add(when, functools.partial(r3, q, p))

    def r3(q, p):
        if p == 0:
            reached(q, 1, 4)
        home = q.sum_home(p)

        def body():
            for k in range(nb - 1):
                arrived(buffer(2, q).at[k], v2.at[p, q.id, k])
            add_into(gwin(q, p, ALL, b, t), [buffer(2, q).at[k] for k in range(nb - 1)])
            for k, source in enumerate(b_from):
                credit(k2, q, k, p, dev(b_=source))
            for k, peer in enumerate(a_peers):
                spend(k3, q, k, p)
                send(
                    gwin(q, p, peer, b, t),
                    buffer(3, q).at[k],
                    s3.at[p, q.id, k],
                    v3.at[p, q.id, k],
                    dev(a_=peer),
                )

        on(home, body)
        for k in range(na - 1):
            when = link_of("z", home, q.unit * na / (na - 1))
        done[q.id, p] = 3
        plan.add(when, functools.partial(r4, q, p))

    def r4(q, p):
        if p == 0:
            reached(q, 1, 5)
        home = q.sum_home(p)
        mine = gwin(q, p, a, b, t)

        def summed():
            for k in range(na - 1):
                arrived(buffer(3, q).at[k], v3.at[p, q.id, k])
            total = mine[...].astype(f32)
            for k in range(na - 1):
                total = total + buffer(3, q)[k].astype(f32)
            for k, source in enumerate(a_from):
                credit(k3, q, k, p, dev(a_=source))
            return total

        def keep(total):
            gout(q)[...] = total

        def pass_on(total):
            buffer(5, q)[...] = total.astype(bf16)
            remote(buffer(5, q), buffer(4, q), s4.at[p, q.id], v4.at[p, q.id], dev(s_=p)).start()

        if home is None:
            total = summed()
            pl.when(s == p)(functools.partial(keep, total))
            pl.when(s != p)(functools.partial(pass_on, total))
        else:

            @pl.when(s == home)
            def _():
                (keep if home == p else pass_on)(summed())

        if home == p:
            done[q.id, p] = 5
            return
        done[q.id, p] = 4
        plan.add(plan.link(f"x{other(p)}", q.unit, LINK, HOP), functools.partial(r5, q, p))

    def r5(q, p):
        home = q.sum_home(p)

        @pl.when(s == p)
        def _():
            arrived(buffer(4, q), v4.at[p, q.id])
            out = gout(q)
            value = buffer(4, q)[...].astype(f32)
            out[...] = value if home is not None else out[...] + value

        @pl.when(s != p)
        def _():
            arrived(buffer(5, q), s4.at[p, q.id])

        done[q.id, p] = 5

    def settle(q, p):
        home = q.sum_home(p)
        for k, peer in enumerate(c_peers):
            arrived(gwin(q, p, ALL, ALL, peer), s1.at[p, q.id, k])

        def plane():
            for k, peer in enumerate(b_peers):
                arrived(gwin(q, p, ALL, peer, t), s2.at[p, q.id, k])
            for k, peer in enumerate(a_peers):
                arrived(gwin(q, p, peer, b, t), s3.at[p, q.id, k])

        on(home, plane)
        if home is not None:

            @pl.when(s != home)
            def _():
                arrived(gwin(q, p, ALL, ALL, t), r.s6.at[p, q.id])

    def add_into(mine, others):
        lead = mine.shape[:-2]
        count = int(np.prod(lead))

        def one(i, _):
            index = []
            rest = i
            for extent in reversed(lead):
                index.append(lax.rem(rest, extent))
                rest = rest // extent
            index = tuple(reversed(index))
            total = mine[index].astype(f32)
            for o in others:
                total = total + o[index].astype(f32)
            mine[index] = total.astype(bf16)
            return 0

        lax.fori_loop(0, count, one, 0)

    lists = [
        [dev(t_=p) for p in c_peers],
        [dev(b_=p) for p in b_peers],
        [dev(a_=p) for p in a_peers],
    ]
    takes = [r.ra, r.rc, r.rd]
    ss, sv = r.ss, r.sv

    def sum_send(p, k):
        if k == 0:
            r.sums[p, 0] = SG[p].astype(bf16)
        src = r.sums.at[p, k]
        if k < 3:
            for j, target in enumerate(lists[k]):
                send(src, takes[k].at[p, j], ss.at[p, k, j], sv.at[p, k, j], target)
        else:

            @pl.when(s != p)
            def _():
                send(src, r.rb, ss.at[p, k, 0], sv.at[p, k, 0], dev(s_=p))

        size = SG.size * nt * (na if k == 2 else 1)
        link = ("c", "y", "z", f"x{other(p)}")[k]
        when = link_of(link, None, size) if k in (1, 2) else plan.link(link, size, LINK, HOP)
        plan.add(when, functools.partial(sum_take, p, k))

    def sum_take(p, k):
        total = r.sums[p, k].astype(f32)
        if k < 3:
            for j in range(len(lists[k])):
                arrived(takes[k].at[p, j], sv.at[p, k, j])
                total = total + takes[k][p, j].astype(f32)
            r.sums[p, k + 1] = total.astype(bf16)
            sum_send(p, k + 1)
        else:

            @pl.when(s == p)
            def _():
                arrived(r.rb, sv.at[p, k, 0])
                r.small_out[...] = total + r.rb[...].astype(f32)

    def sums_sent():
        for p in range(ns):
            for k in range(3):
                for j in range(len(lists[k])):
                    arrived(r.sums.at[p, k], ss.at[p, k, j])

            @pl.when(s != p)
            def _():
                arrived(r.sums.at[p, 3], ss.at[p, 3, 0])

    def is_sum(step, names):
        return step.func is sum_take and (r3 in names and step.args[1] < 2 or r4 in names)

    first = [q for q in pieces if q.kind == QKV]
    plan.pop()
    for q in first:
        go_z(q, 0)
    plan.until(plan.clock)
    proj = [q for q in pieces if q.kind == PROJ]
    mixed = [q for k in range(2) for q in pieces if q.kind in (FC1, FC2) and q.index == k]
    order = [(q, 0) for q in proj + mixed] + [(q, 1) for q in first + proj + mixed]

    def z_free(q, p):
        return max(plan.free.get(f"z{h}", 0.0) for h in planes(q.home(p)))

    def next_z(k):
        q, p = order[k]
        go_z(q, p)
        if k + 1 < len(order):
            after = order[k + 1]
            plan.add(
                max(x_at[after[0].id, after[1]], z_free(*after) - 8.0), functools.partial(next_z, k + 1)
            )

    plan.add(x_at[order[0][0].id, 0], functools.partial(next_z, 0))
    for q in range(ns):
        arrived(tbl.at[q, t], r.tx.at[q])
        for k, peer in enumerate(c_peers):
            send(tbl.at[q, t], tbl.at[q, t], r.tcs.at[q, k], r.tcr.at[q, k], dev(t_=peer))
    spent(0.5)
    image_ready(0)
    load_rows(0, X)
    spent(0.3)
    for q in range(ns):
        for k, source in enumerate(c_from):
            arrived(tbl.at[q, source], r.tcr.at[q, k])
    for p in range(2):
        build_bias(p)
        spent(0.7)
    image_ready(1)
    load_rows(1, G)
    spent(0.2)

    for p in range(2):
        forward(p)
    for p in (1, 0):
        backward(p)

    for steps_of in ((r1, r2, r2x, r3), (r4,), (r5, sum_take)):
        while plan.pop_of(lambda step: step.func in steps_of or is_sum(step, steps_of)):
            pass

    for q in pieces:
        for p in range(2):
            settle(q, p)
    small_sent()
    received(0)
    received(1)
    shipped(1, 1, 0)
    shipped(1, 0, 1)
    for k in range(ns - 1):
        arrived(r.tbl_in, r.txs.at[k])
    for q in range(ns):
        for k in range(nt - 1):
            arrived(tbl.at[q, t], r.tcs.at[q, k])
    for j, src in enumerate((r.images, r.cotangent)):
        for k in range(nt - 1):
            arrived(outb.at[j, t], r.xcs.at[j, k])
    sums_sent()


def per_device(z, images, cotangent, norm1_gain, norm1_bias, qkv_weight, qkv_bias, position_table,
               proj_weight, proj_bias, norm2_gain, norm2_bias, fc1_weight, fc1_bias, fc2_weight,
               fc2_bias):
    s = lax.axis_index(SECTION)
    d = lax.axis_index(DP)
    t = lax.axis_index(TENSOR)
    D, nt, na, nb, ns, ni = z.d, z.parts, z.na, z.nb, z.sections, z.ni
    part = t * z.dp + d

    def spread_to(values, width, at):
        blank = jnp.zeros((values.shape[0], width), bf16)
        return lax.dynamic_update_slice(blank, values, (0, at))

    vectors = jnp.concatenate(
        [norm1_gain, norm1_bias, proj_bias, norm2_gain, norm2_bias, fc2_bias], 0
    )
    vectors = jnp.where(t == 0, vectors, jnp.zeros_like(vectors))
    small = jnp.concatenate(
        [
            spread_to(vectors, D, d * vectors.shape[1]),
            spread_to(qkv_bias[0], D, part * qkv_bias.shape[-1]),
            spread_to(fc1_bias, z.ff, part * fc1_bias.shape[-1]).reshape(-1, D),
        ],
        0,
    )
    small = jnp.pad(small, ((0, GATHER_ROWS - small.shape[0]), (0, 0)))
    table = jnp.pad(position_table[0].T, ((0, 0), (0, TABLE_PAD - position_table.shape[1])))
    perm = window_permutation(nt, z.half, z.hp)

    qrow, prow, f2row = qkv_weight.shape[1], proj_weight.shape[1], fc2_weight.shape[1]
    m, mw, nch = z.m, z.mw, z.nch
    S = jax.ShapeDtypeStruct
    V = pl.BlockSpec(memory_space=pltpu.VMEM)
    A = pl.BlockSpec(memory_space=pl.ANY)
    dma = pltpu.SemaphoreType.DMA
    reg = pltpu.SemaphoreType.REGULAR
    inputs = dict(
        images=(images, A),
        cotangent=(cotangent, A),
        q_in=(qkv_weight[0].transpose(1, 0, 2), A),
        p_in=(proj_weight[0], A),
        f1_in=(fc1_weight[0], A),
        f2_in=(fc2_weight[0], A),
        sm_in=(small, V),
        tbl_in=(table, V),
        pm=(jnp.asarray(perm, bf16), V),
        pmt=(jnp.asarray(perm.transpose(0, 2, 1), bf16), V),
    )
    wide = D + TABLE_PAD
    outputs = dict(
        act=(S(images.shape, bf16), A),
        ig=(S(images.shape, bf16), A),
        gq_out=(S((3, qrow, D // nt), f32), V),
        gp_out=(S((prow, D), f32), V),
        g1_out=(S((qrow, z.ff // nt), f32), V),
        g2_out=(S((f2row, D), f32), V),
        small_out=(S((GATHER_ROWS, wide), f32), V),
        spill=(S((2, nch, m, CH), bf16), A),
    )
    vm = pltpu.VMEM
    z.pieces = make_pieces(z, qrow, prow, f2row)
    W = len(z.pieces)
    scratch = dict(
        wq=vm((2, 3, nt, na, nb, qrow, D // nt), bf16),
        wp=vm((2, nt, na, nb, prow, D), bf16),
        w1=vm((2, nt, 2, na, nb, qrow, z.ff // nt // 2), bf16),
        w2=vm((2, nt, na, nb, f2row, D), bf16),
        p0=vm((2, GATHER_ROWS, D), bf16),
        p1=vm((2, GATHER_ROWS, D), bf16),
        p2=vm((2, GATHER_ROWS, D), bf16),
        pa=vm((na - 1, 2, GATHER_ROWS, D), bf16),
        pb=vm((nb - 1, 2, GATHER_ROWS, D), bf16),
        pc=vm((nt - 1, 2, GATHER_ROWS, D), bf16),
        ps=dma((4, max(na, nb, nt, ns))),
        psr=dma((4, max(na, nb, nt, ns))),
        ws=dma((W, 2, na)),
        wr=dma((W, 2, na)),
        smf=vm((2, GATHER_ROWS, D), f32),
        tbl=vm((2, nt, z.heads_part, TABLE_PAD), f32),
        outb=vm((2, nt, ni, z.half, D), bf16),
        bm=vm((1 + NW, z.ng, WP, z.quad * WP), f32),
        g=vm((m, D), bf16),
        fn=vm((2, m, D), bf16),
        n1=vm((2, m, D), bf16),
        k=vm((m, 4), f32),
        qk=vm((2, 3, mw, D), bf16),
        pr=vm((2, ni * NW, z.ng, WP, z.quad * WP), bf16),
        ctx=vm((mw, D), bf16),
        ctxt=vm((2, m, D), bf16),
        mid=vm((m, D), f32),
        mg=vm((m, D), f32),
        sn=vm((2, m, D), bf16),
        n2=vm((2, m, D), bf16),
        actv=vm((nch, m, CH), bf16),
        sl=vm((nch, m, CH), bf16),
        sg=vm((2, GATHER_ROWS, wide), f32),
        db=vm((z.ng, WP, z.quad * WP), f32),
        gq=vm((3, nt, na, nb, qrow, D // nt), bf16),
        gp=vm((nt, na, nb, prow, D), bf16),
        g1=vm((nt, 2, na, nb, qrow, z.ff // nt // 2), bf16),
        g2=vm((nt, na, nb, f2row, D), bf16),
        sums=vm((2, 4, GATHER_ROWS, wide), bf16),
        ra=vm((2, nt - 1, GATHER_ROWS, wide), bf16),
        rb=vm((GATHER_ROWS, wide), bf16),
        rc=vm((2, nb - 1, GATHER_ROWS, wide), bf16),
        rd=vm((2, na - 1, GATHER_ROWS, wide), bf16),
        lx=dma((W, ns)),
        xs=dma((W,)),
        zs=dma((W, 2, na - 1)),
        zr=dma((W, 2, na - 1)),
        ys=dma((W, 2, na, nb - 1)),
        yr=dma((W, 2, na, nb - 1)),
        cs=dma((W, 2, na, nt - 1)),
        cr=dma((W, 2, na, nt - 1)),
        tx=dma((ns,)),
        txs=dma((ns - 1,)),
        tcs=dma((ns, nt - 1)),
        tcr=dma((ns, nt - 1)),
        xl=dma((2,)),
        xcs=dma((2, nt - 1)),
        xcr=dma((2, nt - 1)),
        os=dma((2, 2, nt)),
        orr=dma((2, ns * nt)),
        sp=dma((2,)),
        s1=dma((2, W, nt - 1)),
        v1=dma((2, W, nt - 1)),
        s2=dma((2, W, nb - 1)),
        v2=dma((2, W, nb - 1)),
        s3=dma((2, W, na - 1)),
        v3=dma((2, W, na - 1)),
        s4=dma((2, W)),
        v4=dma((2, W)),
        s6=dma((2, W)),
        v6=dma((2, W)),
        k6=reg((W, 1)),
        k1=reg((W, nt - 1)),
        k2=reg((W, nb - 1)),
        k3=reg((W, na - 1)),
        ss=dma((2, 4, max(na, nb, nt, ns))),
        sv=dma((2, 4, max(na, nb, nt, ns))),
    )
    for q in z.pieces:
        scratch[f"r1_{q.id}"] = vm((nt - 1, na, nb, q.rows, q.cols), bf16)
        scratch[f"r2_{q.id}"] = vm((nb - 1, na, q.rows, q.cols), bf16)
        scratch[f"r3_{q.id}"] = vm((na - 1, q.rows, q.cols), bf16)
        scratch[f"r4_{q.id}"] = vm((q.rows, q.cols), bf16)
        scratch[f"r5_{q.id}"] = vm((q.rows, q.cols), bf16)
        if q.sum_home(0) is not None:
            scratch[f"r6_{q.id}"] = vm((na, nb, q.rows, q.cols), bf16)
    z.names = list(inputs) + list(outputs) + list(scratch)
    results = pl.pallas_call(
        functools.partial(kernel, z),
        out_shape=tuple(o for o, _ in outputs.values()),
        in_specs=[spec for _, spec in inputs.values()],
        out_specs=tuple(spec for _, spec in outputs.values()),
        scratch_shapes=list(scratch.values()),
        compiler_params=pltpu.CompilerParams(
            collective_id=0, has_side_effects=True, vmem_limit_bytes=67043328
        ),
        name="two_blocks",
    )(*[x for x, _ in inputs.values()])
    act, ig, gq, gp, g1, g2, sums, _ = results

    def own_vector(k):
        width = norm1_gain.shape[1]
        return lax.dynamic_slice(sums, (k, d * width), (1, width))

    width = qkv_bias.shape[-1]
    qkv_bias_grad = lax.dynamic_slice(sums, (6, part * width), (3, width))[None]
    width = fc1_bias.shape[1]
    fc1_flat = sums[9 : 9 + nch, :D].reshape(1, -1)
    fc1_bias_grad = lax.dynamic_slice(fc1_flat, (0, part * width), (1, width))
    tables = lax.dynamic_slice(sums, (t * z.heads_part, D), (z.heads_part, TABLE_PAD))
    tables = tables[:, : position_table.shape[1]][:, ::-1].T[None]
    return (
        act[None],
        ig[None],
        own_vector(0),
        own_vector(1),
        gq.transpose(1, 0, 2)[None],
        qkv_bias_grad,
        tables,
        gp[None],
        own_vector(2),
        own_vector(3),
        own_vector(4),
        g1[None],
        fc1_bias_grad,
        g2[None],
        own_vector(5),
    )


def solution(mesh):
    def run(*args):
        z = Sizes(mesh, args[0], args[11])
        return per_device(z, *args)

    in_specs = (
        P(DP, TENSOR, None),
        P(DP, TENSOR, None),
        P(SECTION, DP),
        P(SECTION, DP),
        P(SECTION, DP, None, TENSOR),
        P(SECTION, None, (TENSOR, DP)),
        P(SECTION, None, TENSOR),
        P(SECTION, (TENSOR, DP), None),
        P(SECTION, DP),
        P(SECTION, DP),
        P(SECTION, DP),
        P(SECTION, DP, TENSOR),
        P(SECTION, (TENSOR, DP)),
        P(SECTION, (TENSOR, DP), None),
        P(SECTION, DP),
    )
    out_specs = (
        P(SECTION, DP, TENSOR, None),
        P(SECTION, DP, TENSOR, None),
        P(SECTION, DP),
        P(SECTION, DP),
        P(SECTION, DP, None, TENSOR),
        P(SECTION, None, (TENSOR, DP)),
        P(SECTION, None, TENSOR),
        P(SECTION, (TENSOR, DP), None),
        P(SECTION, DP),
        P(SECTION, DP),
        P(SECTION, DP),
        P(SECTION, DP, TENSOR),
        P(SECTION, (TENSOR, DP)),
        P(SECTION, (TENSOR, DP), None),
        P(SECTION, DP),
    )
    return jax.shard_map(
        run, mesh=mesh, in_specs=in_specs, out_specs=out_specs, check_vma=False
    )
```

```python
import functools
import heapq
import math
import types

import jax
import jax.numpy as jnp
import numpy as np
from jax import lax
from jax.experimental import pallas as pl
from jax.experimental.pallas import tpu as pltpu
from jax.sharding import PartitionSpec as P

HEADS = 16
WIN = 7
SIDE = 14
SHIFT = 3

EPS = 1e-05
MASK_FILL = -100.0
ROOT_HALF = 0.7071067811865476
INV_ROOT_TWO_PI = 0.3989422804014327
NEG_LOG2_E = -1.4426950408889634

ACROSS = SIDE // WIN
NW = ACROSS * ACROSS
WT = WIN * WIN
WP = 64
TABLE_SIDE = 2 * WIN - 1
CENTER = (WIN - 1) * TABLE_SIDE + WIN - 1
TABLE_PAD = 256
CH = 512
GATHER_ROWS = 16
BATCH = 2

SECTION = "section"
DP = "dp"
TENSOR = "tensor"

f32 = jnp.float32
bf16 = jnp.bfloat16
MESH = pl.DeviceIdType.MESH
NN = ((1,), (0,))
NT = ((1,), (1,))
TN = ((0,), (0,))


def round_up(n, m):
    return -(-n // m) * m


def window_slots(shift):
    slot = np.zeros(SIDE * SIDE, np.int64)
    for p in range(SIDE):
        for q in range(SIDE):
            token = ((p + shift) % SIDE) * SIDE + (q + shift) % SIDE
            window = (p // WIN) * ACROSS + q // WIN
            slot[token] = window * WP + (p % WIN) * WIN + q % WIN
    return slot


def window_permutation(parts, half, padded):
    perm = np.zeros((2, NW * WP, parts * padded), np.float32)
    for block in range(2):
        for token, slot in enumerate(window_slots(SHIFT * block)):
            perm[block, slot, (token // half) * padded + token % half] = 1
    return perm


def dotf(a, b, dims):
    return lax.dot_general(a, b, (dims, ((), ())), preferred_element_type=f32)


def normalize(values):
    center = values - jnp.mean(values, -1, keepdims=True)
    inverse = lax.rsqrt(jnp.mean(center * center, -1, keepdims=True) + EPS)
    return center * inverse, inverse


def norm_pull(upstream, normed, inverse, gain):
    scaled = upstream * gain
    return inverse * (
        scaled
        - jnp.mean(scaled, -1, keepdims=True)
        - normed * jnp.mean(scaled * normed, -1, keepdims=True)
    )


def block(i, n):
    if isinstance(i, int):
        return pl.ds(i * n, n)
    return pl.ds(pl.multiple_of(i * n, n), n)


def column_sum(v):
    return jnp.sum(v, 0, keepdims=True)


class Sizes:
    def __init__(self, mesh, images, fc1_weight):
        self.sections = mesh.shape[SECTION]
        self.dp = mesh.shape[DP]
        self.parts = mesh.shape[TENSOR]
        inner = int(math.isqrt(self.dp))
        while self.dp % inner:
            inner -= 1
        self.nb = inner
        self.na = self.dp // inner
        self.local_images, self.half, self.d = images.shape
        self.ff = fc1_weight.shape[-1] * self.parts
        self.ni = self.local_images // (self.sections * self.parts)
        self.hp = round_up(self.half, 8)
        self.rows = self.parts * self.hp
        self.m = self.ni * self.rows
        self.mw = self.ni * NW * WP
        self.hd = self.d // HEADS
        self.quad = 128 // self.hd
        self.ng = HEADS // self.quad
        self.nch = self.ff // CH
        self.scaling = self.hd**-0.5
        self.heads_part = HEADS // self.parts


LINK = 90.0e3
CORE_LINK = 430.0e3
HOP = 2.0
CORE_HOP = 0.8
MARGIN = 0.3
SKEW = 0.0
LEAD = 4.0
ZLAG = 0.0


class Plan:
    def __init__(self):
        self.clock = 0.0
        self.free = {}
        self.queue = []
        self.count = 0

    def link(self, name, size, rate, hop):
        begin = max(self.free.get(name, 0.0), self.clock)
        self.free[name] = begin + size / rate
        return begin + size / rate + hop + MARGIN

    def add(self, when, step):
        heapq.heappush(self.queue, (when, self.count, step))
        self.count += 1

    def pop(self):
        when, _, step = heapq.heappop(self.queue)
        self.clock = max(self.clock, when)
        step()

    def pop_of(self, wanted):
        found = [e for e in self.queue if isinstance(e[2], functools.partial) and wanted(e[2])]
        if found:
            entry = min(found)
            self.queue.remove(entry)
            heapq.heapify(self.queue)
            self.clock = max(self.clock, entry[0])
            entry[2]()
        return bool(found)

    def until(self, when):
        while self.queue and self.queue[0][0] <= when:
            self.pop()
        self.clock = max(self.clock, when)

    def due(self, when):
        return bool(self.queue) and self.queue[0][0] <= when


class Piece:
    def __init__(self, z, kind, index, rows, cols):
        self.kind, self.index, self.rows, self.cols = kind, index, rows, cols
        self.unit = rows * cols * 2 * z.parts

    def home(self, p):
        if self.kind == PROJ or (self.kind == QKV and (p == 1 or self.index == 2)):
            return None
        if self.kind == QKV:
            return p if self.index == 0 else 1 - p
        if p == 1 and self.index == 1:
            return None
        return p if self.kind == FC1 else 1 - p

    def sum_home(self, p):
        if p == 1 and self.index == 1 and self.kind in (FC1, FC2):
            return 0 if self.kind == FC1 else 1
        return None


QKV, PROJ, FC1, FC2 = range(4)


def make_pieces(z, qrow, prow, f2row):
    pieces = [Piece(z, QKV, k, qrow, z.d // z.parts) for k in range(3)]
    pieces.append(Piece(z, PROJ, 0, prow, z.d))
    pieces += [Piece(z, FC1, k, qrow, z.ff // z.parts // 2) for k in range(2)]
    pieces += [Piece(z, FC2, k, f2row // 2, z.d) for k in range(2)]
    for i, piece in enumerate(pieces):
        piece.id = i
    return pieces


def kernel(z, *refs):
    r = types.SimpleNamespace(**dict(zip(z.names, refs)))
    s = lax.axis_index(SECTION)
    d = lax.axis_index(DP)
    t = lax.axis_index(TENSOR)
    na, nb, nt, ns, ni = z.na, z.nb, z.parts, z.sections, z.ni
    a = d // nb
    b = lax.rem(d, nb)
    rows, m = z.rows, z.m
    pieces = z.pieces
    plan = Plan()

    def dev(s_=None, a_=None, b_=None, t_=None):
        s_ = s if s_ is None else s_
        a_ = a if a_ is None else a_
        b_ = b if b_ is None else b_
        t_ = t if t_ is None else t_
        return (s_, a_ * nb + b_, t_)

    def ahead(base, n):
        return [lax.rem(base + k, n) for k in range(1, n)]

    def behind(base, n):
        return [lax.rem(base + n - k, n) for k in range(1, n)]

    x_peers, x_from = ahead(s, ns), behind(s, ns)
    a_peers, a_from = ahead(a, na), behind(a, na)
    b_peers, b_from = ahead(b, nb), behind(b, nb)
    c_peers, c_from = ahead(t, nt), behind(t, nt)
    ALL = slice(None)

    def win(q, ref, lead, a_, b_, t_):
        if q.kind == QKV:
            return ref.at[lead + (q.index, t_, a_, b_)]
        if q.kind == FC1:
            return ref.at[lead + (t_, q.index, a_, b_)]
        if q.kind == FC2:
            return ref.at[lead + (t_, a_, b_, pl.ds(q.index * q.rows, q.rows))]
        return ref.at[lead + (t_, a_, b_)]

    wref = {QKV: r.wq, PROJ: r.wp, FC1: r.w1, FC2: r.w2}

    def shard(q, q_ref, p_ref, f1_ref, f2_ref):
        if q.kind == QKV:
            return q_ref.at[q.index]
        if q.kind == FC1:
            return f1_ref.at[:, pl.ds(q.index * q.cols, q.cols)]
        if q.kind == FC2:
            return f2_ref.at[pl.ds(q.index * q.rows, q.rows)]
        return p_ref

    lx, xs = r.lx, r.xs
    zs, zr, ys, yr, cs, cr = r.zs, r.zr, r.ys, r.yr, r.cs, r.cr

    def remote(src, dst, ss, rs, device):
        return pltpu.make_async_remote_copy(
            src_ref=src, dst_ref=dst, send_sem=ss, recv_sem=rs, device_id=device, device_id_type=MESH
        )

    def send(src, dst, ss, rs, device):
        remote(src, dst, ss, rs, device).start()

    def arrived(dst, sem):
        pltpu.make_async_copy(dst, dst, sem).wait()

    ready_at, x_at = {}, {}
    steps_left = {}

    def planes(home):
        return range(ns) if home is None else (home,)

    def on(home, body):
        if home is None:
            body()
        else:
            pl.when(s == home)(body)

    def other(home):
        return 1 - home

    crossings = [(q, p) for p in range(ns) for q in pieces if q.home(p) is not None]

    def crossing(q, p):
        return crossings.index((q, p))

    def own_shard(q):
        return shard(q, r.q_in, r.p_in, r.f1_in, r.f2_in)

    def start_x(q):
        for p in range(ns):
            home = q.home(p)
            target = win(q, wref[q.kind], (p,), a, b, t)

            @pl.when(s == p)
            def _():
                if home in (None, p):
                    pltpu.make_async_copy(own_shard(q), target, lx.at[q.id, p]).start()
                if home != p:
                    send(own_shard(q), target, xs.at[q.id], lx.at[q.id, p], dev(s_=other(p)))

            x_at[q.id, p] = plan.clock + 1.0
            if home != p:
                x_at[q.id, p] = plan.link(f"x{p}", q.unit, LINK, HOP)
            steps_left[q.id, p] = na if home is None else 2 * na

    def link_of(name, home, size):
        return max(plan.link(f"{name}{h}", size, LINK, HOP) for h in planes(home))

    def go_z(q, p):
        here = win(q, wref[q.kind], (p,), a, b, t)
        home = q.home(p)
        plan.clock = max(plan.clock, x_at[q.id, p])

        def body():
            arrived(here, lx.at[q.id, p])
            for k, peer in enumerate(a_peers):
                send(here, here, zs.at[q.id, p], zr.at[q.id, p, k], dev(a_=peer))

        on(home, body)
        plan.add(plan.clock, functools.partial(go_y, q, p, 0))
        for k in range(na - 1):
            when = link_of("z", home, q.unit * na / (na - 1))
            plan.add(when + ZLAG * p, functools.partial(go_y, q, p, k + 1))

    def source_row(k):
        return a if k == 0 else a_from[k - 1]

    def go_y(q, p, k):
        here = win(q, wref[q.kind], (p,), source_row(k), b, t)
        home = q.home(p)

        def body():
            if k:
                arrived(here, zr.at[q.id, p, k - 1])
            for j, peer in enumerate(b_peers):
                send(here, here, ys.at[q.id, p], yr.at[q.id, p, k, j], dev(b_=peer))

        on(home, body)
        for j in range(nb - 1):
            when = link_of("y", home, q.unit)
        plan.add(when, functools.partial(go_c, q, p, k))

    def to_core(q, p, k):
        here = win(q, wref[q.kind], (p,), source_row(k), ALL, t)
        for j, peer in enumerate(c_peers):
            send(here, here, cs.at[q.id, p, j], cr.at[q.id, p, j], dev(t_=peer))

    def core_time(q, p):
        when = plan.link("c", q.unit * nb / nt, CORE_LINK, CORE_HOP)
        ready_at[q.id, p] = max(when, ready_at.get((q.id, p), 0.0))
        steps_left[q.id, p] -= 1

    def go_c(q, p, k):
        home = q.home(p)

        def body():
            for j, source in enumerate(b_from):
                arrived(win(q, wref[q.kind], (p,), source_row(k), source, t), yr.at[q.id, p, k, j])
            if home is not None:
                here = win(q, wref[q.kind], (p,), source_row(k), ALL, t)
                send(here, here, r.ws.at[crossing(q, p)], r.wr.at[crossing(q, p), k], dev(s_=other(home)))
            to_core(q, p, k)

        on(home, body)
        core_time(q, p)
        if home is not None:
            when = plan.link(f"x{home}", q.unit * nb, LINK, HOP)
            plan.add(when, functools.partial(go_w, q, p, k))

    def go_w(q, p, k):
        def body():
            arrived(win(q, wref[q.kind], (p,), source_row(k), ALL, t), r.wr.at[crossing(q, p), k])
            to_core(q, p, k)

        on(other(q.home(p)), body)
        core_time(q, p)

    def concerns(group, p, step):
        args = getattr(step, "args", ())
        if step.func is next_z:
            return any(q in group and e == p for q, e in order[args[0] :])
        return len(args) > 1 and args[1] == p and args[0] in group

    def need(kind, p, index=None):
        group = [q for q in pieces if q.kind == kind or (kind == FC1 and q.kind == FC2)]
        mine = [q for q in pieces if q.kind == kind and index in (None, q.index)]
        while any(steps_left[q.id, p] for q in mine):
            plan.pop()
        for q in mine:
            plan.clock = max(plan.clock, ready_at[q.id, p])
            for j, source in enumerate(c_from):
                arrived(win(q, wref[q.kind], (p,), ALL, ALL, source), cr.at[q.id, p, j])

    def gather_sent():
        for q in pieces:
            for p in range(ns):
                home = q.home(p)
                if home != p:

                    @pl.when(s == p)
                    def _():
                        arrived(own_shard(q), xs.at[q.id])

                def plane():
                    ref = wref[q.kind]
                    arrived(win(q, ref, (p,), pl.ds(0, na - 1), b, t), zs.at[q.id, p])
                    arrived(win(q, ref, (p,), ALL, pl.ds(0, nb - 1), t), ys.at[q.id, p])
                    if home is not None:
                        arrived(win(q, ref, (p,), ALL, ALL, t), r.ws.at[crossing(q, p)])

                on(home, plane)
                for j in range(nt - 1):
                    arrived(win(q, wref[q.kind], (p,), ALL, ALL, t), cs.at[q.id, p, j])

    def run(lo, hi, cost, body, before=None):
        def one(i, carry):
            for k in range(lo, hi):
                if before is not None or plan.due(plan.clock):

                    @pl.when(i == k)
                    def _():
                        plan.until(plan.clock)
                        if before is not None:
                            before(k)

                plan.clock += cost

            body(i)
            return carry

        lax.fori_loop(lo, hi, one, 0)
        plan.until(plan.clock)

    def spent(cost):
        plan.until(plan.clock + cost)

    SMF = r.smf
    P0, P1, P2 = r.p0, r.p1, r.p2
    small_ready = []

    def placed(ref, at):
        value = ref[...] if len(ref.shape) == 2 else ref[0]
        width = value.shape[-1]
        col = lax.broadcasted_iota(jnp.int32, (width, z.d), 1)
        src = lax.broadcasted_iota(jnp.int32, (width, z.d), 0)
        return dotf(value, (col == src + at).astype(bf16), NN)

    def pack_small():
        share = t * z.dp + d
        first = (t == 0).astype(f32)
        index = lax.broadcasted_iota(jnp.int32, (GATHER_ROWS, z.d), 0)
        total = jnp.zeros((GATHER_ROWS, z.d), f32)
        vectors = (r.v_n1g, r.v_n1b, r.v_pb, r.v_n2g, r.v_n2b, r.v_f2b)
        width = r.v_n1g.shape[-1]
        for k, ref in enumerate(vectors):
            total = total + jnp.where(index == k, placed(ref, d * width) * first, 0.0)
        qkv_rows = placed(r.v_qb, share * r.v_qb.shape[-1])
        for k in range(3):
            total = total + jnp.where(index == 6 + k, qkv_rows[k : k + 1], 0.0)
        at = share * r.v_f1b.shape[-1]
        total = total + jnp.where(index == 9 + at // z.d, placed(r.v_f1b, lax.rem(at, z.d)), 0.0)
        r.sm_in[...] = total.astype(bf16)

    def small_start():
        P0[s] = r.sm_in[...]
        for k, peer in enumerate(x_peers):
            send(r.sm_in, P0.at[s], r.ps.at[0, 0], r.psr.at[0, 0], dev(s_=peer))
        plan.link("x0", P0.size * nt, LINK, HOP)

    def small_part(src, dst, p, level, targets):
        for k, target in enumerate(targets):
            send(src.at[p], dst.at[p, k], r.ps.at[p, level], r.psr.at[p, level], target)

    def small_sum(base, takes, p, level):
        total = base[p].astype(f32)
        arrived(takes.at[p], r.psr.at[p, level])
        for k in range(takes.shape[1]):
            total = total + takes[p, k].astype(f32)
        return total

    def small_a(p):
        @pl.when(s != p)
        def _():
            arrived(P0.at[p], r.psr.at[0, 0])

        small_part(P0, r.pa, p, 1, [dev(a_=e) for e in a_peers])
        for h in range(ns):
            when = plan.link(f"z{h}", P0.size * nt * na, LINK, HOP)
        plan.add(when, functools.partial(small_b, p))

    def small_b(p):
        P1[p] = small_sum(P0, r.pa, p, 1).astype(bf16)
        small_part(P1, r.pb, p, 2, [dev(b_=e) for e in b_peers])
        for h in range(ns):
            when = plan.link(f"y{h}", P0.size * nt, LINK, HOP)
        plan.add(when, functools.partial(small_c, p))

    def small_c(p):
        P2[p] = small_sum(P1, r.pb, p, 2).astype(bf16)
        small_part(P2, r.pc, p, 3, [dev(t_=e) for e in c_peers])
        plan.add(plan.clock + CORE_HOP, functools.partial(small_d, p))

    def small_d(p):
        SMF[p] = small_sum(P2, r.pc, p, 3)
        small_ready.append(p)

    def need_small(p):
        while p not in small_ready:
            plan.pop()

    def small_sent():
        arrived(r.sm_in, r.ps.at[0, 0])
        for p in range(ns):
            for level, takes in ((1, r.pa), (2, r.pb), (3, r.pc)):
                arrived(takes.at[p], r.ps.at[p, level])

    group = s * nt + t

    def group_images(g):
        return pl.ds(g * ni, ni)

    pack_small()
    r.tbl_in[...] = jnp.zeros(r.tbl_in.shape, f32)
    r.tbl_in[:, 0 : r.v_tab.shape[-1]] = r.v_tab[...]

    barrier = pltpu.get_barrier_semaphore()
    peers = (
        [dev(a_=p) for p in a_peers]
        + [dev(b_=p) for p in b_peers]
        + [dev(t_=p) for p in c_peers]
        + [dev(s_=p) for p in x_peers]
        + [dev(s_=p, t_=q) for p in x_peers for q in c_peers]
    )
    for p in peers:
        pl.semaphore_signal(barrier, inc=1, device_id=p, device_id_type=MESH)
    pl.semaphore_wait(barrier, len(peers))

    tbl = r.tbl
    pltpu.make_async_copy(r.tbl_in, tbl.at[s, t], r.tx.at[s]).start()
    for k, peer in enumerate(x_peers):
        send(r.tbl_in, tbl.at[s, t], r.txs.at[k], r.tx.at[s], dev(s_=peer))
    small_start()
    for q in pieces:
        start_x(q)
    xin = r.outb
    for j, src in enumerate((r.images, r.cotangent)):
        pltpu.make_async_copy(src.at[group_images(t)], xin.at[j, t], r.xl.at[j]).start()
        for k, peer in enumerate(c_peers):
            send(
                src.at[group_images(peer)],
                xin.at[j, t],
                r.xcs.at[j, k],
                r.xcr.at[j, k],
                dev(t_=peer),
            )

    def image_ready(j):
        arrived(xin.at[j, t], r.xl.at[j])
        for k, source in enumerate(c_from):
            arrived(xin.at[j, source], r.xcr.at[j, k])

    pad_rows = jnp.zeros((z.hp - z.half, z.d), f32)

    def load_rows(j, ref):
        def one(i, _):
            pieces = []
            for h in range(nt):
                pieces.append(xin[j, h, i].astype(f32))
                if z.hp > z.half:
                    pieces.append(pad_rows)
            ref[block(i, rows), :] = jnp.concatenate(pieces, 0).astype(ref.dtype)
            return 0

        lax.fori_loop(0, ni, one, 0)

    outb = r.outb

    ships = {}

    def ship(kind, p, slot, i):
        out = r.act if kind == 0 else r.ig
        for h in range(nt):
            target = out.at[group * ni + i]
            mine = jnp.logical_and(s == p, t == h)

            @pl.when(mine)
            def _():
                pltpu.make_async_copy(outb.at[slot, h, i], target, r.os.at[kind, p, h]).start()

            @pl.when(jnp.logical_not(mine))
            def _():
                remote(
                    outb.at[slot, h, i], target, r.os.at[kind, p, h], r.orr.at[kind, group], (p, d, h)
                ).start()

        plan.link(f"x{other(p)}", rows * z.d * 2 * nt, LINK, HOP)
        ships[kind, p] = ships.get((kind, p), 0) + 1

    def ship_later(kind, p, slot, times):
        for i in range(ni):
            plan.add(plan.clock + times[i % len(times)], functools.partial(ship, kind, p, slot, i))

    def shipped(kind, p, slot):
        while ships.get((kind, p), 0) < ni:
            plan.pop()
        for h in range(nt):
            arrived(outb.at[slot, h], r.os.at[kind, p, h])

    def received(kind):
        out = r.act if kind == 0 else r.ig
        for g in range(ns * nt):

            @pl.when(g != group)
            def _():
                arrived(out.at[group_images(g)], r.orr.at[kind, g])

    def stage_out(value, i, slot):
        for h in range(nt):
            outb[slot, h, i] = value[h * z.hp : h * z.hp + z.half].astype(bf16)

    width = z.d // nt

    def w_qkv(p, c, part):
        return r.wq[p, c, part].reshape(z.d, width)

    def q_part(part):
        return slice(part * width, (part + 1) * width)

    def w_proj(p):
        return r.wp[p].reshape(z.d, z.d)

    w1_all = r.w1.reshape(2, z.nch, na, nb, r.w1.shape[-2], CH)

    def w_fc1(p, c):
        return w1_all[p, c].reshape(z.d, CH)

    w2_per = CH // r.w2.shape[-2]
    w2_all = r.w2.reshape(2, z.nch, w2_per, r.w2.shape[-2], z.d)

    def w_fc2(p, c):
        return w2_all[p, c].reshape(CH, z.d)

    def row(p, k):
        return SMF[p, pl.ds(k, 1), :]

    def masks(dtype):
        lane = lax.broadcasted_iota(jnp.int32, (WP, 128), 1) // z.hd
        return [(lane == h).astype(dtype) for h in range(z.quad)]

    def spread(v, mk):
        return jnp.concatenate([v * q for q in mk], 0)

    def collect(v, mk):
        acc = v[0:WP] * mk[0]
        for h in range(1, z.quad):
            acc = acc + v[h * WP : (h + 1) * WP] * mk[h]
        return acc

    BM = r.bm
    lanes = 128
    per_lane = lanes // WP

    def build_bias(p):
        j = lax.broadcasted_iota(jnp.int32, (WP, lanes), 0)
        lane = lax.broadcasted_iota(jnp.int32, (WP, lanes), 1)
        i = lax.rem(lane, WP)
        iy, ix, jy, jx = i // WIN, lax.rem(i, WIN), j // WIN, lax.rem(j, WIN)
        valid = jnp.logical_and(i < WT, j < WT)
        index = (iy - jy + WIN - 1) * TABLE_SIDE + ix - jx + WIN - 1
        index = jnp.where(valid, index, 0)
        low = jnp.where(index < lanes, index, 0)
        high = jnp.where(index < lanes, 0, index - lanes)
        head_of_lane = lane // WP
        tables = tbl.reshape(2, HEADS, TABLE_PAD)

        def look(head):
            entry = tables[p, pl.ds(head, 1), :]
            one = jnp.take_along_axis(jnp.broadcast_to(entry[:, :lanes], (WP, lanes)), low, axis=1)
            two = jnp.take_along_axis(jnp.broadcast_to(entry[:, lanes:], (WP, lanes)), high, axis=1)
            return jnp.where(index < lanes, one, two)

        def region(q, wy):
            first = jnp.zeros_like(q)
            if wy < ACROSS - 1:
                return first
            return jnp.where(q < WIN - SHIFT, first + 1, first + 2)

        def group_of_heads(g, carry):
            for c in range(z.quad // per_lane):
                value = look(g * z.quad + c * per_lane)
                for e in range(1, per_lane):
                    value = jnp.where(head_of_lane == e, look(g * z.quad + c * per_lane + e), value)
                value = jnp.where(j < WT, value, -1e30)
                for w in range(NW if p else 1):
                    out = value
                    if p == 1:
                        wy, wx = w // ACROSS, w % ACROSS
                        label_i = region(iy, wy) * 3 + region(ix, wx)
                        label_j = region(jy, wy) * 3 + region(jx, wx)
                        out = out + jnp.where(
                            jnp.logical_and(valid, label_i != label_j), MASK_FILL, 0.0
                        )
                    BM[p + w, g, :, c * lanes : (c + 1) * lanes] = out
            return carry

        lax.fori_loop(0, z.ng, group_of_heads, 0)

    X, G = r.mg, r.g
    PM, PMT = r.pm, r.pmt
    FN, N1, K = r.fn, r.n1, r.k
    QK, PR, CTX, CTXT = r.qk, r.pr, r.ctx, r.ctxt
    MID, MG, SN, N2, ACT, SL = r.mid, r.mg, r.sn, r.n2, r.actv, r.sl
    SG, DB = r.sg, r.db

    def forward(p):
        need_small(p)

        def ln1(i):
            n, inv = normalize(X[block(i, rows), :])
            N1[p, block(i, rows), :] = n.astype(bf16)
            K[block(i, rows), 2 * p : 2 * p + 1] = inv
            f = (n * row(p, 0) + row(p, 1)).astype(bf16)
            FN[p, block(i, rows), :] = f
            CTX[block(i, NW * WP), :] = dotf(PM[p], f, NN).astype(bf16)

        run(0, ni, 0.45, ln1)

        def qkv(c):
            for e in range(nt):
                bias = row(p, 6 + c)[:, q_part(e)]
                QK[p, c, :, q_part(e)] = (dotf(CTX[...], w_qkv(p, c, e), NN) + bias).astype(bf16)

        need(QKV, p)
        run(0, 3, 0.7, qkv)

        def attention(i):
            mb, mf = masks(bf16), masks(f32)
            units = [(i * BATCH + e, g) for e in range(BATCH) for g in range(z.ng)]
            at = [(block(u, WP), slice(g * 128, (g + 1) * 128)) for u, g in units]
            raw = [dotf(QK[p, 1, S, L], spread(QK[p, 0, S, L], mb), NT) for S, L in at]
            prs = []
            for (u, g), sc in zip(units, raw):
                w = 1 + lax.rem(u, NW) if p else 0
                sc = sc * z.scaling + BM[w, g]
                e = jnp.exp(sc - jnp.max(sc, 0, keepdims=True))
                pr = (e * (1.0 / jnp.sum(e, 0, keepdims=True))).astype(bf16)
                PR[p, u, g] = pr
                prs.append(pr)
            mixed = [dotf(pr, QK[p, 2, S, L], TN) for pr, (S, L) in zip(prs, at)]
            for v, (S, L) in zip(mixed, at):
                CTX[S, L] = collect(v, mf).astype(bf16)

        run(0, ni * NW // BATCH, 0.7, attention)

        def unperm(i):
            CTXT[p, block(i, rows), :] = dotf(PMT[p], CTX[block(i, NW * WP), :], NN).astype(bf16)

        run(0, ni, 0.21, unperm)
        need(PROJ, p)
        MID[...] = dotf(CTXT[p], w_proj(p), NN)
        spent(0.6)

        def ln2(i):
            mid = X[block(i, rows), :] + MID[block(i, rows), :] + row(p, 2)
            MID[block(i, rows), :] = mid
            n, inv = normalize(mid)
            N2[p, block(i, rows), :] = n.astype(bf16)
            K[block(i, rows), 2 * p + 1 : 2 * p + 2] = inv
            SN[p, block(i, rows), :] = (n * row(p, 3) + row(p, 4)).astype(bf16)

        run(0, ni, 0.26, ln2)
        if p == 1:
            for j, ref in enumerate((ACT, SL)):
                arrived(ref, r.sp.at[j])
        per = z.nch // 2

        for j in range(2):
            need(FC1, p, j)

            def rise(i):
                c = j + 2 * i
                u = dotf(SN[p], w_fc1(p, c), NN) + row(p, 9 + c)
                h = u * ROOT_HALF
                e = 0.5 + 0.5 * lax.erf(h)
                ACT[c] = (u * e).astype(bf16)
                SL[c] = (e + (u * INV_ROOT_TWO_PI) * jnp.exp2(h * h * NEG_LOG2_E)).astype(bf16)

            run(0, per, 1.16, rise)
        need(FC2, p)

        def fall(c):
            MID[...] += dotf(ACT[c], w_fc2(p, c), NN)

        run(0, z.nch, 0.6, fall)
        if p == 0:
            for j, ref in enumerate((ACT, SL)):
                pltpu.make_async_copy(ref, r.spill.at[j], r.sp.at[j]).start()

        def finish(i):
            value = MID[block(i, rows), :] + row(p, 5)
            X[block(i, rows), :] = value.astype(bf16).astype(f32)
            stage_out(value, i, p)

        run(0, ni, 0.08, finish)
        ship_later(0, p, p, (9.0, 14.0, 19.0, 24.0) if p == 0 else (0.0, 5.0, 10.0, 15.0))

    g1_own = r.g1.reshape(z.nch, *w1_all.shape[2:])
    g2_own = r.g2.reshape(z.nch, *w2_all.shape[2:])

    def backward(p):
        gq, gp, g1, g2 = (
            (r.gq, r.gp, g1_own, g2_own) if p else (r.wq.at[1], r.wp.at[1], w1_all.at[1], w2_all.at[1])
        )
        def addrow(k, v):
            SG[p, pl.ds(k, 1), 0 : z.d] = SG[p, pl.ds(k, 1), 0 : z.d] + v

        SG[p] = jnp.zeros(SG.shape[1:], f32)
        DB[...] = jnp.zeros(DB.shape, f32)
        if p == 0:
            for j, ref in enumerate((ACT, SL)):
                arrived(ref, r.sp.at[j])
            gather_sent()

        def fc2_grad(c):
            g2[c] = dotf(ACT[c], G[...], TN).astype(bf16).reshape(g2.shape[1:])

        run(0, z.nch, 0.82, fc2_grad)
        emit(FC2, p)

        def hidden(c):
            hg = dotf(G[...], w_fc2(p, c), NT) * SL[c].astype(f32)
            SG[p, pl.ds(9 + c, 1), 0 : z.d] = column_sum(hg)
            SL[c] = hg.astype(bf16)

        run(0, z.nch, 0.76, hidden)

        def fc1(c):
            g1[c] = dotf(SN[p], SL[c], TN).astype(bf16).reshape(g1.shape[1:])

        run(0, z.nch, 0.85, fc1)
        MID[...] = jnp.zeros(MID.shape, f32)
        emit(FC1, p)

        def n2g(c):
            MID[...] += dotf(SL[c], w_fc1(p, c), NT)

        run(0, z.nch, 0.74, n2g)
        if p == 1:
            for j, ref in enumerate((ACT, SL)):
                pltpu.make_async_copy(r.spill.at[j], ref, r.sp.at[j]).start()

        def ln2(i):
            sl = block(i, rows)
            ng = MID[sl, :]
            n = N2[p, sl, :].astype(f32)
            g = G[sl, :].astype(f32)
            mg = g + norm_pull(ng, n, K[sl, 2 * p + 1 : 2 * p + 2], row(p, 3))
            MG[sl, :] = mg
            addrow(5, column_sum(g))
            addrow(3, column_sum(ng * n))
            addrow(4, column_sum(ng))
            addrow(2, column_sum(mg))
            G[sl, :] = mg.astype(bf16)

        run(0, ni, 0.4, ln2)
        gp[...] = dotf(CTXT[p], G[...], TN).astype(bf16).reshape(gp.shape)
        CTXT[p] = dotf(G[...], w_proj(p), NT).astype(bf16)
        spent(1.2)

        def cgrad(i):
            CTX[block(i, NW * WP), :] = dotf(PM[p], CTXT[p, block(i, rows), :], NN).astype(bf16)

        run(0, ni, 0.23, cgrad)
        emit(PROJ, p)

        def attention(i):
            mb, mf = masks(bf16), masks(f32)
            units = [(i * BATCH + e, g) for e in range(BATCH) for g in range(z.ng)]
            at = [(block(u, WP), slice(g * 128, (g + 1) * 128)) for u, g in units]
            cbd = [spread(CTX[S, L], mb) for S, L in at]
            dps = [dotf(QK[p, 2, S, L], c, NT) for (S, L), c in zip(at, cbd)]
            dvs = [dotf(PR[p, u, g], c, NN) for (u, g), c in zip(units, cbd)]
            sbs = []
            for (u, g), dp in zip(units, dps):
                pf = PR[p, u, g].astype(f32)
                tt = pf * dp
                sc = tt - pf * jnp.sum(tt, 0, keepdims=True)
                DB[g] = DB[g] + sc
                sbs.append(sc.astype(bf16))
            for v, (S, L) in zip(dvs, at):
                QK[p, 2, S, L] = v.astype(bf16)
            dks = [dotf(sb, spread(QK[p, 0, S, L], mb), NN) for sb, (S, L) in zip(sbs, at)]
            dqs = [dotf(sb, QK[p, 1, S, L], TN) for sb, (S, L) in zip(sbs, at)]
            for dk, dq, (S, L) in zip(dks, dqs, at):
                QK[p, 1, S, L] = (dk * z.scaling).astype(bf16)
                QK[p, 0, S, L] = (collect(dq, mf) * z.scaling).astype(bf16)

        def un(c, i):
            dv = dotf(PMT[p], QK[p, c, block(i, NW * WP), :], NN)
            addrow(6 + c, column_sum(dv))
            QK[p, c, block(i, rows), :] = dv.astype(bf16)

        def qkv_grad(c):
            value = dotf(FN[p], QK[p, c, 0:m, :], TN).astype(bf16)
            for e in range(nt):
                gq[c, e] = value[:, q_part(e)].reshape(gq.shape[2:])

        def emit_last(k):
            if k:
                emit(QKV, p, k - 1)

        def pull(sl, c):
            return sum(dotf(QK[p, c, sl, q_part(e)], w_qkv(p, c, e), NT) for e in range(nt))

        def ln1(i):
            sl = block(i, rows)
            ng = pull(sl, 0) + pull(sl, 1) + pull(sl, 2)
            n = N1[p, sl, :].astype(f32)
            xg = MG[sl, :] + norm_pull(ng, n, K[sl, 2 * p : 2 * p + 1], row(p, 0))
            addrow(0, column_sum(ng * n))
            addrow(1, column_sum(ng))
            if p:
                G[sl, :] = xg.astype(bf16)
            stage_out(xg, i, 1 - p)

        shipped(0, 1 - p, 1 - p)
        per = NW // BATCH
        cost = 1.7

        def image_step(k):
            attention(k)

            @pl.when(lax.rem(k, per) == per - 1)
            def _():
                for c in range(3):
                    un(c, k // per)
                ln1(k // per)

        first = per * cost
        if p == 0:
            ship_later(1, p, 1 - p, [first * (i + 1) for i in range(ni)])
        else:
            ship_later(1, p, 1 - p, [first * ni + 4.0 + 5.0 * i for i in range(ni)])
        run(0, ni * per, cost, image_step)
        run(0, 3, 0.82, qkv_grad, emit_last)
        emit(QKV, p, 2)
        table_rows(p)
        sum_send(p, 0)

    def table_rows(p):
        src = lax.broadcasted_iota(jnp.int32, (z.quad * WP, TABLE_PAD), 0)
        dst = lax.broadcasted_iota(jnp.int32, (z.quad * WP, TABLE_PAD), 1)
        i = lax.rem(src, WP)
        place = jnp.logical_and(
            i < WT, dst == CENTER - ((i // WIN) * TABLE_SIDE + lax.rem(i, WIN))
        )
        head = src // WP
        pick = jnp.concatenate(
            [jnp.logical_and(place, head == h).astype(bf16) for h in range(z.quad)], 1
        )
        group_row = lax.broadcasted_iota(jnp.int32, (8, WP), 0)
        group_of = lax.broadcasted_iota(jnp.int32, (8, WP), 1)
        rows_of = jnp.logical_and(group_of < WT, group_of // WIN == group_row).astype(bf16)

        def split_dot(x, y, left):
            big = x if left else y
            hi = big.astype(bf16)
            lo = (big - hi.astype(f32)).astype(bf16)
            if left:
                return dotf(hi, y, NN) + dotf(lo, y, NN)
            return dotf(x, hi, NN) + dotf(x, lo, NN)

        def one_group(g):
            e = split_dot(DB[g], pick, True)
            for h in range(z.quad):
                v = e[:, h * TABLE_PAD : (h + 1) * TABLE_PAD]
                v = pltpu.roll(v, 0, 1, stride=1, stride_axis=0)
                v = split_dot(rows_of, v, False)
                v = pltpu.roll(v, 0, 1, stride=TABLE_SIDE - WIN, stride_axis=0)
                SG[p, pl.ds(g * z.quad + h, 1), z.d :] = column_sum(v)

        run(0, z.ng, 0.61, one_group)

    gref = {QKV: r.gq, PROJ: r.gp, FC1: r.g1, FC2: r.g2}
    s1, v1, s2, v2, s3, v3, s4, v4 = (r.s1, r.v1, r.s2, r.v2, r.s3, r.v3, r.s4, r.v4)
    k1, k2, k3 = r.k1, r.k2, r.k3
    done = {}

    def buffer(level, q):
        return getattr(r, f"r{level}_{q.id}")

    def gwin(q, p, a_, b_, t_):
        if p == 0:
            return win(q, wref[q.kind], (1,), a_, b_, t_)
        return win(q, gref[q.kind], (), a_, b_, t_)

    def gout(q):
        return shard(q, r.gq_sum, r.gp_sum, r.g1_sum, r.g2_sum)

    def final(q):
        return pltpu.make_async_copy(
            gout(q), shard(q, r.gq_out, r.gp_out, r.g1_out, r.g2_out), r.og.at[q.id]
        )

    def reached(q, p, level):
        while done.get((q.id, p), 0) < level:
            plan.pop()

    def credit(sem, q, k, p, device):
        if p == 1:
            pl.semaphore_signal(sem.at[q.id, k], inc=1, device_id=device, device_id_type=MESH)

    def spend(sem, q, k, p):
        if p == 0:
            pl.semaphore_wait(sem.at[q.id, k], 1)

    def emit(kind, p, index=None):
        for q in pieces:
            if q.kind == kind and index in (None, q.index):
                r1(q, p)

    def r1(q, p):
        if p == 0:
            reached(q, 1, 2)
        for k, peer in enumerate(c_peers):
            spend(k1, q, k, p)
            send(gwin(q, p, ALL, ALL, peer), buffer(1, q).at[k], s1.at[p, q.id, k], v1.at[p, q.id, k], dev(t_=peer))
            when = plan.link("c", q.unit * na * nb / nt, CORE_LINK, CORE_HOP)
        done[q.id, p] = 1
        plan.add(when, functools.partial(r2, q, p))

    def r2(q, p):
        if p == 0:
            reached(q, 1, 3)
        for k in range(nt - 1):
            arrived(buffer(1, q).at[k], v1.at[p, q.id, k])
        mine = gwin(q, p, ALL, ALL, t)
        add_into(mine, [buffer(1, q).at[k] for k in range(nt - 1)])
        for k, source in enumerate(c_from):
            credit(k1, q, k, p, dev(t_=source))
        plan.clock += q.unit * na * nb / 10e6
        done[q.id, p] = 2
        home = q.sum_home(p)
        if home is None:
            to_y(q, p)
            return

        @pl.when(s != home)
        def _():
            send(mine, buffer(6, q), r.s6.at[q.id], r.v6.at[q.id], dev(s_=home))

        when = plan.link(f"x{other(home)}", q.unit * na * nb, LINK, HOP)
        plan.add(when, functools.partial(r2x, q, p))

    def r2x(q, p):
        home = q.sum_home(p)

        def body():
            arrived(buffer(6, q), r.v6.at[q.id])
            add_into(gwin(q, p, ALL, ALL, t), [buffer(6, q)])

        on(home, body)
        plan.clock += q.unit * na * nb / 10e6
        to_y(q, p)

    def to_y(q, p):
        home = q.sum_home(p)

        def body():
            for k, peer in enumerate(b_peers):
                on(q.sum_home(1), functools.partial(spend, k2, q, k, p))
                send(
                    gwin(q, p, ALL, peer, t),
                    buffer(2, q).at[k],
                    s2.at[p, q.id, k],
                    v2.at[p, q.id, k],
                    dev(b_=peer),
                )

        on(home, body)
        for k in range(nb - 1):
            when = link_of("y", home, q.unit * na)
        plan.add(when, functools.partial(r3, q, p))

    def r3(q, p):
        if p == 0:
            reached(q, 1, 4)
        home = q.sum_home(p)

        def body():
            for k in range(nb - 1):
                arrived(buffer(2, q).at[k], v2.at[p, q.id, k])
            add_into(gwin(q, p, ALL, b, t), [buffer(2, q).at[k] for k in range(nb - 1)])
            for k, source in enumerate(b_from):
                credit(k2, q, k, p, dev(b_=source))
            if p == 0:
                on(q.sum_home(1), lambda: pl.semaphore_wait(k3.at[q.id], na - 1))
            for k, peer in enumerate(a_peers):
                send(
                    gwin(q, p, peer, b, t),
                    buffer(3, q).at[k],
                    s3.at[p, q.id],
                    v3.at[p, q.id],
                    dev(a_=peer),
                )

        on(home, body)
        for k in range(na - 1):
            when = link_of("z", home, q.unit * na / (na - 1))
        done[q.id, p] = 3
        plan.add(when, functools.partial(r4, q, p))

    def r4(q, p):
        if p == 0:
            reached(q, 1, 5)
        home = q.sum_home(p)
        mine = gwin(q, p, a, b, t)

        def summed():
            arrived(buffer(3, q), v3.at[p, q.id])
            total = mine[...].astype(f32)
            for k in range(na - 1):
                total = total + buffer(3, q)[k].astype(f32)
            for k, source in enumerate(a_from):
                if p == 1:
                    pl.semaphore_signal(
                        k3.at[q.id], inc=1, device_id=dev(a_=source), device_id_type=MESH
                    )
            return total

        def keep(total):
            gout(q)[...] = total

        def pass_on(total):
            buffer(5, q)[...] = total.astype(bf16)
            remote(buffer(5, q), buffer(4, q), s4.at[p, q.id], v4.at[p, q.id], dev(s_=p)).start()

        if home is None:
            total = summed()
            pl.when(s == p)(functools.partial(keep, total))
            pl.when(s != p)(functools.partial(pass_on, total))
        else:

            @pl.when(s == home)
            def _():
                (keep if home == p else pass_on)(summed())
                if home == p:
                    final(q).start()

        if home == p:
            done[q.id, p] = 5
            return
        done[q.id, p] = 4
        plan.add(plan.link(f"x{other(p)}", q.unit, LINK, HOP), functools.partial(r5, q, p))

    def r5(q, p):
        home = q.sum_home(p)

        @pl.when(s == p)
        def _():
            arrived(buffer(4, q), v4.at[p, q.id])
            out = gout(q)
            value = buffer(4, q)[...].astype(f32)
            out[...] = value if home is not None else out[...] + value
            final(q).start()

        @pl.when(s != p)
        def _():
            arrived(buffer(5, q), s4.at[p, q.id])

        done[q.id, p] = 5

    def settle(q, p):
        home = q.sum_home(p)
        for k, peer in enumerate(c_peers):
            arrived(gwin(q, p, ALL, ALL, peer), s1.at[p, q.id, k])

        def plane():
            for k, peer in enumerate(b_peers):
                arrived(gwin(q, p, ALL, peer, t), s2.at[p, q.id, k])
            arrived(gwin(q, p, pl.ds(0, na - 1), b, t), s3.at[p, q.id])

        on(home, plane)
        if home is not None:

            @pl.when(s != home)
            def _():
                arrived(gwin(q, p, ALL, ALL, t), r.s6.at[q.id])

    def add_into(mine, others):
        lead = mine.shape[:-2]
        count = int(np.prod(lead))

        def one(i, _):
            index = []
            rest = i
            for extent in reversed(lead):
                index.append(lax.rem(rest, extent))
                rest = rest // extent
            index = tuple(reversed(index))
            total = mine[index].astype(f32)
            for o in others:
                total = total + o[index].astype(f32)
            mine[index] = total.astype(bf16)
            return 0

        lax.fori_loop(0, count, one, 0)

    lists = [
        [dev(t_=p) for p in c_peers],
        [dev(b_=p) for p in b_peers],
        [dev(a_=p) for p in a_peers],
    ]
    takes = [r.ra, r.rc, r.rd]
    ss, sv = r.ss, r.sv

    def sum_send(p, k):
        if k == 0:
            r.sums[p, 0] = SG[p].astype(bf16)
        src = r.sums.at[p, k]
        if k < 3:
            for j, target in enumerate(lists[k]):
                send(src, takes[k].at[p, j], ss.at[p, k], sv.at[p, k], target)
        else:

            @pl.when(s != p)
            def _():
                send(src, r.rb, ss.at[p, k], sv.at[p, k], dev(s_=p))

        size = SG.size * nt * (na if k == 2 else 1)
        link = ("c", "y", "z", f"x{other(p)}")[k]
        when = link_of(link, None, size) if k in (1, 2) else plan.link(link, size, LINK, HOP)
        plan.add(when, functools.partial(sum_take, p, k))

    def small_final():
        return pltpu.make_async_copy(r.small_sum, r.small_out, r.og.at[len(pieces)])

    def sum_take(p, k):
        total = r.sums[p, k].astype(f32)
        if k < 3:
            arrived(takes[k].at[p], sv.at[p, k])
            for j in range(len(lists[k])):
                total = total + takes[k][p, j].astype(f32)
            r.sums[p, k + 1] = total.astype(bf16)
            sum_send(p, k + 1)
        else:

            @pl.when(s == p)
            def _():
                arrived(r.rb, sv.at[p, k])
                r.small_sum[...] = total + r.rb[...].astype(f32)
                small_final().start()

    def sums_sent():
        for p in range(ns):
            for k in range(3):
                arrived(takes[k].at[p], ss.at[p, k])

            @pl.when(s != p)
            def _():
                arrived(r.sums.at[p, 3], ss.at[p, 3])

    def is_sum(step, names):
        return step.func is sum_take and (r3 in names and step.args[1] < 2 or r4 in names)

    first = [q for q in pieces if q.kind == QKV]
    for q in first:
        go_z(q, 0)
    small_a(0)
    plan.add(plan.clock + 18.0, functools.partial(small_a, 1))
    plan.until(plan.clock)
    proj = [q for q in pieces if q.kind == PROJ]
    mixed = [q for k in range(2) for q in pieces if q.kind in (FC1, FC2) and q.index == k]
    order = [(q, 0) for q in proj + mixed] + [(q, 1) for q in first + proj + mixed]

    def z_free(q, p):
        return max(plan.free.get(f"z{h}", 0.0) for h in planes(q.home(p)))

    def next_z(k):
        q, p = order[k]
        go_z(q, p)
        if k + 1 < len(order):
            after = order[k + 1]
            plan.add(
                max(x_at[after[0].id, after[1]], z_free(*after) - LEAD), functools.partial(next_z, k + 1)
            )

    plan.add(x_at[order[0][0].id, 0], functools.partial(next_z, 0))
    for q in range(ns):
        arrived(tbl.at[q, t], r.tx.at[q])
        for k, peer in enumerate(c_peers):
            send(tbl.at[q, t], tbl.at[q, t], r.tcs.at[q, k], r.tcr.at[q, k], dev(t_=peer))
    spent(0.5)
    image_ready(0)
    load_rows(0, X)
    spent(0.3)
    for q in range(ns):
        for k, source in enumerate(c_from):
            arrived(tbl.at[q, source], r.tcr.at[q, k])
    for p in range(2):
        build_bias(p)
        spent(0.7)
    image_ready(1)
    load_rows(1, G)
    spent(0.2)

    for p in range(2):
        forward(p)
    for p in (1, 0):
        backward(p)

    for steps_of in ((r1, r2, r2x, r3), (r4,), (r5, sum_take)):
        while plan.pop_of(lambda step: step.func in steps_of or is_sum(step, steps_of)):
            pass

    for q in pieces:
        for p in range(2):
            settle(q, p)
    for q in pieces:
        final(q).wait()
    small_final().wait()
    small_sent()
    received(0)
    received(1)
    shipped(1, 1, 0)
    shipped(1, 0, 1)
    for k in range(ns - 1):
        arrived(r.tbl_in, r.txs.at[k])
    for q in range(ns):
        for k in range(nt - 1):
            arrived(tbl.at[q, t], r.tcs.at[q, k])
    for j, src in enumerate((r.images, r.cotangent)):
        for k in range(nt - 1):
            arrived(outb.at[j, t], r.xcs.at[j, k])
    sums_sent()


def per_device(z, images, cotangent, norm1_gain, norm1_bias, qkv_weight, qkv_bias, position_table,
               proj_weight, proj_bias, norm2_gain, norm2_bias, fc1_weight, fc1_bias, fc2_weight,
               fc2_bias):
    s = lax.axis_index(SECTION)
    d = lax.axis_index(DP)
    t = lax.axis_index(TENSOR)
    D, nt, na, nb, ns, ni = z.d, z.parts, z.na, z.nb, z.sections, z.ni
    part = t * z.dp + d

    def chosen(values):
        return lax.dynamic_slice_in_dim(values, s * nt * ni, nt * ni, 0)

    perm = window_permutation(nt, z.half, z.hp)

    qrow, prow, f2row = qkv_weight.shape[1], proj_weight.shape[1], fc2_weight.shape[1]
    m, mw, nch = z.m, z.mw, z.nch
    S = jax.ShapeDtypeStruct
    V = pl.BlockSpec(memory_space=pltpu.VMEM)
    A = pl.BlockSpec(memory_space=pl.ANY)
    dma = pltpu.SemaphoreType.DMA
    reg = pltpu.SemaphoreType.REGULAR
    inputs = dict(
        images=(chosen(images), A),
        cotangent=(chosen(cotangent), A),
        q_in=(qkv_weight[0].transpose(1, 0, 2), A),
        p_in=(proj_weight[0], A),
        f1_in=(fc1_weight[0], A),
        f2_in=(fc2_weight[0], A),
        v_n1g=(norm1_gain, V),
        v_n1b=(norm1_bias, V),
        v_pb=(proj_bias, V),
        v_n2g=(norm2_gain, V),
        v_n2b=(norm2_bias, V),
        v_f2b=(fc2_bias, V),
        v_qb=(qkv_bias[0], V),
        v_f1b=(fc1_bias, V),
        v_tab=(position_table[0].T, V),
        pm=(jnp.asarray(perm, bf16), V),
        pmt=(jnp.asarray(perm.transpose(0, 2, 1), bf16), V),
    )
    wide = D + TABLE_PAD
    outputs = dict(
        act=(S(images.shape, bf16), A),
        ig=(S(images.shape, bf16), A),
        gq_out=(S((3, qrow, D // nt), f32), A),
        gp_out=(S((prow, D), f32), A),
        g1_out=(S((qrow, z.ff // nt), f32), A),
        g2_out=(S((f2row, D), f32), A),
        small_out=(S((GATHER_ROWS, wide), f32), A),
        spill=(S((2, nch, m, CH), bf16), A),
    )
    vm = pltpu.VMEM
    z.pieces = make_pieces(z, qrow, prow, f2row)
    W = len(z.pieces)
    cross = sum(q.home(p) is not None for q in z.pieces for p in range(2))
    scratch = dict(
        wq=vm((2, 3, nt, na, nb, qrow, D // nt), bf16),
        wp=vm((2, nt, na, nb, prow, D), bf16),
        w1=vm((2, nt, 2, na, nb, qrow, z.ff // nt // 2), bf16),
        w2=vm((2, nt, na, nb, f2row, D), bf16),
        gq_sum=vm((3, qrow, D // nt), f32),
        gp_sum=vm((prow, D), f32),
        g1_sum=vm((qrow, z.ff // nt), f32),
        g2_sum=vm((f2row, D), f32),
        small_sum=vm((GATHER_ROWS, wide), f32),
        og=dma((W + 1,)),
        sm_in=vm((GATHER_ROWS, D), bf16),
        tbl_in=vm((z.heads_part, TABLE_PAD), f32),
        p0=vm((2, GATHER_ROWS, D), bf16),
        p1=vm((2, GATHER_ROWS, D), bf16),
        p2=vm((2, GATHER_ROWS, D), bf16),
        pa=vm((2, na - 1, GATHER_ROWS, D), bf16),
        pb=vm((2, nb - 1, GATHER_ROWS, D), bf16),
        pc=vm((2, nt - 1, GATHER_ROWS, D), bf16),
        ps=dma((2, 4)),
        psr=dma((2, 4)),
        ws=dma((cross,)),
        wr=dma((cross, na)),
        smf=vm((2, GATHER_ROWS, D), f32),
        tbl=vm((2, nt, z.heads_part, TABLE_PAD), f32),
        outb=vm((2, nt, ni, z.half, D), bf16),
        bm=vm((1 + NW, z.ng, WP, z.quad * WP), f32),
        g=vm((m, D), bf16),
        fn=vm((2, m, D), bf16),
        n1=vm((2, m, D), bf16),
        k=vm((m, 4), f32),
        qk=vm((2, 3, mw, D), bf16),
        pr=vm((2, ni * NW, z.ng, WP, z.quad * WP), bf16),
        ctx=vm((mw, D), bf16),
        ctxt=vm((2, m, D), bf16),
        mid=vm((m, D), f32),
        mg=vm((m, D), f32),
        sn=vm((2, m, D), bf16),
        n2=vm((2, m, D), bf16),
        actv=vm((nch, m, CH), bf16),
        sl=vm((nch, m, CH), bf16),
        sg=vm((2, GATHER_ROWS, wide), f32),
        db=vm((z.ng, WP, z.quad * WP), f32),
        gq=vm((3, nt, na, nb, qrow, D // nt), bf16),
        gp=vm((nt, na, nb, prow, D), bf16),
        g1=vm((nt, 2, na, nb, qrow, z.ff // nt // 2), bf16),
        g2=vm((nt, na, nb, f2row, D), bf16),
        sums=vm((2, 4, GATHER_ROWS, wide), bf16),
        ra=vm((2, nt - 1, GATHER_ROWS, wide), bf16),
        rb=vm((GATHER_ROWS, wide), bf16),
        rc=vm((2, nb - 1, GATHER_ROWS, wide), bf16),
        rd=vm((2, na - 1, GATHER_ROWS, wide), bf16),
        lx=dma((W, ns)),
        xs=dma((W,)),
        zs=dma((W, 2)),
        zr=dma((W, 2, na - 1)),
        ys=dma((W, 2)),
        yr=dma((W, 2, na, nb - 1)),
        cs=dma((W, 2, nt - 1)),
        cr=dma((W, 2, nt - 1)),
        tx=dma((ns,)),
        txs=dma((ns - 1,)),
        tcs=dma((ns, nt - 1)),
        tcr=dma((ns, nt - 1)),
        xl=dma((2,)),
        xcs=dma((2, nt - 1)),
        xcr=dma((2, nt - 1)),
        os=dma((2, 2, nt)),
        orr=dma((2, ns * nt)),
        sp=dma((2,)),
        s1=dma((2, W, nt - 1)),
        v1=dma((2, W, nt - 1)),
        s2=dma((2, W, nb - 1)),
        v2=dma((2, W, nb - 1)),
        s3=dma((2, W)),
        v3=dma((2, W)),
        s4=dma((2, W)),
        v4=dma((2, W)),
        s6=dma((W,)),
        v6=dma((W,)),
        k1=reg((W, nt - 1)),
        k2=reg((W, nb - 1)),
        k3=reg((W,)),
        ss=dma((2, 4)),
        sv=dma((2, 4)),
    )
    for q in z.pieces:
        scratch[f"r1_{q.id}"] = vm((nt - 1, na, nb, q.rows, q.cols), bf16)
        scratch[f"r2_{q.id}"] = vm((nb - 1, na, q.rows, q.cols), bf16)
        scratch[f"r3_{q.id}"] = vm((na - 1, q.rows, q.cols), bf16)
        scratch[f"r4_{q.id}"] = vm((q.rows, q.cols), bf16)
        scratch[f"r5_{q.id}"] = vm((q.rows, q.cols), bf16)
        if q.sum_home(1) is not None:
            scratch[f"r6_{q.id}"] = vm((na, nb, q.rows, q.cols), bf16)
    z.names = list(inputs) + list(outputs) + list(scratch)
    results = pl.pallas_call(
        functools.partial(kernel, z),
        out_shape=tuple(o for o, _ in outputs.values()),
        in_specs=[spec for _, spec in inputs.values()],
        out_specs=tuple(spec for _, spec in outputs.values()),
        scratch_shapes=list(scratch.values()),
        compiler_params=pltpu.CompilerParams(
            collective_id=0, has_side_effects=True, vmem_limit_bytes=67043328
        ),
        name="two_blocks",
    )(*[x for x, _ in inputs.values()])
    act, ig, gq, gp, g1, g2, sums, _ = results

    def own_vector(k):
        width = norm1_gain.shape[1]
        return lax.dynamic_slice(sums, (k, d * width), (1, width))

    width = qkv_bias.shape[-1]
    qkv_bias_grad = lax.dynamic_slice(sums, (6, part * width), (3, width))[None]
    width = fc1_bias.shape[1]
    fc1_flat = sums[9 : 9 + nch, :D].reshape(1, -1)
    fc1_bias_grad = lax.dynamic_slice(fc1_flat, (0, part * width), (1, width))
    tables = lax.dynamic_slice(sums, (t * z.heads_part, D), (z.heads_part, TABLE_PAD))
    tables = tables[:, : position_table.shape[1]][:, ::-1].T[None]
    return (
        act[None],
        ig[None],
        own_vector(0),
        own_vector(1),
        gq.transpose(1, 0, 2)[None],
        qkv_bias_grad,
        tables,
        gp[None],
        own_vector(2),
        own_vector(3),
        own_vector(4),
        g1[None],
        fc1_bias_grad,
        g2[None],
        own_vector(5),
    )


def solution(mesh):
    def run(*args):
        z = Sizes(mesh, args[0], args[11])
        return per_device(z, *args)

    in_specs = (
        P(DP, TENSOR, None),
        P(DP, TENSOR, None),
        P(SECTION, DP),
        P(SECTION, DP),
        P(SECTION, DP, None, TENSOR),
        P(SECTION, None, (TENSOR, DP)),
        P(SECTION, None, TENSOR),
        P(SECTION, (TENSOR, DP), None),
        P(SECTION, DP),
        P(SECTION, DP),
        P(SECTION, DP),
        P(SECTION, DP, TENSOR),
        P(SECTION, (TENSOR, DP)),
        P(SECTION, (TENSOR, DP), None),
        P(SECTION, DP),
    )
    out_specs = (
        P(SECTION, DP, TENSOR, None),
        P(SECTION, DP, TENSOR, None),
        P(SECTION, DP),
        P(SECTION, DP),
        P(SECTION, DP, None, TENSOR),
        P(SECTION, None, (TENSOR, DP)),
        P(SECTION, None, TENSOR),
        P(SECTION, (TENSOR, DP), None),
        P(SECTION, DP),
        P(SECTION, DP),
        P(SECTION, DP),
        P(SECTION, DP, TENSOR),
        P(SECTION, (TENSOR, DP)),
        P(SECTION, (TENSOR, DP), None),
        P(SECTION, DP),
    )
    return jax.shard_map(
        run, mesh=mesh, in_specs=in_specs, out_specs=out_specs, check_vma=False
    )
```

```python
import functools
import heapq
import math
import types

import jax
import jax.numpy as jnp
import numpy as np
from jax import lax
from jax.experimental import pallas as pl
from jax.experimental.pallas import tpu as pltpu
from jax.sharding import PartitionSpec as P

HEADS = 16
WIN = 7
SIDE = 14
SHIFT = 3

EPS = 1e-05
MASK_FILL = -100.0
ROOT_HALF = 0.7071067811865476
INV_ROOT_TWO_PI = 0.3989422804014327
NEG_LOG2_E = -1.4426950408889634

ACROSS = SIDE // WIN
NW = ACROSS * ACROSS
WT = WIN * WIN
WP = 64
TABLE_SIDE = 2 * WIN - 1
CENTER = (WIN - 1) * TABLE_SIDE + WIN - 1
TABLE_PAD = 256
CH = 512
GATHER_ROWS = 16
BATCH = 2

SECTION = "section"
DP = "dp"
TENSOR = "tensor"

f32 = jnp.float32
bf16 = jnp.bfloat16
MESH = pl.DeviceIdType.MESH
NN = ((1,), (0,))
NT = ((1,), (1,))
TN = ((0,), (0,))


def round_up(n, m):
    return -(-n // m) * m


def window_slots(shift):
    slot = np.zeros(SIDE * SIDE, np.int64)
    for p in range(SIDE):
        for q in range(SIDE):
            token = ((p + shift) % SIDE) * SIDE + (q + shift) % SIDE
            window = (p // WIN) * ACROSS + q // WIN
            slot[token] = window * WP + (p % WIN) * WIN + q % WIN
    return slot


def window_permutation(parts, half, padded):
    perm = np.zeros((2, NW * WP, parts * padded), np.float32)
    for block in range(2):
        for token, slot in enumerate(window_slots(SHIFT * block)):
            perm[block, slot, (token // half) * padded + token % half] = 1
    return perm


def dotf(a, b, dims):
    return lax.dot_general(a, b, (dims, ((), ())), preferred_element_type=f32)


def normalize(values):
    center = values - jnp.mean(values, -1, keepdims=True)
    inverse = lax.rsqrt(jnp.mean(center * center, -1, keepdims=True) + EPS)
    return center * inverse, inverse


def norm_pull(upstream, normed, inverse, gain):
    scaled = upstream * gain
    return inverse * (
        scaled
        - jnp.mean(scaled, -1, keepdims=True)
        - normed * jnp.mean(scaled * normed, -1, keepdims=True)
    )


def block(i, n):
    if isinstance(i, int):
        return pl.ds(i * n, n)
    return pl.ds(pl.multiple_of(i * n, n), n)


def column_sum(v):
    return jnp.sum(v, 0, keepdims=True)


class Sizes:
    def __init__(self, mesh, images, fc1_weight):
        self.sections = mesh.shape[SECTION]
        self.dp = mesh.shape[DP]
        self.parts = mesh.shape[TENSOR]
        inner = int(math.isqrt(self.dp))
        while self.dp % inner:
            inner -= 1
        self.nb = inner
        self.na = self.dp // inner
        self.local_images, self.half, self.d = images.shape
        self.ff = fc1_weight.shape[-1] * self.parts
        self.ni = self.local_images // (self.sections * self.parts)
        self.hp = round_up(self.half, 8)
        self.rows = self.parts * self.hp
        self.m = self.ni * self.rows
        self.mw = self.ni * NW * WP
        self.hd = self.d // HEADS
        self.quad = 128 // self.hd
        self.ng = HEADS // self.quad
        self.nch = self.ff // CH
        self.scaling = self.hd**-0.5
        self.heads_part = HEADS // self.parts


LINK = 90.0e3
CORE_LINK = 430.0e3
HOP = 2.0
CORE_HOP = 0.8
MARGIN = 0.3
SKEW = 0.0
LEAD = 4.0
FIRST = 1.0
SHIP = 16.0
ZLAG = 0.0


class Plan:
    def __init__(self):
        self.clock = 0.0
        self.free = {}
        self.queue = []
        self.count = 0

    def link(self, name, size, rate, hop):
        begin = max(self.free.get(name, 0.0), self.clock)
        self.free[name] = begin + size / rate
        return begin + size / rate + hop + MARGIN

    def add(self, when, step):
        heapq.heappush(self.queue, (when, self.count, step))
        self.count += 1

    def pop(self):
        when, _, step = heapq.heappop(self.queue)
        self.clock = max(self.clock, when)
        step()

    def pop_of(self, wanted):
        found = [e for e in self.queue if isinstance(e[2], functools.partial) and wanted(e[2])]
        if found:
            entry = min(found)
            self.queue.remove(entry)
            heapq.heapify(self.queue)
            self.clock = max(self.clock, entry[0])
            entry[2]()
        return bool(found)

    def until(self, when):
        while self.queue and self.queue[0][0] <= when:
            self.pop()
        self.clock = max(self.clock, when)

    def due(self, when):
        return bool(self.queue) and self.queue[0][0] <= when


class Piece:
    def __init__(self, z, kind, index, rows, cols):
        self.kind, self.index, self.rows, self.cols = kind, index, rows, cols
        self.unit = rows * cols * 2 * z.parts

    def home(self, p):
        if self.kind == PROJ or (self.kind == QKV and (p == 1 or self.index == 2)):
            return None
        if self.kind == QKV:
            return p if self.index == 0 else 1 - p
        if p == 1 and self.index == 1:
            return None
        return p if self.kind == FC1 else 1 - p

    def sum_home(self, p):
        if self.index == 1 and self.kind in (FC1, FC2):
            return 0 if self.kind == FC1 else 1
        return None


QKV, PROJ, FC1, FC2 = range(4)


def make_pieces(z, qrow, prow, f2row):
    pieces = [Piece(z, QKV, k, qrow, z.d // z.parts) for k in range(3)]
    pieces.append(Piece(z, PROJ, 0, prow, z.d))
    pieces += [Piece(z, FC1, k, qrow, z.ff // z.parts // 2) for k in range(2)]
    pieces += [Piece(z, FC2, k, f2row // 2, z.d) for k in range(2)]
    for i, piece in enumerate(pieces):
        piece.id = i
    return pieces


def kernel(z, *refs):
    r = types.SimpleNamespace(**dict(zip(z.names, refs)))
    s = lax.axis_index(SECTION)
    d = lax.axis_index(DP)
    t = lax.axis_index(TENSOR)
    na, nb, nt, ns, ni = z.na, z.nb, z.parts, z.sections, z.ni
    a = d // nb
    b = lax.rem(d, nb)
    rows, m = z.rows, z.m
    pieces = z.pieces
    plan = Plan()

    def dev(s_=None, a_=None, b_=None, t_=None):
        s_ = s if s_ is None else s_
        a_ = a if a_ is None else a_
        b_ = b if b_ is None else b_
        t_ = t if t_ is None else t_
        return (s_, a_ * nb + b_, t_)

    def ahead(base, n):
        return [lax.rem(base + k, n) for k in range(1, n)]

    def behind(base, n):
        return [lax.rem(base + n - k, n) for k in range(1, n)]

    x_peers, x_from = ahead(s, ns), behind(s, ns)
    a_peers, a_from = ahead(a, na), behind(a, na)
    b_peers, b_from = ahead(b, nb), behind(b, nb)
    c_peers, c_from = ahead(t, nt), behind(t, nt)
    ALL = slice(None)

    def win(q, ref, lead, a_, b_, t_):
        if q.kind == QKV:
            return ref.at[lead + (q.index, t_, a_, b_)]
        if q.kind == FC1:
            return ref.at[lead + (t_, q.index, a_, b_)]
        if q.kind == FC2:
            return ref.at[lead + (t_, a_, b_, pl.ds(q.index * q.rows, q.rows))]
        return ref.at[lead + (t_, a_, b_)]

    wref = {QKV: r.wq, PROJ: r.wp, FC1: r.w1, FC2: r.w2}

    def shard(q, q_ref, p_ref, f1_ref, f2_ref):
        if q.kind == QKV:
            return q_ref.at[q.index]
        if q.kind == FC1:
            return f1_ref.at[:, pl.ds(q.index * q.cols, q.cols)]
        if q.kind == FC2:
            return f2_ref.at[pl.ds(q.index * q.rows, q.rows)]
        return p_ref

    lx, xs = r.lx, r.xs
    zs, zr, ys, yr, cs, cr = r.zs, r.zr, r.ys, r.yr, r.cs, r.cr

    def remote(src, dst, ss, rs, device):
        return pltpu.make_async_remote_copy(
            src_ref=src, dst_ref=dst, send_sem=ss, recv_sem=rs, device_id=device, device_id_type=MESH
        )

    def send(src, dst, ss, rs, device):
        remote(src, dst, ss, rs, device).start()

    def arrived(dst, sem):
        pltpu.make_async_copy(dst, dst, sem).wait()

    ready_at, x_at = {}, {}
    steps_left = {}

    def planes(home):
        return range(ns) if home is None else (home,)

    def on(home, body):
        if home is None:
            body()
        else:
            pl.when(s == home)(body)

    def other(home):
        return 1 - home

    crossings = [(q, p) for p in range(ns) for q in pieces if q.home(p) is not None]

    def crossing(q, p):
        return crossings.index((q, p))

    def own_shard(q):
        return shard(q, r.q_in, r.p_in, r.f1_in, r.f2_in)

    def start_own(q):
        for p in range(ns):
            if q.home(p) in (None, p):

                @pl.when(s == p)
                def _():
                    target = win(q, wref[q.kind], (p,), a, b, t)
                    pltpu.make_async_copy(own_shard(q), target, lx.at[q.id, p]).start()

    def start_x(q):
        for p in range(ns):
            home = q.home(p)
            target = win(q, wref[q.kind], (p,), a, b, t)

            if home != p:

                @pl.when(s == p)
                def _():
                    send(own_shard(q), target, xs.at[q.id], lx.at[q.id, p], dev(s_=other(p)))

            x_at[q.id, p] = plan.clock + 1.0
            if home != p:
                x_at[q.id, p] = plan.link(f"x{p}", q.unit, LINK, HOP)
            steps_left[q.id, p] = na if home is None else 2 * na

    def link_of(name, home, size):
        return max(plan.link(f"{name}{h}", size, LINK, HOP) for h in planes(home))

    def go_z(q, p):
        here = win(q, wref[q.kind], (p,), a, b, t)
        home = q.home(p)
        plan.clock = max(plan.clock, x_at[q.id, p])

        def body():
            arrived(here, lx.at[q.id, p])
            for k, peer in enumerate(a_peers):
                send(here, here, zs.at[q.id, p], zr.at[q.id, p, k], dev(a_=peer))

        on(home, body)
        plan.add(plan.clock, functools.partial(go_y, q, p, 0))
        for k in range(na - 1):
            when = link_of("z", home, q.unit * na / (na - 1))
            plan.add(when + ZLAG * p, functools.partial(go_y, q, p, k + 1))

    def source_row(k):
        return a if k == 0 else a_from[k - 1]

    def go_y(q, p, k):
        here = win(q, wref[q.kind], (p,), source_row(k), b, t)
        home = q.home(p)

        def body():
            if k:
                arrived(here, zr.at[q.id, p, k - 1])
            for j, peer in enumerate(b_peers):
                send(here, here, ys.at[q.id, p], yr.at[q.id, p, k, j], dev(b_=peer))

        on(home, body)
        for j in range(nb - 1):
            when = link_of("y", home, q.unit)
        plan.add(when, functools.partial(go_c, q, p, k))

    def to_core(q, p, k):
        here = win(q, wref[q.kind], (p,), source_row(k), ALL, t)
        for j, peer in enumerate(c_peers):
            send(here, here, cs.at[q.id, p, j], cr.at[q.id, p, j], dev(t_=peer))

    def core_time(q, p):
        when = plan.link("c", q.unit * nb / nt, CORE_LINK, CORE_HOP)
        ready_at[q.id, p] = max(when, ready_at.get((q.id, p), 0.0))
        steps_left[q.id, p] -= 1

    def go_c(q, p, k):
        home = q.home(p)

        def body():
            for j, source in enumerate(b_from):
                arrived(win(q, wref[q.kind], (p,), source_row(k), source, t), yr.at[q.id, p, k, j])
            if home is not None:
                here = win(q, wref[q.kind], (p,), source_row(k), ALL, t)
                send(here, here, r.ws.at[crossing(q, p)], r.wr.at[crossing(q, p), k], dev(s_=other(home)))
            to_core(q, p, k)

        on(home, body)
        core_time(q, p)
        if home is not None:
            when = plan.link(f"x{home}", q.unit * nb, LINK, HOP)
            plan.add(when, functools.partial(go_w, q, p, k))

    def go_w(q, p, k):
        def body():
            arrived(win(q, wref[q.kind], (p,), source_row(k), ALL, t), r.wr.at[crossing(q, p), k])
            to_core(q, p, k)

        on(other(q.home(p)), body)
        core_time(q, p)

    def concerns(group, p, step):
        args = getattr(step, "args", ())
        if step.func is next_z:
            return any(q in group and e == p for q, e in order[args[0] :])
        return len(args) > 1 and args[1] == p and args[0] in group

    def need(kind, p, index=None):
        group = [q for q in pieces if q.kind == kind or (kind == FC1 and q.kind == FC2)]
        mine = [q for q in pieces if q.kind == kind and index in (None, q.index)]
        while any(steps_left[q.id, p] for q in mine):
            plan.pop()
        for q in mine:
            plan.clock = max(plan.clock, ready_at[q.id, p])
            for j, source in enumerate(c_from):
                arrived(win(q, wref[q.kind], (p,), ALL, ALL, source), cr.at[q.id, p, j])

    def gather_sent():
        for q in pieces:
            for p in range(ns):
                home = q.home(p)
                if home != p:

                    @pl.when(s == p)
                    def _():
                        arrived(own_shard(q), xs.at[q.id])

                def plane():
                    ref = wref[q.kind]
                    arrived(win(q, ref, (p,), pl.ds(0, na - 1), b, t), zs.at[q.id, p])
                    arrived(win(q, ref, (p,), ALL, pl.ds(0, nb - 1), t), ys.at[q.id, p])
                    if home is not None:
                        arrived(win(q, ref, (p,), ALL, ALL, t), r.ws.at[crossing(q, p)])

                on(home, plane)
                for j in range(nt - 1):
                    arrived(win(q, wref[q.kind], (p,), ALL, ALL, t), cs.at[q.id, p, j])

    def run(lo, hi, cost, body, before=None):
        def one(i, carry):
            for k in range(lo, hi):
                if before is not None or plan.due(plan.clock):

                    @pl.when(i == k)
                    def _():
                        plan.until(plan.clock)
                        if before is not None:
                            before(k)

                plan.clock += cost

            body(i)
            return carry

        lax.fori_loop(lo, hi, one, 0)
        plan.until(plan.clock)

    def spent(cost):
        plan.until(plan.clock + cost)

    SMF = r.smf
    P0, P1, P2 = r.p0, r.p1, r.p2
    small_ready = []

    def placed(ref, at):
        value = ref[...] if len(ref.shape) == 2 else ref[0]
        width = value.shape[-1]
        col = lax.broadcasted_iota(jnp.int32, (width, z.d), 1)
        src = lax.broadcasted_iota(jnp.int32, (width, z.d), 0)
        return dotf(value, (col == src + at).astype(bf16), NN)

    def pack_small():
        share = t * z.dp + d
        first = (t == 0).astype(f32)
        index = lax.broadcasted_iota(jnp.int32, (GATHER_ROWS, z.d), 0)
        total = jnp.zeros((GATHER_ROWS, z.d), f32)
        vectors = (r.v_n1g, r.v_n1b, r.v_pb, r.v_n2g, r.v_n2b, r.v_f2b)
        width = r.v_n1g.shape[-1]
        for k, ref in enumerate(vectors):
            total = total + jnp.where(index == k, placed(ref, d * width) * first, 0.0)
        qkv_rows = placed(r.v_qb, share * r.v_qb.shape[-1])
        for k in range(3):
            total = total + jnp.where(index == 6 + k, qkv_rows[k : k + 1], 0.0)
        at = share * r.v_f1b.shape[-1]
        total = total + jnp.where(index == 9 + at // z.d, placed(r.v_f1b, lax.rem(at, z.d)), 0.0)
        r.sm_in[...] = total.astype(bf16)

    def small_start():
        P0[s] = r.sm_in[...]
        for k, peer in enumerate(x_peers):
            send(r.sm_in, P0.at[s], r.ps.at[0, 0], r.psr.at[0, 0], dev(s_=peer))
        plan.link("x0", P0.size * nt, LINK, HOP)

    def small_part(src, dst, p, level, targets):
        for k, target in enumerate(targets):
            send(src.at[p], dst.at[p, k], r.ps.at[p, level], r.psr.at[p, level], target)

    def small_sum(base, takes, p, level):
        total = base[p].astype(f32)
        arrived(takes.at[p], r.psr.at[p, level])
        for k in range(takes.shape[1]):
            total = total + takes[p, k].astype(f32)
        return total

    def small_a(p):
        @pl.when(s != p)
        def _():
            arrived(P0.at[p], r.psr.at[0, 0])

        small_part(P0, r.pa, p, 1, [dev(a_=e) for e in a_peers])
        for h in range(ns):
            when = plan.link(f"z{h}", P0.size * nt * na, LINK, HOP)
        plan.add(when, functools.partial(small_b, p))

    def small_b(p):
        P1[p] = small_sum(P0, r.pa, p, 1).astype(bf16)
        small_part(P1, r.pb, p, 2, [dev(b_=e) for e in b_peers])
        for h in range(ns):
            when = plan.link(f"y{h}", P0.size * nt, LINK, HOP)
        plan.add(when, functools.partial(small_c, p))

    def small_c(p):
        P2[p] = small_sum(P1, r.pb, p, 2).astype(bf16)
        small_part(P2, r.pc, p, 3, [dev(t_=e) for e in c_peers])
        plan.add(plan.clock + CORE_HOP, functools.partial(small_d, p))

    def small_d(p):
        SMF[p] = small_sum(P2, r.pc, p, 3)
        small_ready.append(p)

    def need_small(p):
        while p not in small_ready:
            plan.pop()

    def small_sent():
        arrived(r.sm_in, r.ps.at[0, 0])
        for p in range(ns):
            for level, takes in ((1, r.pa), (2, r.pb), (3, r.pc)):
                arrived(takes.at[p], r.ps.at[p, level])

    group = s * nt + t

    def group_images(g):
        return pl.ds(g * ni, ni)

    barrier = pltpu.get_barrier_semaphore()
    peers = (
        [dev(a_=p) for p in a_peers]
        + [dev(b_=p) for p in b_peers]
        + [dev(t_=p) for p in c_peers]
        + [dev(s_=p) for p in x_peers]
        + [dev(s_=p, t_=q) for p in x_peers for q in c_peers]
    )
    for p in peers:
        pl.semaphore_signal(barrier, inc=1, device_id=p, device_id_type=MESH)
    pack_small()
    r.tbl_in[...] = jnp.zeros(r.tbl_in.shape, f32)
    r.tbl_in[:, 0 : r.v_tab.shape[-1]] = r.v_tab[...]
    for q in pieces:
        start_own(q)
    for j, src in enumerate((r.images, r.cotangent)):
        pltpu.make_async_copy(src.at[group_images(t)], r.outb.at[j, t], r.xl.at[j]).start()
    pl.semaphore_wait(barrier, len(peers))

    tbl = r.tbl
    pltpu.make_async_copy(r.tbl_in, tbl.at[s, t], r.tx.at[s]).start()
    for k, peer in enumerate(x_peers):
        send(r.tbl_in, tbl.at[s, t], r.txs.at[k], r.tx.at[s], dev(s_=peer))
    small_start()
    for q in pieces:
        start_x(q)
    xin = r.outb
    for j, src in enumerate((r.images, r.cotangent)):
        for k, peer in enumerate(c_peers):
            send(
                src.at[group_images(peer)],
                xin.at[j, t],
                r.xcs.at[j, k],
                r.xcr.at[j, k],
                dev(t_=peer),
            )

    def image_ready(j):
        arrived(xin.at[j, t], r.xl.at[j])
        for k, source in enumerate(c_from):
            arrived(xin.at[j, source], r.xcr.at[j, k])

    pad_rows = jnp.zeros((z.hp - z.half, z.d), f32)

    def load_rows(j, ref):
        def one(i, _):
            pieces = []
            for h in range(nt):
                pieces.append(xin[j, h, i].astype(f32))
                if z.hp > z.half:
                    pieces.append(pad_rows)
            ref[block(i, rows), :] = jnp.concatenate(pieces, 0).astype(ref.dtype)
            return 0

        lax.fori_loop(0, ni, one, 0)

    outb = r.outb

    ships = {}

    def ship(kind, p, slot, i):
        out = r.act if kind == 0 else r.ig
        for h in range(nt):
            target = out.at[group * ni + i]
            mine = jnp.logical_and(s == p, t == h)

            @pl.when(mine)
            def _():
                pltpu.make_async_copy(outb.at[slot, h, i], target, r.os.at[kind, p, h]).start()

            @pl.when(jnp.logical_not(mine))
            def _():
                remote(
                    outb.at[slot, h, i], target, r.os.at[kind, p, h], r.orr.at[kind, group], (p, d, h)
                ).start()

        plan.link(f"x{other(p)}", rows * z.d * 2 * nt, LINK, HOP)
        ships[kind, p] = ships.get((kind, p), 0) + 1

    def ship_later(kind, p, slot, times):
        for i in range(ni):
            plan.add(plan.clock + times[i % len(times)], functools.partial(ship, kind, p, slot, i))

    def shipped(kind, p, slot):
        while ships.get((kind, p), 0) < ni:
            plan.pop()
        for h in range(nt):
            arrived(outb.at[slot, h], r.os.at[kind, p, h])

    def received(kind):
        out = r.act if kind == 0 else r.ig
        for g in range(ns * nt):

            @pl.when(g != group)
            def _():
                arrived(out.at[group_images(g)], r.orr.at[kind, g])

    def stage_out(value, i, slot):
        for h in range(nt):
            outb[slot, h, i] = value[h * z.hp : h * z.hp + z.half].astype(bf16)

    width = z.d // nt

    def w_qkv(p, c, part):
        return r.wq[p, c, part].reshape(z.d, width)

    def q_part(part):
        return slice(part * width, (part + 1) * width)

    def w_proj(p):
        return r.wp[p].reshape(z.d, z.d)

    w1_all = r.w1.reshape(2, z.nch, na, nb, r.w1.shape[-2], CH)

    def w_fc1(p, c):
        return w1_all[p, c].reshape(z.d, CH)

    w2_per = CH // r.w2.shape[-2]
    w2_all = r.w2.reshape(2, z.nch, w2_per, r.w2.shape[-2], z.d)

    def w_fc2(p, c):
        return w2_all[p, c].reshape(CH, z.d)

    def row(p, k):
        return SMF[p, pl.ds(k, 1), :]

    def masks(dtype):
        lane = lax.broadcasted_iota(jnp.int32, (WP, 128), 1) // z.hd
        return [(lane == h).astype(dtype) for h in range(z.quad)]

    def spread(v, mk):
        return jnp.concatenate([v * q for q in mk], 0)

    def collect(v, mk):
        acc = v[0:WP] * mk[0]
        for h in range(1, z.quad):
            acc = acc + v[h * WP : (h + 1) * WP] * mk[h]
        return acc

    BM = r.bm
    lanes = 128
    per_lane = lanes // WP

    def build_bias(p):
        j = lax.broadcasted_iota(jnp.int32, (WP, lanes), 0)
        lane = lax.broadcasted_iota(jnp.int32, (WP, lanes), 1)
        i = lax.rem(lane, WP)
        iy, ix, jy, jx = i // WIN, lax.rem(i, WIN), j // WIN, lax.rem(j, WIN)
        valid = jnp.logical_and(i < WT, j < WT)
        index = (iy - jy + WIN - 1) * TABLE_SIDE + ix - jx + WIN - 1
        index = jnp.where(valid, index, 0)
        low = jnp.where(index < lanes, index, 0)
        high = jnp.where(index < lanes, 0, index - lanes)
        head_of_lane = lane // WP
        tables = tbl.reshape(2, HEADS, TABLE_PAD)

        def look(head):
            entry = tables[p, pl.ds(head, 1), :]
            one = jnp.take_along_axis(jnp.broadcast_to(entry[:, :lanes], (WP, lanes)), low, axis=1)
            two = jnp.take_along_axis(jnp.broadcast_to(entry[:, lanes:], (WP, lanes)), high, axis=1)
            return jnp.where(index < lanes, one, two)

        def region(q, wy):
            first = jnp.zeros_like(q)
            if wy < ACROSS - 1:
                return first
            return jnp.where(q < WIN - SHIFT, first + 1, first + 2)

        def group_of_heads(g, carry):
            for c in range(z.quad // per_lane):
                value = look(g * z.quad + c * per_lane)
                for e in range(1, per_lane):
                    value = jnp.where(head_of_lane == e, look(g * z.quad + c * per_lane + e), value)
                value = jnp.where(j < WT, value, -1e30)
                for w in range(NW if p else 1):
                    out = value
                    if p == 1:
                        wy, wx = w // ACROSS, w % ACROSS
                        label_i = region(iy, wy) * 3 + region(ix, wx)
                        label_j = region(jy, wy) * 3 + region(jx, wx)
                        out = out + jnp.where(
                            jnp.logical_and(valid, label_i != label_j), MASK_FILL, 0.0
                        )
                    BM[p + w, g, :, c * lanes : (c + 1) * lanes] = out
            return carry

        lax.fori_loop(0, z.ng, group_of_heads, 0)

    X, G = r.mg, r.g
    PM, PMT = r.pm, r.pmt
    FN, N1, K = r.fn, r.n1, r.k
    QK, PR, CTX, CTXT = r.qk, r.pr, r.ctx, r.ctxt
    MID, MG, SN, N2, ACT, SL = r.mid, r.mg, r.sn, r.n2, r.actv, r.sl
    SG, DB = r.sg, r.db

    def forward(p):
        need_small(p)

        def ln1(i):
            if p == 0:
                n = MID[block(i, rows), :]
            else:
                n, inv = normalize(X[block(i, rows), :])
                N1[p, block(i, rows), :] = n.astype(bf16)
                K[block(i, rows), 2 * p : 2 * p + 1] = inv
            f = (n * row(p, 0) + row(p, 1)).astype(bf16)
            FN[p, block(i, rows), :] = f
            CTX[block(i, NW * WP), :] = dotf(PM[p], f, NN).astype(bf16)

        run(0, ni, 0.45 if p else 0.25, ln1)

        def qkv(c):
            for e in range(nt):
                bias = row(p, 6 + c)[:, q_part(e)]
                QK[p, c, :, q_part(e)] = (dotf(CTX[...], w_qkv(p, c, e), NN) + bias).astype(bf16)

        need(QKV, p)
        run(0, 3, 0.7, qkv)

        def attention(i):
            mb, mf = masks(bf16), masks(f32)
            units = [(i * BATCH + e, g) for e in range(BATCH) for g in range(z.ng)]
            at = [(block(u, WP), slice(g * 128, (g + 1) * 128)) for u, g in units]
            raw = [dotf(QK[p, 1, S, L], spread(QK[p, 0, S, L], mb), NT) for S, L in at]
            prs = []
            for (u, g), sc in zip(units, raw):
                w = 1 + lax.rem(u, NW) if p else 0
                sc = sc * z.scaling + BM[w, g]
                e = jnp.exp(sc - jnp.max(sc, 0, keepdims=True))
                pr = (e * (1.0 / jnp.sum(e, 0, keepdims=True))).astype(bf16)
                PR[p, u, g] = pr
                prs.append(pr)
            mixed = [dotf(pr, QK[p, 2, S, L], TN) for pr, (S, L) in zip(prs, at)]
            for v, (S, L) in zip(mixed, at):
                CTX[S, L] = collect(v, mf).astype(bf16)

        run(0, ni * NW // BATCH, 0.7, attention)

        def unperm(i):
            CTXT[p, block(i, rows), :] = dotf(PMT[p], CTX[block(i, NW * WP), :], NN).astype(bf16)

        run(0, ni, 0.21, unperm)
        need(PROJ, p)
        MID[...] = dotf(CTXT[p], w_proj(p), NN)
        spent(0.6)

        def ln2(i):
            mid = X[block(i, rows), :] + MID[block(i, rows), :] + row(p, 2)
            MID[block(i, rows), :] = mid
            n, inv = normalize(mid)
            N2[p, block(i, rows), :] = n.astype(bf16)
            K[block(i, rows), 2 * p + 1 : 2 * p + 2] = inv
            SN[p, block(i, rows), :] = (n * row(p, 3) + row(p, 4)).astype(bf16)

        run(0, ni, 0.26, ln2)
        if p == 1:
            for j, ref in enumerate((ACT, SL)):
                arrived(ref, r.sp.at[j])
        per = z.nch // 2

        for j in range(2):
            need(FC1, p, j)

            def rise(i):
                c = j + 2 * i
                u = dotf(SN[p], w_fc1(p, c), NN) + row(p, 9 + c)
                h = u * ROOT_HALF
                e = 0.5 + 0.5 * lax.erf(h)
                ACT[c] = (u * e).astype(bf16)
                SL[c] = (e + (u * INV_ROOT_TWO_PI) * jnp.exp2(h * h * NEG_LOG2_E)).astype(bf16)

            run(0, per, 1.16, rise)
        need(FC2, p)

        def fall(c):
            MID[...] += dotf(ACT[c], w_fc2(p, c), NN)

        run(0, z.nch, 0.6, fall)
        if p == 0:
            for j, ref in enumerate((ACT, SL)):
                pltpu.make_async_copy(ref, r.spill.at[j], r.sp.at[j]).start()

        def finish(i):
            value = MID[block(i, rows), :] + row(p, 5)
            X[block(i, rows), :] = value.astype(bf16).astype(f32)
            stage_out(value, i, p)

        run(0, ni, 0.08, finish)
        ship_later(0, p, p, (9.0, 14.0, 19.0, 24.0) if p == 0 else (0.0, 5.0, 10.0, 15.0))

    g1_own = r.g1.reshape(z.nch, *w1_all.shape[2:])
    g2_own = r.g2.reshape(z.nch, *w2_all.shape[2:])

    def backward(p):
        gq, gp, g1, g2 = (
            (r.gq, r.gp, g1_own, g2_own) if p else (r.wq.at[1], r.wp.at[1], w1_all.at[1], w2_all.at[1])
        )
        def addrow(k, v):
            SG[p, pl.ds(k, 1), 0 : z.d] = SG[p, pl.ds(k, 1), 0 : z.d] + v

        SG[p] = jnp.zeros(SG.shape[1:], f32)
        DB[...] = jnp.zeros(DB.shape, f32)
        if p == 0:
            for j, ref in enumerate((ACT, SL)):
                arrived(ref, r.sp.at[j])
            gather_sent()

        def fc2_grad(c):
            g2[c] = dotf(ACT[c], G[...], TN).astype(bf16).reshape(g2.shape[1:])

        run(0, z.nch, 0.82, fc2_grad)
        emit(FC2, p)

        def hidden(c):
            hg = dotf(G[...], w_fc2(p, c), NT) * SL[c].astype(f32)
            SG[p, pl.ds(9 + c, 1), 0 : z.d] = column_sum(hg)
            SL[c] = hg.astype(bf16)

        run(0, z.nch, 0.76, hidden)

        def fc1(c):
            g1[c] = dotf(SN[p], SL[c], TN).astype(bf16).reshape(g1.shape[1:])

        run(0, z.nch, 0.85, fc1)
        MID[...] = jnp.zeros(MID.shape, f32)
        emit(FC1, p)

        def n2g(c):
            MID[...] += dotf(SL[c], w_fc1(p, c), NT)

        run(0, z.nch, 0.74, n2g)
        if p == 1:
            for j, ref in enumerate((ACT, SL)):
                pltpu.make_async_copy(r.spill.at[j], ref, r.sp.at[j]).start()

        def ln2(i):
            sl = block(i, rows)
            ng = MID[sl, :]
            n = N2[p, sl, :].astype(f32)
            g = G[sl, :].astype(f32)
            mg = g + norm_pull(ng, n, K[sl, 2 * p + 1 : 2 * p + 2], row(p, 3))
            MG[sl, :] = mg
            addrow(5, column_sum(g))
            addrow(3, column_sum(ng * n))
            addrow(4, column_sum(ng))
            addrow(2, column_sum(mg))
            G[sl, :] = mg.astype(bf16)

        run(0, ni, 0.4, ln2)
        gp[...] = dotf(CTXT[p], G[...], TN).astype(bf16).reshape(gp.shape)
        CTXT[p] = dotf(G[...], w_proj(p), NT).astype(bf16)
        spent(1.2)

        def cgrad(i):
            CTX[block(i, NW * WP), :] = dotf(PM[p], CTXT[p, block(i, rows), :], NN).astype(bf16)

        run(0, ni, 0.23, cgrad)
        emit(PROJ, p)

        def attention(i):
            mb, mf = masks(bf16), masks(f32)
            units = [(i * BATCH + e, g) for e in range(BATCH) for g in range(z.ng)]
            at = [(block(u, WP), slice(g * 128, (g + 1) * 128)) for u, g in units]
            cbd = [spread(CTX[S, L], mb) for S, L in at]
            dps = [dotf(QK[p, 2, S, L], c, NT) for (S, L), c in zip(at, cbd)]
            dvs = [dotf(PR[p, u, g], c, NN) for (u, g), c in zip(units, cbd)]
            sbs = []
            for (u, g), dp in zip(units, dps):
                pf = PR[p, u, g].astype(f32)
                tt = pf * dp
                sc = tt - pf * jnp.sum(tt, 0, keepdims=True)
                DB[g] = DB[g] + sc
                sbs.append(sc.astype(bf16))
            for v, (S, L) in zip(dvs, at):
                QK[p, 2, S, L] = v.astype(bf16)
            dks = [dotf(sb, spread(QK[p, 0, S, L], mb), NN) for sb, (S, L) in zip(sbs, at)]
            dqs = [dotf(sb, QK[p, 1, S, L], TN) for sb, (S, L) in zip(sbs, at)]
            for dk, dq, (S, L) in zip(dks, dqs, at):
                QK[p, 1, S, L] = (dk * z.scaling).astype(bf16)
                QK[p, 0, S, L] = (collect(dq, mf) * z.scaling).astype(bf16)

        def un(c, i):
            dv = dotf(PMT[p], QK[p, c, block(i, NW * WP), :], NN)
            addrow(6 + c, column_sum(dv))
            QK[p, c, block(i, rows), :] = dv.astype(bf16)

        def qkv_grad(c):
            value = dotf(FN[p], QK[p, c, 0:m, :], TN).astype(bf16)
            for e in range(nt):
                gq[c, e] = value[:, q_part(e)].reshape(gq.shape[2:])

        def emit_last(k):
            if k:
                emit(QKV, p, k - 1)

        def pull(sl, c):
            return sum(dotf(QK[p, c, sl, q_part(e)], w_qkv(p, c, e), NT) for e in range(nt))

        def ln1(i):
            sl = block(i, rows)
            ng = pull(sl, 0) + pull(sl, 1) + pull(sl, 2)
            n = N1[p, sl, :].astype(f32)
            xg = MG[sl, :] + norm_pull(ng, n, K[sl, 2 * p : 2 * p + 1], row(p, 0))
            addrow(0, column_sum(ng * n))
            addrow(1, column_sum(ng))
            if p:
                G[sl, :] = xg.astype(bf16)
            stage_out(xg, i, 1 - p)

        shipped(0, 1 - p, 1 - p)
        per = NW // BATCH
        cost = 1.7

        def image_step(k):
            attention(k)

            @pl.when(lax.rem(k, per) == per - 1)
            def _():
                for c in range(3):
                    un(c, k // per)
                ln1(k // per)

        first = per * cost
        if p == 0:
            ship_later(1, p, 1 - p, [first * (i + 1) for i in range(ni)])
        else:
            ship_later(1, p, 1 - p, [first * ni + SHIP + 5.0 * i for i in range(ni)])
        run(0, ni * per, cost, image_step)
        run(0, 3, 0.82, qkv_grad, emit_last)
        emit(QKV, p, 2)
        table_rows(p)
        sum_send(p, 0)

    def table_rows(p):
        src = lax.broadcasted_iota(jnp.int32, (z.quad * WP, TABLE_PAD), 0)
        dst = lax.broadcasted_iota(jnp.int32, (z.quad * WP, TABLE_PAD), 1)
        i = lax.rem(src, WP)
        place = jnp.logical_and(
            i < WT, dst == CENTER - ((i // WIN) * TABLE_SIDE + lax.rem(i, WIN))
        )
        head = src // WP
        pick = jnp.concatenate(
            [jnp.logical_and(place, head == h).astype(bf16) for h in range(z.quad)], 1
        )
        group_row = lax.broadcasted_iota(jnp.int32, (8, WP), 0)
        group_of = lax.broadcasted_iota(jnp.int32, (8, WP), 1)
        rows_of = jnp.logical_and(group_of < WT, group_of // WIN == group_row).astype(bf16)

        def split_dot(x, y, left):
            big = x if left else y
            hi = big.astype(bf16)
            lo = (big - hi.astype(f32)).astype(bf16)
            if left:
                return dotf(hi, y, NN) + dotf(lo, y, NN)
            return dotf(x, hi, NN) + dotf(x, lo, NN)

        def one_group(g):
            e = split_dot(DB[g], pick, True)
            for h in range(z.quad):
                v = e[:, h * TABLE_PAD : (h + 1) * TABLE_PAD]
                v = pltpu.roll(v, 0, 1, stride=1, stride_axis=0)
                v = split_dot(rows_of, v, False)
                v = pltpu.roll(v, 0, 1, stride=TABLE_SIDE - WIN, stride_axis=0)
                SG[p, pl.ds(g * z.quad + h, 1), z.d :] = column_sum(v)

        run(0, z.ng, 0.61, one_group)

    gref = {QKV: r.gq, PROJ: r.gp, FC1: r.g1, FC2: r.g2}
    s1, v1, s2, v2, s3, v3, s4, v4 = (r.s1, r.v1, r.s2, r.v2, r.s3, r.v3, r.s4, r.v4)
    k1, k2, k3 = r.k1, r.k2, r.k3
    done = {}

    def buffer(level, q):
        return getattr(r, f"r{level}_{q.id}")

    def gwin(q, p, a_, b_, t_):
        if p == 0:
            return win(q, wref[q.kind], (1,), a_, b_, t_)
        return win(q, gref[q.kind], (), a_, b_, t_)

    def gout(q):
        return shard(q, r.gq_sum, r.gp_sum, r.g1_sum, r.g2_sum)

    def final(q):
        return pltpu.make_async_copy(
            gout(q), shard(q, r.gq_out, r.gp_out, r.g1_out, r.g2_out), r.og.at[q.id]
        )

    def reached(q, p, level):
        while done.get((q.id, p), 0) < level:
            plan.pop()

    def credit(sem, q, k, p, device):
        if p == 1:
            pl.semaphore_signal(sem.at[q.id, k], inc=1, device_id=device, device_id_type=MESH)

    def spend(sem, q, k, p):
        if p == 0:
            pl.semaphore_wait(sem.at[q.id, k], 1)

    def emit(kind, p, index=None):
        for q in pieces:
            if q.kind == kind and index in (None, q.index):
                r1(q, p)

    def r1(q, p):
        if p == 0:
            reached(q, 1, 2)
        for k, peer in enumerate(c_peers):
            spend(k1, q, k, p)
            send(gwin(q, p, ALL, ALL, peer), buffer(1, q).at[k], s1.at[p, q.id, k], v1.at[p, q.id, k], dev(t_=peer))
            when = plan.link("c", q.unit * na * nb / nt, CORE_LINK, CORE_HOP)
        done[q.id, p] = 1
        plan.add(when, functools.partial(r2, q, p))

    def r2(q, p):
        if p == 0:
            reached(q, 1, 3)
        for k in range(nt - 1):
            arrived(buffer(1, q).at[k], v1.at[p, q.id, k])
        mine = gwin(q, p, ALL, ALL, t)
        add_into(mine, [buffer(1, q).at[k] for k in range(nt - 1)])
        for k, source in enumerate(c_from):
            credit(k1, q, k, p, dev(t_=source))
        plan.clock += q.unit * na * nb / 10e6
        done[q.id, p] = 2
        home = q.sum_home(p)
        if home is None:
            to_y(q, p)
            return

        @pl.when(s != home)
        def _():
            if p == 0:
                pl.semaphore_wait(r.k6.at[q.id], 1)
            send(mine, buffer(6, q), r.s6.at[p, q.id], r.v6.at[p, q.id], dev(s_=home))

        when = plan.link(f"x{other(home)}", q.unit * na * nb, LINK, HOP)
        plan.add(when, functools.partial(r2x, q, p))

    def r2x(q, p):
        home = q.sum_home(p)

        def body():
            arrived(buffer(6, q), r.v6.at[p, q.id])
            add_into(gwin(q, p, ALL, ALL, t), [buffer(6, q)])
            if p == 1:
                pl.semaphore_signal(
                    r.k6.at[q.id], inc=1, device_id=dev(s_=other(home)), device_id_type=MESH
                )

        on(home, body)
        plan.clock += q.unit * na * nb / 10e6
        to_y(q, p)

    def to_y(q, p):
        home = q.sum_home(p)

        def body():
            for k, peer in enumerate(b_peers):
                on(q.sum_home(1), functools.partial(spend, k2, q, k, p))
                send(
                    gwin(q, p, ALL, peer, t),
                    buffer(2, q).at[k],
                    s2.at[p, q.id, k],
                    v2.at[p, q.id, k],
                    dev(b_=peer),
                )

        on(home, body)
        for k in range(nb - 1):
            when = link_of("y", home, q.unit * na)
        plan.add(when, functools.partial(r3, q, p))

    def r3(q, p):
        if p == 0:
            reached(q, 1, 4)
        home = q.sum_home(p)

        def body():
            for k in range(nb - 1):
                arrived(buffer(2, q).at[k], v2.at[p, q.id, k])
            add_into(gwin(q, p, ALL, b, t), [buffer(2, q).at[k] for k in range(nb - 1)])
            for k, source in enumerate(b_from):
                credit(k2, q, k, p, dev(b_=source))
            if p == 0:
                on(q.sum_home(1), lambda: pl.semaphore_wait(k3.at[q.id], na - 1))
            for k, peer in enumerate(a_peers):
                send(
                    gwin(q, p, peer, b, t),
                    buffer(3, q).at[k],
                    s3.at[p, q.id],
                    v3.at[p, q.id],
                    dev(a_=peer),
                )

        on(home, body)
        for k in range(na - 1):
            when = link_of("z", home, q.unit * na / (na - 1))
        done[q.id, p] = 3
        plan.add(when, functools.partial(r4, q, p))

    def r4(q, p):
        if p == 0:
            reached(q, 1, 5)
        home = q.sum_home(p)
        mine = gwin(q, p, a, b, t)

        def summed():
            arrived(buffer(3, q), v3.at[p, q.id])
            total = mine[...].astype(f32)
            for k in range(na - 1):
                total = total + buffer(3, q)[k].astype(f32)
            for k, source in enumerate(a_from):
                if p == 1:
                    pl.semaphore_signal(
                        k3.at[q.id], inc=1, device_id=dev(a_=source), device_id_type=MESH
                    )
            return total

        def keep(total):
            gout(q)[...] = total

        def pass_on(total):
            buffer(5, q)[...] = total.astype(bf16)
            remote(buffer(5, q), buffer(4, q), s4.at[p, q.id], v4.at[p, q.id], dev(s_=p)).start()

        if home is None:
            total = summed()
            pl.when(s == p)(functools.partial(keep, total))
            pl.when(s != p)(functools.partial(pass_on, total))
        else:

            @pl.when(s == home)
            def _():
                (keep if home == p else pass_on)(summed())
                if home == p:
                    final(q).start()

        if home == p:
            done[q.id, p] = 5
            return
        done[q.id, p] = 4
        plan.add(plan.link(f"x{other(p)}", q.unit, LINK, HOP), functools.partial(r5, q, p))

    def r5(q, p):
        home = q.sum_home(p)

        @pl.when(s == p)
        def _():
            arrived(buffer(4, q), v4.at[p, q.id])
            out = gout(q)
            value = buffer(4, q)[...].astype(f32)
            out[...] = value if home is not None else out[...] + value
            final(q).start()

        @pl.when(s != p)
        def _():
            arrived(buffer(5, q), s4.at[p, q.id])

        done[q.id, p] = 5

    def settle(q, p):
        home = q.sum_home(p)
        for k, peer in enumerate(c_peers):
            arrived(gwin(q, p, ALL, ALL, peer), s1.at[p, q.id, k])

        def plane():
            for k, peer in enumerate(b_peers):
                arrived(gwin(q, p, ALL, peer, t), s2.at[p, q.id, k])
            arrived(gwin(q, p, pl.ds(0, na - 1), b, t), s3.at[p, q.id])

        on(home, plane)
        if home is not None:

            @pl.when(s != home)
            def _():
                arrived(gwin(q, p, ALL, ALL, t), r.s6.at[p, q.id])

    def add_into(mine, others):
        lead = mine.shape[:-2]
        count = int(np.prod(lead))

        def one(i, _):
            index = []
            rest = i
            for extent in reversed(lead):
                index.append(lax.rem(rest, extent))
                rest = rest // extent
            index = tuple(reversed(index))
            total = mine[index].astype(f32)
            for o in others:
                total = total + o[index].astype(f32)
            mine[index] = total.astype(bf16)
            return 0

        lax.fori_loop(0, count, one, 0)

    lists = [
        [dev(t_=p) for p in c_peers],
        [dev(b_=p) for p in b_peers],
        [dev(a_=p) for p in a_peers],
    ]
    takes = [r.ra, r.rc, r.rd]
    ss, sv = r.ss, r.sv

    def sum_send(p, k):
        if k == 0:
            r.sums[p, 0] = SG[p].astype(bf16)
        src = r.sums.at[p, k]
        if k < 3:
            for j, target in enumerate(lists[k]):
                send(src, takes[k].at[p, j], ss.at[p, k], sv.at[p, k], target)
        else:

            @pl.when(s != p)
            def _():
                send(src, r.rb, ss.at[p, k], sv.at[p, k], dev(s_=p))

        size = SG.size * nt * (na if k == 2 else 1)
        link = ("c", "y", "z", f"x{other(p)}")[k]
        when = link_of(link, None, size) if k in (1, 2) else plan.link(link, size, LINK, HOP)
        plan.add(when, functools.partial(sum_take, p, k))

    def small_final():
        return pltpu.make_async_copy(r.small_sum, r.small_out, r.og.at[len(pieces)])

    def sum_take(p, k):
        total = r.sums[p, k].astype(f32)
        if k < 3:
            arrived(takes[k].at[p], sv.at[p, k])
            for j in range(len(lists[k])):
                total = total + takes[k][p, j].astype(f32)
            r.sums[p, k + 1] = total.astype(bf16)
            sum_send(p, k + 1)
        else:

            @pl.when(s == p)
            def _():
                arrived(r.rb, sv.at[p, k])
                r.small_sum[...] = total + r.rb[...].astype(f32)
                small_final().start()

    def sums_sent():
        for p in range(ns):
            for k in range(3):
                arrived(takes[k].at[p], ss.at[p, k])

            @pl.when(s != p)
            def _():
                arrived(r.sums.at[p, 3], ss.at[p, 3])

    def is_sum(step, names):
        return step.func is sum_take and (r3 in names and step.args[1] < 2 or r4 in names)

    first = [q for q in pieces if q.kind == QKV]
    for q in first:
        go_z(q, 0)
    small_a(0)
    plan.add(plan.clock + 18.0, functools.partial(small_a, 1))
    plan.until(plan.clock)
    proj = [q for q in pieces if q.kind == PROJ]
    mixed = [q for k in range(2) for q in pieces if q.kind in (FC1, FC2) and q.index == k]
    order = [(q, 0) for q in proj + mixed] + [(q, 1) for q in first + proj + mixed]

    def z_free(q, p):
        return max(plan.free.get(f"z{h}", 0.0) for h in planes(q.home(p)))

    def next_z(k):
        q, p = order[k]
        go_z(q, p)
        if k + 1 < len(order):
            after = order[k + 1]
            plan.add(
                max(x_at[after[0].id, after[1]], z_free(*after) - LEAD), functools.partial(next_z, k + 1)
            )

    plan.add(
        max(x_at[order[0][0].id, 0], z_free(*order[0]) - FIRST), functools.partial(next_z, 0)
    )
    for q in range(ns):
        arrived(tbl.at[q, t], r.tx.at[q])
        for k, peer in enumerate(c_peers):
            send(tbl.at[q, t], tbl.at[q, t], r.tcs.at[q, k], r.tcr.at[q, k], dev(t_=peer))
    spent(0.5)
    image_ready(0)
    load_rows(0, X)

    def early_norm(i, carry):
        n, inv = normalize(X[block(i, rows), :])
        MID[block(i, rows), :] = n
        N1[0, block(i, rows), :] = n.astype(bf16)
        K[block(i, rows), 0:1] = inv
        return carry

    lax.fori_loop(0, ni, early_norm, 0)
    spent(1.3)
    for q in range(ns):
        for k, source in enumerate(c_from):
            arrived(tbl.at[q, source], r.tcr.at[q, k])
    for p in range(2):
        build_bias(p)
        spent(0.7)
    image_ready(1)
    load_rows(1, G)
    spent(0.2)

    for p in range(2):
        forward(p)
    for p in (1, 0):
        backward(p)

    for steps_of in ((r1, r2, r2x, r3), (r4,), (r5, sum_take)):
        while plan.pop_of(lambda step: step.func in steps_of or is_sum(step, steps_of)):
            pass

    for q in pieces:
        for p in range(2):
            settle(q, p)
    for q in pieces:
        final(q).wait()
    small_final().wait()
    small_sent()
    received(0)
    received(1)
    shipped(1, 1, 0)
    shipped(1, 0, 1)
    for k in range(ns - 1):
        arrived(r.tbl_in, r.txs.at[k])
    for q in range(ns):
        for k in range(nt - 1):
            arrived(tbl.at[q, t], r.tcs.at[q, k])
    for j, src in enumerate((r.images, r.cotangent)):
        for k in range(nt - 1):
            arrived(outb.at[j, t], r.xcs.at[j, k])
    sums_sent()


def per_device(z, images, cotangent, norm1_gain, norm1_bias, qkv_weight, qkv_bias, position_table,
               proj_weight, proj_bias, norm2_gain, norm2_bias, fc1_weight, fc1_bias, fc2_weight,
               fc2_bias):
    s = lax.axis_index(SECTION)
    d = lax.axis_index(DP)
    t = lax.axis_index(TENSOR)
    D, nt, na, nb, ns, ni = z.d, z.parts, z.na, z.nb, z.sections, z.ni
    part = t * z.dp + d

    def chosen(values):
        return lax.dynamic_slice_in_dim(values, s * nt * ni, nt * ni, 0)

    perm = window_permutation(nt, z.half, z.hp)

    qrow, prow, f2row = qkv_weight.shape[1], proj_weight.shape[1], fc2_weight.shape[1]
    m, mw, nch = z.m, z.mw, z.nch
    S = jax.ShapeDtypeStruct
    V = pl.BlockSpec(memory_space=pltpu.VMEM)
    A = pl.BlockSpec(memory_space=pl.ANY)
    dma = pltpu.SemaphoreType.DMA
    reg = pltpu.SemaphoreType.REGULAR
    inputs = dict(
        images=(chosen(images), A),
        cotangent=(chosen(cotangent), A),
        q_in=(qkv_weight[0].transpose(1, 0, 2), A),
        p_in=(proj_weight[0], A),
        f1_in=(fc1_weight[0], A),
        f2_in=(fc2_weight[0], A),
        v_n1g=(norm1_gain, V),
        v_n1b=(norm1_bias, V),
        v_pb=(proj_bias, V),
        v_n2g=(norm2_gain, V),
        v_n2b=(norm2_bias, V),
        v_f2b=(fc2_bias, V),
        v_qb=(qkv_bias[0], V),
        v_f1b=(fc1_bias, V),
        v_tab=(position_table[0].T, V),
        pm=(jnp.asarray(perm, bf16), V),
        pmt=(jnp.asarray(perm.transpose(0, 2, 1), bf16), V),
    )
    wide = D + TABLE_PAD
    outputs = dict(
        act=(S(images.shape, bf16), A),
        ig=(S(images.shape, bf16), A),
        gq_out=(S((3, qrow, D // nt), f32), A),
        gp_out=(S((prow, D), f32), A),
        g1_out=(S((qrow, z.ff // nt), f32), A),
        g2_out=(S((f2row, D), f32), A),
        small_out=(S((GATHER_ROWS, wide), f32), A),
        spill=(S((2, nch, m, CH), bf16), A),
    )
    vm = pltpu.VMEM
    z.pieces = make_pieces(z, qrow, prow, f2row)
    W = len(z.pieces)
    cross = sum(q.home(p) is not None for q in z.pieces for p in range(2))
    scratch = dict(
        wq=vm((2, 3, nt, na, nb, qrow, D // nt), bf16),
        wp=vm((2, nt, na, nb, prow, D), bf16),
        w1=vm((2, nt, 2, na, nb, qrow, z.ff // nt // 2), bf16),
        w2=vm((2, nt, na, nb, f2row, D), bf16),
        gq_sum=vm((3, qrow, D // nt), f32),
        gp_sum=vm((prow, D), f32),
        g1_sum=vm((qrow, z.ff // nt), f32),
        g2_sum=vm((f2row, D), f32),
        small_sum=vm((GATHER_ROWS, wide), f32),
        og=dma((W + 1,)),
        sm_in=vm((GATHER_ROWS, D), bf16),
        tbl_in=vm((z.heads_part, TABLE_PAD), f32),
        p0=vm((2, GATHER_ROWS, D), bf16),
        p1=vm((2, GATHER_ROWS, D), bf16),
        p2=vm((2, GATHER_ROWS, D), bf16),
        pa=vm((2, na - 1, GATHER_ROWS, D), bf16),
        pb=vm((2, nb - 1, GATHER_ROWS, D), bf16),
        pc=vm((2, nt - 1, GATHER_ROWS, D), bf16),
        ps=dma((2, 4)),
        psr=dma((2, 4)),
        ws=dma((cross,)),
        wr=dma((cross, na)),
        smf=vm((2, GATHER_ROWS, D), f32),
        tbl=vm((2, nt, z.heads_part, TABLE_PAD), f32),
        outb=vm((2, nt, ni, z.half, D), bf16),
        bm=vm((1 + NW, z.ng, WP, z.quad * WP), f32),
        g=vm((m, D), bf16),
        fn=vm((2, m, D), bf16),
        n1=vm((2, m, D), bf16),
        k=vm((m, 4), f32),
        qk=vm((2, 3, mw, D), bf16),
        pr=vm((2, ni * NW, z.ng, WP, z.quad * WP), bf16),
        ctx=vm((mw, D), bf16),
        ctxt=vm((2, m, D), bf16),
        mid=vm((m, D), f32),
        mg=vm((m, D), f32),
        sn=vm((2, m, D), bf16),
        n2=vm((2, m, D), bf16),
        actv=vm((nch, m, CH), bf16),
        sl=vm((nch, m, CH), bf16),
        sg=vm((2, GATHER_ROWS, wide), f32),
        db=vm((z.ng, WP, z.quad * WP), f32),
        gq=vm((3, nt, na, nb, qrow, D // nt), bf16),
        gp=vm((nt, na, nb, prow, D), bf16),
        g1=vm((nt, 2, na, nb, qrow, z.ff // nt // 2), bf16),
        g2=vm((nt, na, nb, f2row, D), bf16),
        sums=vm((2, 4, GATHER_ROWS, wide), bf16),
        ra=vm((2, nt - 1, GATHER_ROWS, wide), bf16),
        rb=vm((GATHER_ROWS, wide), bf16),
        rc=vm((2, nb - 1, GATHER_ROWS, wide), bf16),
        rd=vm((2, na - 1, GATHER_ROWS, wide), bf16),
        lx=dma((W, ns)),
        xs=dma((W,)),
        zs=dma((W, 2)),
        zr=dma((W, 2, na - 1)),
        ys=dma((W, 2)),
        yr=dma((W, 2, na, nb - 1)),
        cs=dma((W, 2, nt - 1)),
        cr=dma((W, 2, nt - 1)),
        tx=dma((ns,)),
        txs=dma((ns - 1,)),
        tcs=dma((ns, nt - 1)),
        tcr=dma((ns, nt - 1)),
        xl=dma((2,)),
        xcs=dma((2, nt - 1)),
        xcr=dma((2, nt - 1)),
        os=dma((2, 2, nt)),
        orr=dma((2, ns * nt)),
        sp=dma((2,)),
        s1=dma((2, W, nt - 1)),
        v1=dma((2, W, nt - 1)),
        s2=dma((2, W, nb - 1)),
        v2=dma((2, W, nb - 1)),
        s3=dma((2, W)),
        v3=dma((2, W)),
        s4=dma((2, W)),
        v4=dma((2, W)),
        s6=dma((2, W)),
        v6=dma((2, W)),
        k6=reg((W,)),
        k1=reg((W, nt - 1)),
        k2=reg((W, nb - 1)),
        k3=reg((W,)),
        ss=dma((2, 4)),
        sv=dma((2, 4)),
    )
    for q in z.pieces:
        scratch[f"r1_{q.id}"] = vm((nt - 1, na, nb, q.rows, q.cols), bf16)
        scratch[f"r2_{q.id}"] = vm((nb - 1, na, q.rows, q.cols), bf16)
        scratch[f"r3_{q.id}"] = vm((na - 1, q.rows, q.cols), bf16)
        scratch[f"r4_{q.id}"] = vm((q.rows, q.cols), bf16)
        scratch[f"r5_{q.id}"] = vm((q.rows, q.cols), bf16)
        if q.sum_home(1) is not None:
            scratch[f"r6_{q.id}"] = vm((na, nb, q.rows, q.cols), bf16)
    z.names = list(inputs) + list(outputs) + list(scratch)
    results = pl.pallas_call(
        functools.partial(kernel, z),
        out_shape=tuple(o for o, _ in outputs.values()),
        in_specs=[spec for _, spec in inputs.values()],
        out_specs=tuple(spec for _, spec in outputs.values()),
        scratch_shapes=list(scratch.values()),
        compiler_params=pltpu.CompilerParams(
            collective_id=0, has_side_effects=True, vmem_limit_bytes=67043328
        ),
        name="two_blocks",
    )(*[x for x, _ in inputs.values()])
    act, ig, gq, gp, g1, g2, sums, _ = results

    def own_vector(k):
        width = norm1_gain.shape[1]
        return lax.dynamic_slice(sums, (k, d * width), (1, width))

    width = qkv_bias.shape[-1]
    qkv_bias_grad = lax.dynamic_slice(sums, (6, part * width), (3, width))[None]
    width = fc1_bias.shape[1]
    fc1_flat = sums[9 : 9 + nch, :D].reshape(1, -1)
    fc1_bias_grad = lax.dynamic_slice(fc1_flat, (0, part * width), (1, width))
    tables = lax.dynamic_slice(sums, (t * z.heads_part, D), (z.heads_part, TABLE_PAD))
    tables = tables[:, : position_table.shape[1]][:, ::-1].T[None]
    return (
        act[None],
        ig[None],
        own_vector(0),
        own_vector(1),
        gq.transpose(1, 0, 2)[None],
        qkv_bias_grad,
        tables,
        gp[None],
        own_vector(2),
        own_vector(3),
        own_vector(4),
        g1[None],
        fc1_bias_grad,
        g2[None],
        own_vector(5),
    )


def solution(mesh):
    def run(*args):
        z = Sizes(mesh, args[0], args[11])
        return per_device(z, *args)

    in_specs = (
        P(DP, TENSOR, None),
        P(DP, TENSOR, None),
        P(SECTION, DP),
        P(SECTION, DP),
        P(SECTION, DP, None, TENSOR),
        P(SECTION, None, (TENSOR, DP)),
        P(SECTION, None, TENSOR),
        P(SECTION, (TENSOR, DP), None),
        P(SECTION, DP),
        P(SECTION, DP),
        P(SECTION, DP),
        P(SECTION, DP, TENSOR),
        P(SECTION, (TENSOR, DP)),
        P(SECTION, (TENSOR, DP), None),
        P(SECTION, DP),
    )
    out_specs = (
        P(SECTION, DP, TENSOR, None),
        P(SECTION, DP, TENSOR, None),
        P(SECTION, DP),
        P(SECTION, DP),
        P(SECTION, DP, None, TENSOR),
        P(SECTION, None, (TENSOR, DP)),
        P(SECTION, None, TENSOR),
        P(SECTION, (TENSOR, DP), None),
        P(SECTION, DP),
        P(SECTION, DP),
        P(SECTION, DP),
        P(SECTION, DP, TENSOR),
        P(SECTION, (TENSOR, DP)),
        P(SECTION, (TENSOR, DP), None),
        P(SECTION, DP),
    )
    return jax.shard_map(
        run, mesh=mesh, in_specs=in_specs, out_specs=out_specs, check_vma=False
    )
```

```python
import functools
import heapq
import math
import types

import jax
import jax.numpy as jnp
import numpy as np
from jax import lax
from jax.experimental import pallas as pl
from jax.experimental.pallas import tpu as pltpu
from jax.sharding import PartitionSpec as P

HEADS = 16
WIN = 7
SIDE = 14
SHIFT = 3

EPS = 1e-05
MASK_FILL = -100.0
ROOT_HALF = 0.7071067811865476
INV_ROOT_TWO_PI = 0.3989422804014327
NEG_LOG2_E = -1.4426950408889634

ACROSS = SIDE // WIN
NW = ACROSS * ACROSS
WT = WIN * WIN
WP = 64
TABLE_SIDE = 2 * WIN - 1
CENTER = (WIN - 1) * TABLE_SIDE + WIN - 1
TABLE_PAD = 256
CH = 512
GATHER_ROWS = 16
BATCH = 2

SECTION = "section"
DP = "dp"
TENSOR = "tensor"

f32 = jnp.float32
bf16 = jnp.bfloat16
MESH = pl.DeviceIdType.MESH
NN = ((1,), (0,))
NT = ((1,), (1,))
TN = ((0,), (0,))


def round_up(n, m):
    return -(-n // m) * m


def window_slots(shift):
    slot = np.zeros(SIDE * SIDE, np.int64)
    for p in range(SIDE):
        for q in range(SIDE):
            token = ((p + shift) % SIDE) * SIDE + (q + shift) % SIDE
            window = (p // WIN) * ACROSS + q // WIN
            slot[token] = window * WP + (p % WIN) * WIN + q % WIN
    return slot


def window_permutation(parts, half, padded):
    perm = np.zeros((2, NW * WP, parts * padded), np.float32)
    for block in range(2):
        for token, slot in enumerate(window_slots(SHIFT * block)):
            perm[block, slot, (token // half) * padded + token % half] = 1
    return perm


def dotf(a, b, dims):
    return lax.dot_general(a, b, (dims, ((), ())), preferred_element_type=f32)


def normalize(values):
    center = values - jnp.mean(values, -1, keepdims=True)
    inverse = lax.rsqrt(jnp.mean(center * center, -1, keepdims=True) + EPS)
    return center * inverse, inverse


def norm_pull(upstream, normed, inverse, gain):
    scaled = upstream * gain
    return inverse * (
        scaled
        - jnp.mean(scaled, -1, keepdims=True)
        - normed * jnp.mean(scaled * normed, -1, keepdims=True)
    )


def block(i, n):
    if isinstance(i, int):
        return pl.ds(i * n, n)
    return pl.ds(pl.multiple_of(i * n, n), n)


def column_sum(v):
    return jnp.sum(v, 0, keepdims=True)


class Sizes:
    def __init__(self, mesh, images, fc1_weight):
        self.sections = mesh.shape[SECTION]
        self.dp = mesh.shape[DP]
        self.parts = mesh.shape[TENSOR]
        inner = int(math.isqrt(self.dp))
        while self.dp % inner:
            inner -= 1
        self.nb = inner
        self.na = self.dp // inner
        self.local_images, self.half, self.d = images.shape
        self.ff = fc1_weight.shape[-1] * self.parts
        self.ni = self.local_images // (self.sections * self.parts)
        self.hp = round_up(self.half, 8)
        self.rows = self.parts * self.hp
        self.m = self.ni * self.rows
        self.mw = self.ni * NW * WP
        self.hd = self.d // HEADS
        self.quad = 128 // self.hd
        self.ng = HEADS // self.quad
        self.nch = self.ff // CH
        self.scaling = self.hd**-0.5
        self.heads_part = HEADS // self.parts


LINK = 90.0e3
CORE_LINK = 430.0e3
HOP = 2.3
CORE_HOP = 0.8
MARGIN = 0.3
SKEW = 0.0
LEAD = 4.0
FIRST = 1.0
SHIP = 16.0
ZLAG = 0.0


class Plan:
    def __init__(self):
        self.clock = 0.0
        self.free = {}
        self.queue = []
        self.count = 0

    def link(self, name, size, rate, hop):
        begin = max(self.free.get(name, 0.0), self.clock)
        self.free[name] = begin + size / rate
        return begin + size / rate + hop + MARGIN

    def add(self, when, step):
        heapq.heappush(self.queue, (when, self.count, step))
        self.count += 1

    def pop(self):
        when, _, step = heapq.heappop(self.queue)
        self.clock = max(self.clock, when)
        step()

    def pop_of(self, wanted):
        found = [e for e in self.queue if isinstance(e[2], functools.partial) and wanted(e[2])]
        if found:
            entry = min(found)
            self.queue.remove(entry)
            heapq.heapify(self.queue)
            self.clock = max(self.clock, entry[0])
            entry[2]()
        return bool(found)

    def until(self, when):
        while self.queue and self.queue[0][0] <= when:
            self.pop()
        self.clock = max(self.clock, when)

    def due(self, when):
        return bool(self.queue) and self.queue[0][0] <= when


class Piece:
    def __init__(self, z, kind, index, rows, cols):
        self.kind, self.index, self.rows, self.cols = kind, index, rows, cols
        self.unit = rows * cols * 2 * z.parts

    def home(self, p):
        if self.kind == PROJ or (self.kind == QKV and (p == 1 or self.index == 2)):
            return None
        if self.kind == QKV:
            return p if self.index == 0 else 1 - p
        if p == 1 and self.index == 1:
            return None
        return p if self.kind == FC1 else 1 - p

    def sum_home(self, p):
        if self.index == 1 and self.kind in (FC1, FC2):
            return 0 if self.kind == FC1 else 1
        return None


QKV, PROJ, FC1, FC2 = range(4)


def make_pieces(z, qrow, prow, f2row):
    pieces = [Piece(z, QKV, k, qrow, z.d // z.parts) for k in range(3)]
    pieces.append(Piece(z, PROJ, 0, prow, z.d))
    pieces += [Piece(z, FC1, k, qrow, z.ff // z.parts // 2) for k in range(2)]
    pieces += [Piece(z, FC2, k, f2row // 2, z.d) for k in range(2)]
    for i, piece in enumerate(pieces):
        piece.id = i
    return pieces


def kernel(z, *refs):
    r = types.SimpleNamespace(**dict(zip(z.names, refs)))
    s = lax.axis_index(SECTION)
    d = lax.axis_index(DP)
    t = lax.axis_index(TENSOR)
    na, nb, nt, ns, ni = z.na, z.nb, z.parts, z.sections, z.ni
    a = d // nb
    b = lax.rem(d, nb)
    rows, m = z.rows, z.m
    pieces = z.pieces
    plan = Plan()

    def dev(s_=None, a_=None, b_=None, t_=None):
        s_ = s if s_ is None else s_
        a_ = a if a_ is None else a_
        b_ = b if b_ is None else b_
        t_ = t if t_ is None else t_
        return (s_, a_ * nb + b_, t_)

    def ahead(base, n):
        return [lax.rem(base + k, n) for k in range(1, n)]

    def behind(base, n):
        return [lax.rem(base + n - k, n) for k in range(1, n)]

    x_peers, x_from = ahead(s, ns), behind(s, ns)
    a_peers, a_from = ahead(a, na), behind(a, na)
    b_peers, b_from = ahead(b, nb), behind(b, nb)
    c_peers, c_from = ahead(t, nt), behind(t, nt)
    ALL = slice(None)

    def win(q, ref, lead, a_, b_, t_):
        if q.kind == QKV:
            return ref.at[lead + (q.index, t_, a_, b_)]
        if q.kind == FC1:
            return ref.at[lead + (t_, q.index, a_, b_)]
        if q.kind == FC2:
            return ref.at[lead + (t_, a_, b_, pl.ds(q.index * q.rows, q.rows))]
        return ref.at[lead + (t_, a_, b_)]

    wref = {QKV: r.wq, PROJ: r.wp, FC1: r.w1, FC2: r.w2}

    def shard(q, q_ref, p_ref, f1_ref, f2_ref):
        if q.kind == QKV:
            return q_ref.at[q.index]
        if q.kind == FC1:
            return f1_ref.at[:, pl.ds(q.index * q.cols, q.cols)]
        if q.kind == FC2:
            return f2_ref.at[pl.ds(q.index * q.rows, q.rows)]
        return p_ref

    lx, xs = r.lx, r.xs
    zs, zr, ys, yr, cs, cr = r.zs, r.zr, r.ys, r.yr, r.cs, r.cr

    def remote(src, dst, ss, rs, device):
        return pltpu.make_async_remote_copy(
            src_ref=src, dst_ref=dst, send_sem=ss, recv_sem=rs, device_id=device, device_id_type=MESH
        )

    def send(src, dst, ss, rs, device):
        remote(src, dst, ss, rs, device).start()

    def arrived(dst, sem):
        pltpu.make_async_copy(dst, dst, sem).wait()

    ready_at, x_at = {}, {}
    steps_left = {}

    def planes(home):
        return range(ns) if home is None else (home,)

    def on(home, body):
        if home is None:
            body()
        else:
            pl.when(s == home)(body)

    def other(home):
        return 1 - home

    crossings = [(q, p) for p in range(ns) for q in pieces if q.home(p) is not None]

    def crossing(q, p):
        return crossings.index((q, p))

    def own_shard(q):
        return shard(q, r.q_in, r.p_in, r.f1_in, r.f2_in)

    def start_own(q):
        for p in range(ns):
            if q.home(p) in (None, p):

                @pl.when(s == p)
                def _():
                    target = win(q, wref[q.kind], (p,), a, b, t)
                    pltpu.make_async_copy(own_shard(q), target, lx.at[q.id, p]).start()

    def start_x(q):
        for p in range(ns):
            home = q.home(p)
            target = win(q, wref[q.kind], (p,), a, b, t)

            if home != p:

                @pl.when(s == p)
                def _():
                    send(own_shard(q), target, xs.at[q.id], lx.at[q.id, p], dev(s_=other(p)))

            x_at[q.id, p] = plan.clock + 1.0
            if home != p:
                x_at[q.id, p] = plan.link(f"x{p}", q.unit, LINK, HOP)
            steps_left[q.id, p] = na if home is None else 2 * na

    def link_of(name, home, size):
        return max(plan.link(f"{name}{h}", size, LINK, HOP) for h in planes(home))

    def go_z(q, p):
        here = win(q, wref[q.kind], (p,), a, b, t)
        home = q.home(p)
        plan.clock = max(plan.clock, x_at[q.id, p])

        def body():
            arrived(here, lx.at[q.id, p])
            for k, peer in enumerate(a_peers):
                send(here, here, zs.at[q.id, p], zr.at[q.id, p, k], dev(a_=peer))

        on(home, body)
        plan.add(plan.clock, functools.partial(go_y, q, p, 0))
        for k in range(na - 1):
            when = link_of("z", home, q.unit * na / (na - 1))
            plan.add(when + ZLAG * p, functools.partial(go_y, q, p, k + 1))

    def source_row(k):
        return a if k == 0 else a_from[k - 1]

    def go_y(q, p, k):
        here = win(q, wref[q.kind], (p,), source_row(k), b, t)
        home = q.home(p)

        def body():
            if k:
                arrived(here, zr.at[q.id, p, k - 1])
            for j, peer in enumerate(b_peers):
                send(here, here, ys.at[q.id, p], yr.at[q.id, p, k, j], dev(b_=peer))

        on(home, body)
        for j in range(nb - 1):
            when = link_of("y", home, q.unit)
        plan.add(when, functools.partial(go_c, q, p, k))

    def to_core(q, p, k):
        here = win(q, wref[q.kind], (p,), source_row(k), ALL, t)
        for j, peer in enumerate(c_peers):
            send(here, here, cs.at[q.id, p, j], cr.at[q.id, p, j], dev(t_=peer))

    def core_time(q, p):
        when = plan.link("c", q.unit * nb / nt, CORE_LINK, CORE_HOP)
        ready_at[q.id, p] = max(when, ready_at.get((q.id, p), 0.0))
        steps_left[q.id, p] -= 1

    def go_c(q, p, k):
        home = q.home(p)

        def body():
            for j, source in enumerate(b_from):
                arrived(win(q, wref[q.kind], (p,), source_row(k), source, t), yr.at[q.id, p, k, j])
            if home is not None:
                here = win(q, wref[q.kind], (p,), source_row(k), ALL, t)
                send(here, here, r.ws.at[crossing(q, p)], r.wr.at[crossing(q, p), k], dev(s_=other(home)))
            to_core(q, p, k)

        on(home, body)
        core_time(q, p)
        if home is not None:
            when = plan.link(f"x{home}", q.unit * nb, LINK, HOP)
            plan.add(when, functools.partial(go_w, q, p, k))

    def go_w(q, p, k):
        def body():
            arrived(win(q, wref[q.kind], (p,), source_row(k), ALL, t), r.wr.at[crossing(q, p), k])
            to_core(q, p, k)

        on(other(q.home(p)), body)
        core_time(q, p)

    def concerns(group, p, step):
        args = getattr(step, "args", ())
        if step.func is next_z:
            return any(q in group and e == p for q, e in order[args[0] :])
        return len(args) > 1 and args[1] == p and args[0] in group

    def need(kind, p, index=None):
        group = [q for q in pieces if q.kind == kind or (kind == FC1 and q.kind == FC2)]
        mine = [q for q in pieces if q.kind == kind and index in (None, q.index)]
        while any(steps_left[q.id, p] for q in mine):
            plan.pop()
        for q in mine:
            plan.clock = max(plan.clock, ready_at[q.id, p])
            for j, source in enumerate(c_from):
                arrived(win(q, wref[q.kind], (p,), ALL, ALL, source), cr.at[q.id, p, j])

    def gather_sent():
        for q in pieces:
            for p in range(ns):
                home = q.home(p)
                if home != p:

                    @pl.when(s == p)
                    def _():
                        arrived(own_shard(q), xs.at[q.id])

                def plane():
                    ref = wref[q.kind]
                    arrived(win(q, ref, (p,), pl.ds(0, na - 1), b, t), zs.at[q.id, p])
                    arrived(win(q, ref, (p,), ALL, pl.ds(0, nb - 1), t), ys.at[q.id, p])
                    if home is not None:
                        arrived(win(q, ref, (p,), ALL, ALL, t), r.ws.at[crossing(q, p)])

                on(home, plane)
                for j in range(nt - 1):
                    arrived(win(q, wref[q.kind], (p,), ALL, ALL, t), cs.at[q.id, p, j])

    def run(lo, hi, cost, body, before=None):
        def one(i, carry):
            for k in range(lo, hi):
                if before is not None or plan.due(plan.clock):

                    @pl.when(i == k)
                    def _():
                        plan.until(plan.clock)
                        if before is not None:
                            before(k)

                plan.clock += cost

            body(i)
            return carry

        lax.fori_loop(lo, hi, one, 0)
        plan.until(plan.clock)

    def spent(cost):
        plan.until(plan.clock + cost)

    SMF = r.smf
    P0, P1, P2 = r.p0, r.p1, r.p2
    small_ready = []

    def placed(ref, at):
        value = ref[...] if len(ref.shape) == 2 else ref[0]
        width = value.shape[-1]
        col = lax.broadcasted_iota(jnp.int32, (width, z.d), 1)
        src = lax.broadcasted_iota(jnp.int32, (width, z.d), 0)
        return dotf(value, (col == src + at).astype(bf16), NN)

    def pack_small():
        share = t * z.dp + d
        first = (t == 0).astype(f32)
        index = lax.broadcasted_iota(jnp.int32, (GATHER_ROWS, z.d), 0)
        total = jnp.zeros((GATHER_ROWS, z.d), f32)
        vectors = (r.v_n1g, r.v_n1b, r.v_pb, r.v_n2g, r.v_n2b, r.v_f2b)
        width = r.v_n1g.shape[-1]
        for k, ref in enumerate(vectors):
            total = total + jnp.where(index == k, placed(ref, d * width) * first, 0.0)
        qkv_rows = placed(r.v_qb, share * r.v_qb.shape[-1])
        for k in range(3):
            total = total + jnp.where(index == 6 + k, qkv_rows[k : k + 1], 0.0)
        at = share * r.v_f1b.shape[-1]
        total = total + jnp.where(index == 9 + at // z.d, placed(r.v_f1b, lax.rem(at, z.d)), 0.0)
        r.sm_in[...] = total.astype(bf16)

    def small_start():
        P0[s] = r.sm_in[...]
        for k, peer in enumerate(x_peers):
            send(r.sm_in, P0.at[s], r.ps.at[0, 0], r.psr.at[0, 0], dev(s_=peer))
        plan.link("x0", P0.size * nt, LINK, HOP)

    def small_part(src, dst, p, level, targets):
        for k, target in enumerate(targets):
            send(src.at[p], dst.at[p, k], r.ps.at[p, level], r.psr.at[p, level], target)

    def small_sum(base, takes, p, level):
        total = base[p].astype(f32)
        arrived(takes.at[p], r.psr.at[p, level])
        for k in range(takes.shape[1]):
            total = total + takes[p, k].astype(f32)
        return total

    def small_a(p):
        @pl.when(s != p)
        def _():
            arrived(P0.at[p], r.psr.at[0, 0])

        small_part(P0, r.pa, p, 1, [dev(a_=e) for e in a_peers])
        for h in range(ns):
            when = plan.link(f"z{h}", P0.size * nt * na, LINK, HOP)
        plan.add(when, functools.partial(small_b, p))

    def small_b(p):
        P1[p] = small_sum(P0, r.pa, p, 1).astype(bf16)
        small_part(P1, r.pb, p, 2, [dev(b_=e) for e in b_peers])
        for h in range(ns):
            when = plan.link(f"y{h}", P0.size * nt, LINK, HOP)
        plan.add(when, functools.partial(small_c, p))

    def small_c(p):
        P2[p] = small_sum(P1, r.pb, p, 2).astype(bf16)
        small_part(P2, r.pc, p, 3, [dev(t_=e) for e in c_peers])
        plan.add(plan.clock + CORE_HOP, functools.partial(small_d, p))

    def small_d(p):
        SMF[p] = small_sum(P2, r.pc, p, 3)
        small_ready.append(p)

    def need_small(p):
        while p not in small_ready:
            plan.pop()

    def small_sent():
        arrived(r.sm_in, r.ps.at[0, 0])
        for p in range(ns):
            for level, takes in ((1, r.pa), (2, r.pb), (3, r.pc)):
                arrived(takes.at[p], r.ps.at[p, level])

    group = s * nt + t

    def group_images(g):
        return pl.ds(g * ni, ni)

    barrier = pltpu.get_barrier_semaphore()
    peers = (
        [dev(a_=p) for p in a_peers]
        + [dev(b_=p) for p in b_peers]
        + [dev(t_=p) for p in c_peers]
        + [dev(s_=p) for p in x_peers]
        + [dev(s_=p, t_=q) for p in x_peers for q in c_peers]
    )
    for p in peers:
        pl.semaphore_signal(barrier, inc=1, device_id=p, device_id_type=MESH)
    pack_small()
    r.tbl_in[...] = jnp.zeros(r.tbl_in.shape, f32)
    r.tbl_in[:, 0 : r.v_tab.shape[-1]] = r.v_tab[...]
    for q in pieces:
        start_own(q)
    for j, src in enumerate((r.images, r.cotangent)):
        pltpu.make_async_copy(src.at[group_images(t)], r.outb.at[j, t], r.xl.at[j]).start()
    pl.semaphore_wait(barrier, len(peers))

    tbl = r.tbl
    pltpu.make_async_copy(r.tbl_in, tbl.at[s, t], r.tx.at[s]).start()
    for k, peer in enumerate(x_peers):
        send(r.tbl_in, tbl.at[s, t], r.txs.at[k], r.tx.at[s], dev(s_=peer))
    small_start()
    for q in pieces:
        start_x(q)
    xin = r.outb
    for j, src in enumerate((r.images, r.cotangent)):
        for k, peer in enumerate(c_peers):
            send(
                src.at[group_images(peer)],
                xin.at[j, t],
                r.xcs.at[j, k],
                r.xcr.at[j, k],
                dev(t_=peer),
            )

    def image_ready(j):
        arrived(xin.at[j, t], r.xl.at[j])
        for k, source in enumerate(c_from):
            arrived(xin.at[j, source], r.xcr.at[j, k])

    pad_rows = jnp.zeros((z.hp - z.half, z.d), f32)

    def load_rows(j, ref):
        def one(i, _):
            pieces = []
            for h in range(nt):
                pieces.append(xin[j, h, i].astype(f32))
                if z.hp > z.half:
                    pieces.append(pad_rows)
            ref[block(i, rows), :] = jnp.concatenate(pieces, 0).astype(ref.dtype)
            return 0

        lax.fori_loop(0, ni, one, 0)

    outb = r.outb

    ships = {}

    def ship(kind, p, slot, i):
        out = r.act if kind == 0 else r.ig
        for h in range(nt):
            target = out.at[group * ni + i]
            mine = jnp.logical_and(s == p, t == h)

            @pl.when(mine)
            def _():
                pltpu.make_async_copy(outb.at[slot, h, i], target, r.os.at[kind, p, h]).start()

            @pl.when(jnp.logical_not(mine))
            def _():
                remote(
                    outb.at[slot, h, i], target, r.os.at[kind, p, h], r.orr.at[kind, group], (p, d, h)
                ).start()

        plan.link(f"x{other(p)}", rows * z.d * 2 * nt, LINK, HOP)
        ships[kind, p] = ships.get((kind, p), 0) + 1

    def ship_later(kind, p, slot, times):
        for i in range(ni):
            plan.add(plan.clock + times[i % len(times)], functools.partial(ship, kind, p, slot, i))

    def shipped(kind, p, slot):
        while ships.get((kind, p), 0) < ni:
            plan.pop()
        for h in range(nt):
            arrived(outb.at[slot, h], r.os.at[kind, p, h])

    def received(kind):
        out = r.act if kind == 0 else r.ig
        for g in range(ns * nt):

            @pl.when(g != group)
            def _():
                arrived(out.at[group_images(g)], r.orr.at[kind, g])

    def stage_out(value, i, slot):
        for h in range(nt):
            outb[slot, h, i] = value[h * z.hp : h * z.hp + z.half].astype(bf16)

    width = z.d // nt

    def w_qkv(p, c, part):
        return r.wq[p, c, part].reshape(z.d, width)

    def q_part(part):
        return slice(part * width, (part + 1) * width)

    def w_proj(p):
        return r.wp[p].reshape(z.d, z.d)

    w1_all = r.w1.reshape(2, z.nch, na, nb, r.w1.shape[-2], CH)

    def w_fc1(p, c):
        return w1_all[p, c].reshape(z.d, CH)

    w2_per = CH // r.w2.shape[-2]
    w2_all = r.w2.reshape(2, z.nch, w2_per, r.w2.shape[-2], z.d)

    def w_fc2(p, c):
        return w2_all[p, c].reshape(CH, z.d)

    def row(p, k):
        return SMF[p, pl.ds(k, 1), :]

    def masks(dtype):
        lane = lax.broadcasted_iota(jnp.int32, (WP, 128), 1) // z.hd
        return [(lane == h).astype(dtype) for h in range(z.quad)]

    def spread(v, mk):
        return jnp.concatenate([v * q for q in mk], 0)

    def collect(v, mk):
        acc = v[0:WP] * mk[0]
        for h in range(1, z.quad):
            acc = acc + v[h * WP : (h + 1) * WP] * mk[h]
        return acc

    BM = r.bm
    lanes = 128
    per_lane = lanes // WP

    def build_bias(p):
        j = lax.broadcasted_iota(jnp.int32, (WP, lanes), 0)
        lane = lax.broadcasted_iota(jnp.int32, (WP, lanes), 1)
        i = lax.rem(lane, WP)
        iy, ix, jy, jx = i // WIN, lax.rem(i, WIN), j // WIN, lax.rem(j, WIN)
        valid = jnp.logical_and(i < WT, j < WT)
        index = (iy - jy + WIN - 1) * TABLE_SIDE + ix - jx + WIN - 1
        index = jnp.where(valid, index, 0)
        low = jnp.where(index < lanes, index, 0)
        high = jnp.where(index < lanes, 0, index - lanes)
        head_of_lane = lane // WP
        tables = tbl.reshape(2, HEADS, TABLE_PAD)

        def look(head):
            entry = tables[p, pl.ds(head, 1), :]
            one = jnp.take_along_axis(jnp.broadcast_to(entry[:, :lanes], (WP, lanes)), low, axis=1)
            two = jnp.take_along_axis(jnp.broadcast_to(entry[:, lanes:], (WP, lanes)), high, axis=1)
            return jnp.where(index < lanes, one, two)

        def region(q, wy):
            first = jnp.zeros_like(q)
            if wy < ACROSS - 1:
                return first
            return jnp.where(q < WIN - SHIFT, first + 1, first + 2)

        def group_of_heads(g, carry):
            for c in range(z.quad // per_lane):
                value = look(g * z.quad + c * per_lane)
                for e in range(1, per_lane):
                    value = jnp.where(head_of_lane == e, look(g * z.quad + c * per_lane + e), value)
                value = jnp.where(j < WT, value, -1e30)
                for w in range(NW if p else 1):
                    out = value
                    if p == 1:
                        wy, wx = w // ACROSS, w % ACROSS
                        label_i = region(iy, wy) * 3 + region(ix, wx)
                        label_j = region(jy, wy) * 3 + region(jx, wx)
                        out = out + jnp.where(
                            jnp.logical_and(valid, label_i != label_j), MASK_FILL, 0.0
                        )
                    BM[p + w, g, :, c * lanes : (c + 1) * lanes] = out
            return carry

        lax.fori_loop(0, z.ng, group_of_heads, 0)

    X, G = r.mg, r.g
    PM, PMT = r.pm, r.pmt
    FN, N1, K = r.fn, r.n1, r.k
    QK, PR, CTX, CTXT = r.qk, r.pr, r.ctx, r.ctxt
    MID, MG, SN, N2, ACT, SL = r.mid, r.mg, r.sn, r.n2, r.actv, r.sl
    SG, DB = r.sg, r.db

    def forward(p):
        need_small(p)

        def ln1(i):
            if p == 0:
                n = MID[block(i, rows), :]
            else:
                n, inv = normalize(X[block(i, rows), :])
                N1[p, block(i, rows), :] = n.astype(bf16)
                K[block(i, rows), 2 * p : 2 * p + 1] = inv
            f = (n * row(p, 0) + row(p, 1)).astype(bf16)
            FN[p, block(i, rows), :] = f
            CTX[block(i, NW * WP), :] = dotf(PM[p], f, NN).astype(bf16)

        run(0, ni, 0.45 if p else 0.25, ln1)

        def qkv(c):
            for e in range(nt):
                bias = row(p, 6 + c)[:, q_part(e)]
                QK[p, c, :, q_part(e)] = (dotf(CTX[...], w_qkv(p, c, e), NN) + bias).astype(bf16)

        need(QKV, p)
        run(0, 3, 0.7, qkv)

        def attention(i):
            mb, mf = masks(bf16), masks(f32)
            units = [(i * BATCH + e, g) for e in range(BATCH) for g in range(z.ng)]
            at = [(block(u, WP), slice(g * 128, (g + 1) * 128)) for u, g in units]
            raw = [dotf(QK[p, 1, S, L], spread(QK[p, 0, S, L], mb), NT) for S, L in at]
            prs = []
            for (u, g), sc in zip(units, raw):
                w = 1 + lax.rem(u, NW) if p else 0
                sc = sc * z.scaling + BM[w, g]
                e = jnp.exp(sc - jnp.max(sc, 0, keepdims=True))
                pr = (e * (1.0 / jnp.sum(e, 0, keepdims=True))).astype(bf16)
                PR[p, u, g] = pr
                prs.append(pr)
            mixed = [dotf(pr, QK[p, 2, S, L], TN) for pr, (S, L) in zip(prs, at)]
            for v, (S, L) in zip(mixed, at):
                CTX[S, L] = collect(v, mf).astype(bf16)

        run(0, ni * NW // BATCH, 0.7, attention)

        def unperm(i):
            CTXT[p, block(i, rows), :] = dotf(PMT[p], CTX[block(i, NW * WP), :], NN).astype(bf16)

        run(0, ni, 0.21, unperm)
        need(PROJ, p)
        MID[...] = dotf(CTXT[p], w_proj(p), NN)
        spent(0.6)

        def ln2(i):
            mid = X[block(i, rows), :] + MID[block(i, rows), :] + row(p, 2)
            MID[block(i, rows), :] = mid
            n, inv = normalize(mid)
            N2[p, block(i, rows), :] = n.astype(bf16)
            K[block(i, rows), 2 * p + 1 : 2 * p + 2] = inv
            SN[p, block(i, rows), :] = (n * row(p, 3) + row(p, 4)).astype(bf16)

        run(0, ni, 0.26, ln2)
        if p == 1:
            for j, ref in enumerate((ACT, SL)):
                arrived(ref, r.sp.at[j])
        per = z.nch // 2

        for j in range(2):
            need(FC1, p, j)

            def rise(i):
                c = j + 2 * i
                u = dotf(SN[p], w_fc1(p, c), NN) + row(p, 9 + c)
                h = u * ROOT_HALF
                e = 0.5 + 0.5 * lax.erf(h)
                ACT[c] = (u * e).astype(bf16)
                SL[c] = (e + (u * INV_ROOT_TWO_PI) * jnp.exp2(h * h * NEG_LOG2_E)).astype(bf16)

            run(0, per, 1.16, rise)
        need(FC2, p)

        def fall(c):
            MID[...] += dotf(ACT[c], w_fc2(p, c), NN)

        run(0, z.nch, 0.6, fall)
        if p == 0:
            for j, ref in enumerate((ACT, SL)):
                pltpu.make_async_copy(ref, r.spill.at[j], r.sp.at[j]).start()

        def finish(i):
            value = MID[block(i, rows), :] + row(p, 5)
            X[block(i, rows), :] = value.astype(bf16).astype(f32)
            stage_out(value, i, p)

        run(0, ni, 0.08, finish)
        ship_later(0, p, p, (9.0, 14.0, 19.0, 24.0) if p == 0 else (0.0, 5.0, 10.0, 15.0))

    g1_own = r.g1.reshape(z.nch, *w1_all.shape[2:])
    g2_own = r.g2.reshape(z.nch, *w2_all.shape[2:])

    def backward(p):
        gq, gp, g1, g2 = (
            (r.gq, r.gp, g1_own, g2_own) if p else (r.wq.at[1], r.wp.at[1], w1_all.at[1], w2_all.at[1])
        )
        def addrow(k, v):
            SG[p, pl.ds(k, 1), 0 : z.d] = SG[p, pl.ds(k, 1), 0 : z.d] + v

        SG[p] = jnp.zeros(SG.shape[1:], f32)
        DB[...] = jnp.zeros(DB.shape, f32)
        if p == 0:
            for j, ref in enumerate((ACT, SL)):
                arrived(ref, r.sp.at[j])
            gather_sent()

        def fc2_grad(c):
            g2[c] = dotf(ACT[c], G[...], TN).astype(bf16).reshape(g2.shape[1:])

        run(0, z.nch, 0.82, fc2_grad)
        emit(FC2, p)

        def hidden(c):
            hg = dotf(G[...], w_fc2(p, c), NT) * SL[c].astype(f32)
            SG[p, pl.ds(9 + c, 1), 0 : z.d] = column_sum(hg)
            SL[c] = hg.astype(bf16)

        run(0, z.nch, 0.76, hidden)

        def fc1(c):
            g1[c] = dotf(SN[p], SL[c], TN).astype(bf16).reshape(g1.shape[1:])

        run(0, z.nch, 0.85, fc1)
        MID[...] = jnp.zeros(MID.shape, f32)
        emit(FC1, p)

        def n2g(c):
            MID[...] += dotf(SL[c], w_fc1(p, c), NT)

        run(0, z.nch, 0.74, n2g)
        if p == 1:
            for j, ref in enumerate((ACT, SL)):
                pltpu.make_async_copy(r.spill.at[j], ref, r.sp.at[j]).start()

        def ln2(i):
            sl = block(i, rows)
            ng = MID[sl, :]
            n = N2[p, sl, :].astype(f32)
            g = G[sl, :].astype(f32)
            mg = g + norm_pull(ng, n, K[sl, 2 * p + 1 : 2 * p + 2], row(p, 3))
            MG[sl, :] = mg
            addrow(5, column_sum(g))
            addrow(3, column_sum(ng * n))
            addrow(4, column_sum(ng))
            addrow(2, column_sum(mg))
            G[sl, :] = mg.astype(bf16)

        run(0, ni, 0.4, ln2)
        gp[...] = dotf(CTXT[p], G[...], TN).astype(bf16).reshape(gp.shape)
        CTXT[p] = dotf(G[...], w_proj(p), NT).astype(bf16)
        spent(1.2)

        def cgrad(i):
            CTX[block(i, NW * WP), :] = dotf(PM[p], CTXT[p, block(i, rows), :], NN).astype(bf16)

        run(0, ni, 0.23, cgrad)
        emit(PROJ, p)

        def attention(i):
            mb, mf = masks(bf16), masks(f32)
            units = [(i * BATCH + e, g) for e in range(BATCH) for g in range(z.ng)]
            at = [(block(u, WP), slice(g * 128, (g + 1) * 128)) for u, g in units]
            cbd = [spread(CTX[S, L], mb) for S, L in at]
            dps = [dotf(QK[p, 2, S, L], c, NT) for (S, L), c in zip(at, cbd)]
            dvs = [dotf(PR[p, u, g], c, NN) for (u, g), c in zip(units, cbd)]
            sbs = []
            for (u, g), dp in zip(units, dps):
                pf = PR[p, u, g].astype(f32)
                tt = pf * dp
                sc = tt - pf * jnp.sum(tt, 0, keepdims=True)
                DB[g] = DB[g] + sc
                sbs.append(sc.astype(bf16))
            for v, (S, L) in zip(dvs, at):
                QK[p, 2, S, L] = v.astype(bf16)
            dks = [dotf(sb, spread(QK[p, 0, S, L], mb), NN) for sb, (S, L) in zip(sbs, at)]
            dqs = [dotf(sb, QK[p, 1, S, L], TN) for sb, (S, L) in zip(sbs, at)]
            for dk, dq, (S, L) in zip(dks, dqs, at):
                QK[p, 1, S, L] = (dk * z.scaling).astype(bf16)
                QK[p, 0, S, L] = (collect(dq, mf) * z.scaling).astype(bf16)

        def un(c, i):
            dv = dotf(PMT[p], QK[p, c, block(i, NW * WP), :], NN)
            addrow(6 + c, column_sum(dv))
            QK[p, c, block(i, rows), :] = dv.astype(bf16)

        def qkv_grad(c):
            value = dotf(FN[p], QK[p, c, 0:m, :], TN).astype(bf16)
            for e in range(nt):
                gq[c, e] = value[:, q_part(e)].reshape(gq.shape[2:])

        def emit_last(k):
            if k:
                emit(QKV, p, k - 1)

        def pull(sl, c):
            return sum(dotf(QK[p, c, sl, q_part(e)], w_qkv(p, c, e), NT) for e in range(nt))

        def ln1(i):
            sl = block(i, rows)
            ng = pull(sl, 0) + pull(sl, 1) + pull(sl, 2)
            n = N1[p, sl, :].astype(f32)
            xg = MG[sl, :] + norm_pull(ng, n, K[sl, 2 * p : 2 * p + 1], row(p, 0))
            addrow(0, column_sum(ng * n))
            addrow(1, column_sum(ng))
            if p:
                G[sl, :] = xg.astype(bf16)
            stage_out(xg, i, 1 - p)

        shipped(0, 1 - p, 1 - p)
        per = NW // BATCH
        cost = 1.7

        def image_step(k):
            attention(k)

            @pl.when(lax.rem(k, per) == per - 1)
            def _():
                for c in range(3):
                    un(c, k // per)
                ln1(k // per)

        first = per * cost
        if p == 0:
            ship_later(1, p, 1 - p, [first * (i + 1) for i in range(ni)])
        else:
            ship_later(1, p, 1 - p, [first * ni + SHIP + 5.0 * i for i in range(ni)])
        run(0, ni * per, cost, image_step)
        run(0, 3, 0.82, qkv_grad, emit_last)
        emit(QKV, p, 2)
        table_rows(p)
        sum_send(p, 0)

    def table_rows(p):
        src = lax.broadcasted_iota(jnp.int32, (z.quad * WP, TABLE_PAD), 0)
        dst = lax.broadcasted_iota(jnp.int32, (z.quad * WP, TABLE_PAD), 1)
        i = lax.rem(src, WP)
        place = jnp.logical_and(
            i < WT, dst == CENTER - ((i // WIN) * TABLE_SIDE + lax.rem(i, WIN))
        )
        head = src // WP
        pick = jnp.concatenate(
            [jnp.logical_and(place, head == h).astype(bf16) for h in range(z.quad)], 1
        )
        group_row = lax.broadcasted_iota(jnp.int32, (8, WP), 0)
        group_of = lax.broadcasted_iota(jnp.int32, (8, WP), 1)
        rows_of = jnp.logical_and(group_of < WT, group_of // WIN == group_row).astype(bf16)

        def split_dot(x, y, left):
            big = x if left else y
            hi = big.astype(bf16)
            lo = (big - hi.astype(f32)).astype(bf16)
            if left:
                return dotf(hi, y, NN) + dotf(lo, y, NN)
            return dotf(x, hi, NN) + dotf(x, lo, NN)

        def one_group(g):
            e = split_dot(DB[g], pick, True)
            for h in range(z.quad):
                v = e[:, h * TABLE_PAD : (h + 1) * TABLE_PAD]
                v = pltpu.roll(v, 0, 1, stride=1, stride_axis=0)
                v = split_dot(rows_of, v, False)
                v = pltpu.roll(v, 0, 1, stride=TABLE_SIDE - WIN, stride_axis=0)
                SG[p, pl.ds(g * z.quad + h, 1), z.d :] = column_sum(v)

        run(0, z.ng, 0.61, one_group)

    gref = {QKV: r.gq, PROJ: r.gp, FC1: r.g1, FC2: r.g2}
    s1, v1, s2, v2, s3, v3, s4, v4 = (r.s1, r.v1, r.s2, r.v2, r.s3, r.v3, r.s4, r.v4)
    k1, k2, k3 = r.k1, r.k2, r.k3
    done = {}

    def buffer(level, q):
        return getattr(r, f"r{level}_{q.id}")

    def gwin(q, p, a_, b_, t_):
        if p == 0:
            return win(q, wref[q.kind], (1,), a_, b_, t_)
        return win(q, gref[q.kind], (), a_, b_, t_)

    def gout(q):
        return shard(q, r.gq_sum, r.gp_sum, r.g1_sum, r.g2_sum)

    def final(q):
        return pltpu.make_async_copy(
            gout(q), shard(q, r.gq_out, r.gp_out, r.g1_out, r.g2_out), r.og.at[q.id]
        )

    def reached(q, p, level):
        while done.get((q.id, p), 0) < level:
            plan.pop()

    def credit(sem, q, k, p, device):
        if p == 1:
            pl.semaphore_signal(sem.at[q.id, k], inc=1, device_id=device, device_id_type=MESH)

    def spend(sem, q, k, p):
        if p == 0:
            pl.semaphore_wait(sem.at[q.id, k], 1)

    def emit(kind, p, index=None):
        for q in pieces:
            if q.kind == kind and index in (None, q.index):
                r1(q, p)

    def r1(q, p):
        if p == 0:
            reached(q, 1, 2)
        for k, peer in enumerate(c_peers):
            spend(k1, q, k, p)
            send(gwin(q, p, ALL, ALL, peer), buffer(1, q).at[k], s1.at[p, q.id, k], v1.at[p, q.id, k], dev(t_=peer))
            when = plan.link("c", q.unit * na * nb / nt, CORE_LINK, CORE_HOP)
        done[q.id, p] = 1
        plan.add(when, functools.partial(r2, q, p))

    def r2(q, p):
        if p == 0:
            reached(q, 1, 3)
        for k in range(nt - 1):
            arrived(buffer(1, q).at[k], v1.at[p, q.id, k])
        mine = gwin(q, p, ALL, ALL, t)
        add_into(mine, [buffer(1, q).at[k] for k in range(nt - 1)])
        for k, source in enumerate(c_from):
            credit(k1, q, k, p, dev(t_=source))
        plan.clock += q.unit * na * nb / 10e6
        done[q.id, p] = 2
        home = q.sum_home(p)
        if home is None:
            to_y(q, p)
            return

        @pl.when(s != home)
        def _():
            if p == 0:
                pl.semaphore_wait(r.k6.at[q.id], 1)
            send(mine, buffer(6, q), r.s6.at[p, q.id], r.v6.at[p, q.id], dev(s_=home))

        when = plan.link(f"x{other(home)}", q.unit * na * nb, LINK, HOP)
        plan.add(when, functools.partial(r2x, q, p))

    def r2x(q, p):
        home = q.sum_home(p)

        def body():
            arrived(buffer(6, q), r.v6.at[p, q.id])
            add_into(gwin(q, p, ALL, ALL, t), [buffer(6, q)])
            if p == 1:
                pl.semaphore_signal(
                    r.k6.at[q.id], inc=1, device_id=dev(s_=other(home)), device_id_type=MESH
                )

        on(home, body)
        plan.clock += q.unit * na * nb / 10e6
        to_y(q, p)

    def to_y(q, p):
        home = q.sum_home(p)

        def body():
            for k, peer in enumerate(b_peers):
                on(q.sum_home(1), functools.partial(spend, k2, q, k, p))
                send(
                    gwin(q, p, ALL, peer, t),
                    buffer(2, q).at[k],
                    s2.at[p, q.id, k],
                    v2.at[p, q.id, k],
                    dev(b_=peer),
                )

        on(home, body)
        for k in range(nb - 1):
            when = link_of("y", home, q.unit * na)
        plan.add(when, functools.partial(r3, q, p))

    def r3(q, p):
        if p == 0:
            reached(q, 1, 4)
        home = q.sum_home(p)

        def body():
            for k in range(nb - 1):
                arrived(buffer(2, q).at[k], v2.at[p, q.id, k])
            add_into(gwin(q, p, ALL, b, t), [buffer(2, q).at[k] for k in range(nb - 1)])
            for k, source in enumerate(b_from):
                credit(k2, q, k, p, dev(b_=source))
            if p == 0:
                on(q.sum_home(1), lambda: pl.semaphore_wait(k3.at[q.id], na - 1))
            for k, peer in enumerate(a_peers):
                send(
                    gwin(q, p, peer, b, t),
                    buffer(3, q).at[k],
                    s3.at[p, q.id],
                    v3.at[p, q.id],
                    dev(a_=peer),
                )

        on(home, body)
        for k in range(na - 1):
            when = link_of("z", home, q.unit * na / (na - 1))
        done[q.id, p] = 3
        plan.add(when, functools.partial(r4, q, p))

    def r4(q, p):
        if p == 0:
            reached(q, 1, 5)
        home = q.sum_home(p)
        mine = gwin(q, p, a, b, t)

        def summed():
            arrived(buffer(3, q), v3.at[p, q.id])
            total = mine[...].astype(f32)
            for k in range(na - 1):
                total = total + buffer(3, q)[k].astype(f32)
            for k, source in enumerate(a_from):
                if p == 1:
                    pl.semaphore_signal(
                        k3.at[q.id], inc=1, device_id=dev(a_=source), device_id_type=MESH
                    )
            return total

        def keep(total):
            gout(q)[...] = total

        def pass_on(total):
            buffer(5, q)[...] = total.astype(bf16)
            remote(buffer(5, q), buffer(4, q), s4.at[p, q.id], v4.at[p, q.id], dev(s_=p)).start()

        if home is None:
            total = summed()
            pl.when(s == p)(functools.partial(keep, total))
            pl.when(s != p)(functools.partial(pass_on, total))
        else:

            @pl.when(s == home)
            def _():
                (keep if home == p else pass_on)(summed())
                if home == p:
                    final(q).start()

        if home == p:
            done[q.id, p] = 5
            return
        done[q.id, p] = 4
        plan.add(plan.link(f"x{other(p)}", q.unit, LINK, HOP), functools.partial(r5, q, p))

    def r5(q, p):
        home = q.sum_home(p)

        @pl.when(s == p)
        def _():
            arrived(buffer(4, q), v4.at[p, q.id])
            out = gout(q)
            value = buffer(4, q)[...].astype(f32)
            out[...] = value if home is not None else out[...] + value
            final(q).start()

        @pl.when(s != p)
        def _():
            arrived(buffer(5, q), s4.at[p, q.id])

        done[q.id, p] = 5

    def settle(q, p):
        home = q.sum_home(p)
        for k, peer in enumerate(c_peers):
            arrived(gwin(q, p, ALL, ALL, peer), s1.at[p, q.id, k])

        def plane():
            for k, peer in enumerate(b_peers):
                arrived(gwin(q, p, ALL, peer, t), s2.at[p, q.id, k])
            arrived(gwin(q, p, pl.ds(0, na - 1), b, t), s3.at[p, q.id])

        on(home, plane)
        if home is not None:

            @pl.when(s != home)
            def _():
                arrived(gwin(q, p, ALL, ALL, t), r.s6.at[p, q.id])

    def add_into(mine, others):
        lead = mine.shape[:-2]
        count = int(np.prod(lead))

        def one(i, _):
            index = []
            rest = i
            for extent in reversed(lead):
                index.append(lax.rem(rest, extent))
                rest = rest // extent
            index = tuple(reversed(index))
            total = mine[index].astype(f32)
            for o in others:
                total = total + o[index].astype(f32)
            mine[index] = total.astype(bf16)
            return 0

        lax.fori_loop(0, count, one, 0)

    lists = [
        [dev(t_=p) for p in c_peers],
        [dev(b_=p) for p in b_peers],
        [dev(a_=p) for p in a_peers],
    ]
    takes = [r.ra, r.rc, r.rd]
    ss, sv = r.ss, r.sv

    def sum_send(p, k):
        if k == 0:
            r.sums[p, 0] = SG[p].astype(bf16)
        src = r.sums.at[p, k]
        if k < 3:
            for j, target in enumerate(lists[k]):
                send(src, takes[k].at[p, j], ss.at[p, k], sv.at[p, k], target)
        else:

            @pl.when(s != p)
            def _():
                send(src, r.rb, ss.at[p, k], sv.at[p, k], dev(s_=p))

        size = SG.size * nt * (na if k == 2 else 1)
        link = ("c", "y", "z", f"x{other(p)}")[k]
        when = link_of(link, None, size) if k in (1, 2) else plan.link(link, size, LINK, HOP)
        plan.add(when, functools.partial(sum_take, p, k))

    def small_final():
        return pltpu.make_async_copy(r.small_sum, r.small_out, r.og.at[len(pieces)])

    def sum_take(p, k):
        total = r.sums[p, k].astype(f32)
        if k < 3:
            arrived(takes[k].at[p], sv.at[p, k])
            for j in range(len(lists[k])):
                total = total + takes[k][p, j].astype(f32)
            r.sums[p, k + 1] = total.astype(bf16)
            sum_send(p, k + 1)
        else:

            @pl.when(s == p)
            def _():
                arrived(r.rb, sv.at[p, k])
                r.small_sum[...] = total + r.rb[...].astype(f32)
                small_final().start()

    def sums_sent():
        for p in range(ns):
            for k in range(3):
                arrived(takes[k].at[p], ss.at[p, k])

            @pl.when(s != p)
            def _():
                arrived(r.sums.at[p, 3], ss.at[p, 3])

    def is_sum(step, names):
        return step.func is sum_take and (r3 in names and step.args[1] < 2 or r4 in names)

    first = [q for q in pieces if q.kind == QKV]
    for q in first:
        go_z(q, 0)
    small_a(0)
    plan.add(plan.clock + 18.0, functools.partial(small_a, 1))
    plan.until(plan.clock)
    proj = [q for q in pieces if q.kind == PROJ]
    mixed = [q for k in range(2) for q in pieces if q.kind in (FC1, FC2) and q.index == k]
    order = [(q, 0) for q in proj + mixed] + [(q, 1) for q in first + proj + mixed]

    def z_free(q, p):
        return max(plan.free.get(f"z{h}", 0.0) for h in planes(q.home(p)))

    def next_z(k):
        q, p = order[k]
        go_z(q, p)
        if k + 1 < len(order):
            after = order[k + 1]
            plan.add(
                max(x_at[after[0].id, after[1]], z_free(*after) - LEAD), functools.partial(next_z, k + 1)
            )

    plan.add(
        max(x_at[order[0][0].id, 0], z_free(*order[0]) - FIRST), functools.partial(next_z, 0)
    )
    for q in range(ns):
        arrived(tbl.at[q, t], r.tx.at[q])
        for k, peer in enumerate(c_peers):
            send(tbl.at[q, t], tbl.at[q, t], r.tcs.at[q, k], r.tcr.at[q, k], dev(t_=peer))
    spent(0.5)
    image_ready(0)
    load_rows(0, X)

    def early_norm(i, carry):
        n, inv = normalize(X[block(i, rows), :])
        MID[block(i, rows), :] = n
        N1[0, block(i, rows), :] = n.astype(bf16)
        K[block(i, rows), 0:1] = inv
        return carry

    lax.fori_loop(0, ni, early_norm, 0)
    spent(1.3)
    for q in range(ns):
        for k, source in enumerate(c_from):
            arrived(tbl.at[q, source], r.tcr.at[q, k])
    for p in range(2):
        build_bias(p)
        spent(0.7)
    image_ready(1)
    load_rows(1, G)
    spent(0.2)

    for p in range(2):
        forward(p)
    for p in (1, 0):
        backward(p)

    for steps_of in ((r1, r2, r2x, r3), (r4,), (r5, sum_take)):
        while plan.pop_of(lambda step: step.func in steps_of or is_sum(step, steps_of)):
            pass

    for q in pieces:
        for p in range(2):
            settle(q, p)
    for q in pieces:
        final(q).wait()
    small_final().wait()
    small_sent()
    received(0)
    received(1)
    shipped(1, 1, 0)
    shipped(1, 0, 1)
    for k in range(ns - 1):
        arrived(r.tbl_in, r.txs.at[k])
    for q in range(ns):
        for k in range(nt - 1):
            arrived(tbl.at[q, t], r.tcs.at[q, k])
    for j, src in enumerate((r.images, r.cotangent)):
        for k in range(nt - 1):
            arrived(outb.at[j, t], r.xcs.at[j, k])
    sums_sent()


def per_device(z, images, cotangent, norm1_gain, norm1_bias, qkv_weight, qkv_bias, position_table,
               proj_weight, proj_bias, norm2_gain, norm2_bias, fc1_weight, fc1_bias, fc2_weight,
               fc2_bias):
    s = lax.axis_index(SECTION)
    d = lax.axis_index(DP)
    t = lax.axis_index(TENSOR)
    D, nt, na, nb, ns, ni = z.d, z.parts, z.na, z.nb, z.sections, z.ni
    part = t * z.dp + d

    def chosen(values):
        return lax.dynamic_slice_in_dim(values, s * nt * ni, nt * ni, 0)

    perm = window_permutation(nt, z.half, z.hp)

    qrow, prow, f2row = qkv_weight.shape[1], proj_weight.shape[1], fc2_weight.shape[1]
    m, mw, nch = z.m, z.mw, z.nch
    S = jax.ShapeDtypeStruct
    V = pl.BlockSpec(memory_space=pltpu.VMEM)
    A = pl.BlockSpec(memory_space=pl.ANY)
    dma = pltpu.SemaphoreType.DMA
    reg = pltpu.SemaphoreType.REGULAR
    inputs = dict(
        images=(chosen(images), A),
        cotangent=(chosen(cotangent), A),
        q_in=(qkv_weight[0].transpose(1, 0, 2), A),
        p_in=(proj_weight[0], A),
        f1_in=(fc1_weight[0], A),
        f2_in=(fc2_weight[0], A),
        v_n1g=(norm1_gain, V),
        v_n1b=(norm1_bias, V),
        v_pb=(proj_bias, V),
        v_n2g=(norm2_gain, V),
        v_n2b=(norm2_bias, V),
        v_f2b=(fc2_bias, V),
        v_qb=(qkv_bias[0], V),
        v_f1b=(fc1_bias, V),
        v_tab=(position_table[0].T, V),
        pm=(jnp.asarray(perm, bf16), V),
        pmt=(jnp.asarray(perm.transpose(0, 2, 1), bf16), V),
    )
    wide = D + TABLE_PAD
    outputs = dict(
        act=(S(images.shape, bf16), A),
        ig=(S(images.shape, bf16), A),
        gq_out=(S((3, qrow, D // nt), f32), A),
        gp_out=(S((prow, D), f32), A),
        g1_out=(S((qrow, z.ff // nt), f32), A),
        g2_out=(S((f2row, D), f32), A),
        small_out=(S((GATHER_ROWS, wide), f32), A),
        spill=(S((2, nch, m, CH), bf16), A),
    )
    vm = pltpu.VMEM
    z.pieces = make_pieces(z, qrow, prow, f2row)
    W = len(z.pieces)
    cross = sum(q.home(p) is not None for q in z.pieces for p in range(2))
    scratch = dict(
        wq=vm((2, 3, nt, na, nb, qrow, D // nt), bf16),
        wp=vm((2, nt, na, nb, prow, D), bf16),
        w1=vm((2, nt, 2, na, nb, qrow, z.ff // nt // 2), bf16),
        w2=vm((2, nt, na, nb, f2row, D), bf16),
        gq_sum=vm((3, qrow, D // nt), f32),
        gp_sum=vm((prow, D), f32),
        g1_sum=vm((qrow, z.ff // nt), f32),
        g2_sum=vm((f2row, D), f32),
        small_sum=vm((GATHER_ROWS, wide), f32),
        og=dma((W + 1,)),
        sm_in=vm((GATHER_ROWS, D), bf16),
        tbl_in=vm((z.heads_part, TABLE_PAD), f32),
        p0=vm((2, GATHER_ROWS, D), bf16),
        p1=vm((2, GATHER_ROWS, D), bf16),
        p2=vm((2, GATHER_ROWS, D), bf16),
        pa=vm((2, na - 1, GATHER_ROWS, D), bf16),
        pb=vm((2, nb - 1, GATHER_ROWS, D), bf16),
        pc=vm((2, nt - 1, GATHER_ROWS, D), bf16),
        ps=dma((2, 4)),
        psr=dma((2, 4)),
        ws=dma((cross,)),
        wr=dma((cross, na)),
        smf=vm((2, GATHER_ROWS, D), f32),
        tbl=vm((2, nt, z.heads_part, TABLE_PAD), f32),
        outb=vm((2, nt, ni, z.half, D), bf16),
        bm=vm((1 + NW, z.ng, WP, z.quad * WP), f32),
        g=vm((m, D), bf16),
        fn=vm((2, m, D), bf16),
        n1=vm((2, m, D), bf16),
        k=vm((m, 4), f32),
        qk=vm((2, 3, mw, D), bf16),
        pr=vm((2, ni * NW, z.ng, WP, z.quad * WP), bf16),
        ctx=vm((mw, D), bf16),
        ctxt=vm((2, m, D), bf16),
        mid=vm((m, D), f32),
        mg=vm((m, D), f32),
        sn=vm((2, m, D), bf16),
        n2=vm((2, m, D), bf16),
        actv=vm((nch, m, CH), bf16),
        sl=vm((nch, m, CH), bf16),
        sg=vm((2, GATHER_ROWS, wide), f32),
        db=vm((z.ng, WP, z.quad * WP), f32),
        gq=vm((3, nt, na, nb, qrow, D // nt), bf16),
        gp=vm((nt, na, nb, prow, D), bf16),
        g1=vm((nt, 2, na, nb, qrow, z.ff // nt // 2), bf16),
        g2=vm((nt, na, nb, f2row, D), bf16),
        sums=vm((2, 4, GATHER_ROWS, wide), bf16),
        ra=vm((2, nt - 1, GATHER_ROWS, wide), bf16),
        rb=vm((GATHER_ROWS, wide), bf16),
        rc=vm((2, nb - 1, GATHER_ROWS, wide), bf16),
        rd=vm((2, na - 1, GATHER_ROWS, wide), bf16),
        lx=dma((W, ns)),
        xs=dma((W,)),
        zs=dma((W, 2)),
        zr=dma((W, 2, na - 1)),
        ys=dma((W, 2)),
        yr=dma((W, 2, na, nb - 1)),
        cs=dma((W, 2, nt - 1)),
        cr=dma((W, 2, nt - 1)),
        tx=dma((ns,)),
        txs=dma((ns - 1,)),
        tcs=dma((ns, nt - 1)),
        tcr=dma((ns, nt - 1)),
        xl=dma((2,)),
        xcs=dma((2, nt - 1)),
        xcr=dma((2, nt - 1)),
        os=dma((2, 2, nt)),
        orr=dma((2, ns * nt)),
        sp=dma((2,)),
        s1=dma((2, W, nt - 1)),
        v1=dma((2, W, nt - 1)),
        s2=dma((2, W, nb - 1)),
        v2=dma((2, W, nb - 1)),
        s3=dma((2, W)),
        v3=dma((2, W)),
        s4=dma((2, W)),
        v4=dma((2, W)),
        s6=dma((2, W)),
        v6=dma((2, W)),
        k6=reg((W,)),
        k1=reg((W, nt - 1)),
        k2=reg((W, nb - 1)),
        k3=reg((W,)),
        ss=dma((2, 4)),
        sv=dma((2, 4)),
    )
    for q in z.pieces:
        scratch[f"r1_{q.id}"] = vm((nt - 1, na, nb, q.rows, q.cols), bf16)
        scratch[f"r2_{q.id}"] = vm((nb - 1, na, q.rows, q.cols), bf16)
        scratch[f"r3_{q.id}"] = vm((na - 1, q.rows, q.cols), bf16)
        scratch[f"r4_{q.id}"] = vm((q.rows, q.cols), bf16)
        scratch[f"r5_{q.id}"] = vm((q.rows, q.cols), bf16)
        if q.sum_home(1) is not None:
            scratch[f"r6_{q.id}"] = vm((na, nb, q.rows, q.cols), bf16)
    z.names = list(inputs) + list(outputs) + list(scratch)
    results = pl.pallas_call(
        functools.partial(kernel, z),
        out_shape=tuple(o for o, _ in outputs.values()),
        in_specs=[spec for _, spec in inputs.values()],
        out_specs=tuple(spec for _, spec in outputs.values()),
        scratch_shapes=list(scratch.values()),
        compiler_params=pltpu.CompilerParams(
            collective_id=0, has_side_effects=True, vmem_limit_bytes=67043328
        ),
        name="two_blocks",
    )(*[x for x, _ in inputs.values()])
    act, ig, gq, gp, g1, g2, sums, _ = results

    def own_vector(k):
        width = norm1_gain.shape[1]
        return lax.dynamic_slice(sums, (k, d * width), (1, width))

    width = qkv_bias.shape[-1]
    qkv_bias_grad = lax.dynamic_slice(sums, (6, part * width), (3, width))[None]
    width = fc1_bias.shape[1]
    fc1_flat = sums[9 : 9 + nch, :D].reshape(1, -1)
    fc1_bias_grad = lax.dynamic_slice(fc1_flat, (0, part * width), (1, width))
    tables = lax.dynamic_slice(sums, (t * z.heads_part, D), (z.heads_part, TABLE_PAD))
    tables = tables[:, : position_table.shape[1]][:, ::-1].T[None]
    return (
        act[None],
        ig[None],
        own_vector(0),
        own_vector(1),
        gq.transpose(1, 0, 2)[None],
        qkv_bias_grad,
        tables,
        gp[None],
        own_vector(2),
        own_vector(3),
        own_vector(4),
        g1[None],
        fc1_bias_grad,
        g2[None],
        own_vector(5),
    )


def solution(mesh):
    def run(*args):
        z = Sizes(mesh, args[0], args[11])
        return per_device(z, *args)

    in_specs = (
        P(DP, TENSOR, None),
        P(DP, TENSOR, None),
        P(SECTION, DP),
        P(SECTION, DP),
        P(SECTION, DP, None, TENSOR),
        P(SECTION, None, (TENSOR, DP)),
        P(SECTION, None, TENSOR),
        P(SECTION, (TENSOR, DP), None),
        P(SECTION, DP),
        P(SECTION, DP),
        P(SECTION, DP),
        P(SECTION, DP, TENSOR),
        P(SECTION, (TENSOR, DP)),
        P(SECTION, (TENSOR, DP), None),
        P(SECTION, DP),
    )
    out_specs = (
        P(SECTION, DP, TENSOR, None),
        P(SECTION, DP, TENSOR, None),
        P(SECTION, DP),
        P(SECTION, DP),
        P(SECTION, DP, None, TENSOR),
        P(SECTION, None, (TENSOR, DP)),
        P(SECTION, None, TENSOR),
        P(SECTION, (TENSOR, DP), None),
        P(SECTION, DP),
        P(SECTION, DP),
        P(SECTION, DP),
        P(SECTION, DP, TENSOR),
        P(SECTION, (TENSOR, DP)),
        P(SECTION, (TENSOR, DP), None),
        P(SECTION, DP),
    )
    return jax.shard_map(
        run, mesh=mesh, in_specs=in_specs, out_specs=out_specs, check_vma=False
    )
```
